32 devices in a mesh: tm: 8 (over z, y), space: 4 (over x, core).
Axes of the slice: x: 2, y: 2, z: 4, core: 2. Of those that a mesh axis runs over, the one named last changes fastest.
Arguments:
- start_values: float32 [8, 2, 1024, 1024], P('tm', None, 'space'), may hold values from -6 to 6
- node_values: float32 [8, 2, 2, 1024, 1024], P('tm', None, None, 'space'), may hold values from -6 to 6
Outputs:
- next_start: float32 [8, 2, 1024, 1024], P('tm', None, 'space')
- next_nodes: float32 [8, 2, 2, 1024, 1024], P('tm', None, None, 'space')
The draws below stay inside these ranges and needn't reach their ends.
All inputs are finite; a program needn't handle non-finite values.
Results may differ from the reference program's by a relative error of at most 0.00002.
Values sent between devices are 32-bit elements; how exact they have to be, the bound alone decides.
A program may use at most 64 MiB of HBM per device.

```python
import jax
import jax.numpy as jnp
from jax import lax

KX = 1024
KY = 1024
CX = 256
NT = 8


def block_scale(stream_key, dims, shards, low, largest):
    loudness, own = 1.0, jax.random.fold_in(stream_key, 6)
    for dim, shards_of in shards:
        heights = jnp.exp(jax.random.uniform(jax.random.fold_in(own, dim), (shards_of,), jnp.float32, low / len(shards), largest / len(shards)))
        loudness = loudness * jnp.repeat(heights, dims[dim] // shards_of).reshape([-1 if axis == dim else 1 for axis in range(len(dims))])
    return loudness


def scatter_about(key, dims, width, reach, pieces=(), held_as=jnp.bfloat16):
    factor_of = block_scale(key, dims, pieces, -0.22, 0.18) if pieces else 1.0
    values = jax.random.normal(key, dims, jnp.float32) * width * factor_of
    return jnp.minimum(jnp.maximum(values, -reach), reach).astype(held_as)


def setup_inputs(seed: int = 0) -> dict:
    key_list = jax.random.split(jax.random.key(seed), 3)
    start_values = scatter_about(key_list[0], (NT, 2, KX, KY), 1.0, 6.0, ((0, 8), (2, 4)), jnp.float32)
    node_values = scatter_about(key_list[1], (NT, 2, 2, KX, KY), 1.0, 6.0, ((0, 8), (3, 4)), jnp.float32)
    return dict(start_values=start_values, node_values=node_values)


diffusion = 1.5
drift = 0.8
shear = 0.6
first_weights = (5.0 / 24.0, 1.0 / 3.0, -1.0 / 24.0)
second_weights = (-1.0 / 24.0, 1.0 / 3.0, 5.0 / 24.0)
whole_weights = (1.0 / 6.0, 2.0 / 3.0, 1.0 / 6.0)


def spectrum(row_index, column_index):
    along = (row_index.astype(jnp.float32) - KX // 2) / (KX // 2)
    across = (column_index.astype(jnp.float32) - KY // 2) / (KY // 2)
    real_rate = -diffusion * (along[:, None] * along[:, None] + across[None, :] * across[None, :])
    imag_rate = -drift * across[None, :] + 0.0 * along[:, None]
    return real_rate, imag_rate, across


def multiply(real_rate, imag_rate, field):
    return jnp.stack([real_rate * field[..., 0, :, :] - imag_rate * field[..., 1, :, :],
                      real_rate * field[..., 1, :, :] + imag_rate * field[..., 0, :, :]], axis=-3)


def divide(real_part, imag_part, field):
    modulus = real_part * real_part + imag_part * imag_part
    return jnp.stack([(field[..., 0, :, :] * real_part + field[..., 1, :, :] * imag_part) / modulus,
                      (field[..., 1, :, :] * real_part - field[..., 0, :, :] * imag_part) / modulus], axis=-3)


def coupling_of(padded, across):
    sums = padded[..., 2:, :] + padded[..., :-2, :]
    factor = shear * across
    return jnp.stack([factor * sums[..., 1, :, :], -factor * sums[..., 0, :, :]], axis=-3)


def explicit(field, across):
    widths = [(0, 0)] * (field.ndim - 2) + [(1, 1), (0, 0)]
    return coupling_of(jnp.pad(field, widths), across)


def fine_section(begin_value, old_nodes):
    real_rate, imag_rate, across = spectrum(jnp.arange(KX), jnp.arange(KY))
    stacked = jnp.stack([begin_value, old_nodes[0], old_nodes[1]])
    old_coupling = explicit(stacked, across)
    old_slopes = multiply(real_rate, imag_rate, stacked) + old_coupling
    sum_one = first_weights[0] * old_slopes[0] + first_weights[1] * old_slopes[1] + first_weights[2] * old_slopes[2]
    sum_two = second_weights[0] * old_slopes[0] + second_weights[1] * old_slopes[1] + second_weights[2] * old_slopes[2]
    half_real = 1.0 - 0.5 * real_rate
    half_imag = -0.5 * imag_rate
    node_one = divide(half_real, half_imag, begin_value - 0.5 * multiply(real_rate, imag_rate, old_nodes[0]) + sum_one)
    one_coupling = explicit(node_one[None], across)[0]
    node_two = divide(half_real, half_imag, node_one + 0.5 * (one_coupling - old_coupling[1])
                      - 0.5 * multiply(real_rate, imag_rate, old_nodes[1]) + sum_two)
    two_coupling = explicit(node_two[None], across)[0]
    integral = (whole_weights[0] * old_slopes[0]
                + whole_weights[1] * (multiply(real_rate, imag_rate, node_one) + one_coupling)
                + whole_weights[2] * (multiply(real_rate, imag_rate, node_two) + two_coupling))
    low_row = KX // 2 - CX // 2
    low_column = KY // 2 - CX // 2
    coarse_real = real_rate[low_row:low_row + CX, low_column:low_column + CX]
    coarse_imag = imag_rate[low_row:low_row + CX, low_column:low_column + CX]
    begin_coarse = begin_value[:, low_row:low_row + CX, low_column:low_column + CX]
    end_coarse = node_two[:, low_row:low_row + CX, low_column:low_column + CX]
    tau = integral[:, low_row:low_row + CX, low_column:low_column + CX] - 0.5 * multiply(coarse_real, coarse_imag, begin_coarse + end_coarse)
    offset = 0.5 * multiply(coarse_real, coarse_imag, begin_coarse - end_coarse) + tau
    return node_one, node_two, begin_coarse, end_coarse, offset


def reference(start_values, node_values):
    node_one, node_two, begin_coarse, end_coarse, offset = lax.map(
        lambda paired: fine_section(paired[0], paired[1]), (start_values, node_values))
    real_rate, imag_rate, across = spectrum(jnp.arange(KX), jnp.arange(KY))
    low_row = KX // 2 - CX // 2
    low_column = KY // 2 - CX // 2
    coarse_real = real_rate[low_row:low_row + CX, low_column:low_column + CX]
    coarse_imag = imag_rate[low_row:low_row + CX, low_column:low_column + CX]
    step_real = 1.0 - coarse_real
    step_imag = -coarse_imag
    coarse_starts = [begin_coarse[0]]
    for slice_index in range(1, NT):
        coarse_starts.append(divide(step_real, step_imag, coarse_starts[-1] + offset[slice_index - 1]))
    begin_new = jnp.stack(coarse_starts)
    end_new = divide(step_real, step_imag, begin_new + offset)
    delta_begin = begin_new - begin_coarse
    delta_end = end_new - end_coarse
    widths = ((0, 0), (0, 0), (low_row, KX - low_row - CX), (low_column, KY - low_column - CX))
    fixed_one = node_one + jnp.pad(0.5 * (delta_begin + delta_end), widths)
    fixed_two = node_two + jnp.pad(delta_end, widths)
    next_start = jnp.concatenate([start_values[:1], fixed_two[:-1]], axis=0)
    next_nodes = jnp.stack([fixed_one, fixed_two], axis=1)
    return (next_start, next_nodes)
```

```python
import jax
import jax.numpy as jnp
from jax import lax
from jax.experimental import pallas as pl
from jax.experimental.pallas import tpu as pltpu
from jax.sharding import PartitionSpec as P

CX = 256

diffusion = 1.5
drift = 0.8
shear = 0.6
first_weights = (5.0 / 24.0, 1.0 / 3.0, -1.0 / 24.0)
second_weights = (-1.0 / 24.0, 1.0 / 3.0, 5.0 / 24.0)
whole_weights = (1.0 / 6.0, 2.0 / 3.0, 1.0 / 6.0)

MESH = pl.DeviceIdType.MESH
HALO = 8
BLOCK = 32
PARTS = 4
TURN = 3
LANES = 128


def weighted(weights, fields):
    return [sum(w * f[k] for w, f in zip(weights, fields)) for k in range(2)]


def times(real, imag, field):
    return [real * field[0] - imag * field[1], real * field[1] + imag * field[0]]


def coupled(factor, field):
    length = field[0].shape[0]
    sums = [pltpu.roll(f, 1, 0) + pltpu.roll(f, length - 1, 0) for f in field]
    return [factor * sums[1], -factor * sums[0]]


def kernel(
    begin_hbm,
    nodes_hbm,
    start_out,
    nodes_out,
    ext,
    gain,
    shift,
    load_sem,
    start_sem,
    halo_send,
    halo_recv,
    bulk_send,
    bulk_recv,
    relay_send,
    relay_recv,
):
    slab, columns = begin_hbm.shape[1:]
    peers, count = lax.axis_size("space"), lax.axis_size("tm")
    total = slab * peers
    tm, rank = lax.axis_index("tm"), lax.axis_index("space")
    has_prev, has_next = tm > 0, tm < count - 1
    has_up, has_down = rank > 0, rank < peers - 1
    blocks = slab // BLOCK
    low_row = total // 2 - CX // 2
    low_column = columns // 2 - CX // 2
    coarse_rows = gain.shape[1]
    coarse_blocks = coarse_rows // BLOCK
    inward = min(HALO, slab - coarse_rows)
    coarse_rank = (rank * slab < low_row + CX) & (rank * slab + slab > low_row)
    lower = rank < peers // 2
    coarse_start = jnp.clip(low_row - rank * slab, 0, slab - coarse_rows)
    coarse_block = coarse_start // BLOCK
    first = jnp.where(
        coarse_rank,
        jnp.where(lower, coarse_block, blocks - coarse_block - coarse_blocks),
        0,
    )
    ascending = lower != coarse_rank

    def block_of(step):
        index = jnp.where(step < blocks - first, first + step, blocks - 1 - step)
        return jnp.where(lower, index, blocks - 1 - index)

    def rows_of(block):
        return pl.ds(pl.multiple_of(block * BLOCK, BLOCK), BLOCK)

    def load(slot, top, height, left, width, act):
        top, left = pl.multiple_of(top, HALO), pl.multiple_of(left, LANES)
        source, here = pl.ds(top, height), pl.ds(left, width)
        target = pl.ds(pl.multiple_of(top + HALO, HALO), height)
        act(
            pltpu.make_async_copy(
                begin_hbm.at[:, source, here], ext.at[0, :, target, here], load_sem.at[0, slot]
            )
        )
        act(
            pltpu.make_async_copy(
                nodes_hbm.at[:, :, source, here],
                ext.at[1:3, :, target, here],
                load_sem.at[1, slot],
            )
        )

    def load_step(step, act):
        @pl.when(step < blocks - 1)
        def _():
            top = block_of(step) * BLOCK + jnp.where(ascending, HALO, -HALO)
            load(PARTS + step, top, BLOCK, 0, columns, act)

        @pl.when(step == blocks - 1)
        def _():
            height = BLOCK - HALO
            load(PARTS + step, jnp.where(ascending, slab - height, 0), height, 0, columns, act)

    def load_part(part, act):
        height, width = BLOCK + HALO, columns // PARTS
        load(part, jnp.where(ascending, 0, slab - height), height, part * width, width, act)

    def load_coarse(slot, act):
        height = coarse_rows + inward
        top = jnp.where(lower, slab - height, 0)
        if slot == 0:
            load(0, top, height, low_column, CX, act)
        else:
            load(slot, top, height, (slot - 1) * (low_column + CX), low_column, act)

    def begin_copies(act):
        def copy(index, top, height, left, width):
            place = (slice(None), pl.ds(pl.multiple_of(top, HALO), height), pl.ds(left, width))
            act(pltpu.make_async_copy(begin_hbm.at[place], start_out.at[place], start_sem.at[index]))

        @pl.when(coarse_rank)
        def _():
            copy(0, coarse_start, coarse_rows, 0, low_column)
            copy(1, coarse_start, coarse_rows, low_column + CX, low_column)
            if slab > coarse_rows:
                top = jnp.where(lower, 0, coarse_rows)
                copy(2, top, slab - coarse_rows, 0, columns)

        @pl.when(jnp.logical_not(coarse_rank))
        def _():
            copy(0, 0, slab, 0, columns)

    def halos(side):
        source = pl.ds(0 if side == 0 else slab - HALO, HALO)
        target = pl.ds(slab + HALO if side == 0 else 0, HALO)
        there = {"space": rank - 1 if side == 0 else rank + 1}
        return (
            pltpu.make_async_remote_copy(
                begin_hbm.at[:, source, :],
                ext.at[0, :, target, :],
                halo_send.at[0, side],
                halo_recv.at[0, side],
                device_id=there,
                device_id_type=MESH,
            ),
            pltpu.make_async_remote_copy(
                nodes_hbm.at[:, :, source, :],
                ext.at[1:3, :, target, :],
                halo_send.at[1, side],
                halo_recv.at[1, side],
                device_id=there,
                device_id_type=MESH,
            ),
        )

    following = {"tm": tm + 1}

    def relay_copy(step):
        place = (slice(None), rows_of(block_of(step)), pl.ds(low_column, CX))
        return pltpu.make_async_remote_copy(
            nodes_out.at[(1,) + place],
            start_out.at[place],
            relay_send.at[step],
            relay_recv.at[step],
            device_id=following,
            device_id_type=MESH,
        )

    def bulk(unit, act):
        step, part = unit // PARTS, unit % PARTS
        block = block_of(step)
        strip = coarse_rank & (step < coarse_blocks)

        def copy(left, width):
            place = (slice(None), rows_of(block), pl.ds(pl.multiple_of(left, LANES), width))
            act(
                pltpu.make_async_remote_copy(
                    nodes_out.at[(1,) + place],
                    start_out.at[place],
                    bulk_send.at[unit],
                    bulk_recv.at[unit],
                    device_id=following,
                    device_id_type=MESH,
                )
            )

        @pl.when(strip & (part >= PARTS - 2))
        def _():
            copy((part - (PARTS - 2)) * (low_column + CX), low_column)

        quick = (step == 0) & jnp.logical_not(coarse_rank)

        @pl.when(quick)
        def _():
            copy(part * (columns // PARTS), columns // PARTS)

        @pl.when(jnp.logical_not(quick | strip) & (part == PARTS - 1))
        def _():
            copy(0, columns)

    def send(low, high):
        @pl.when(has_next)
        def _():
            @pl.loop(low, high)
            def _(unit):
                bulk(unit, lambda c: c.start())

    barrier = pltpu.get_barrier_semaphore()
    for there, exists in (
        ({"space": rank - 1}, has_up),
        ({"space": rank + 1}, has_down),
        ({"tm": tm - 1}, has_prev),
        ({"tm": tm + 1}, has_next),
    ):

        @pl.when(exists)
        def _(there=there):
            pl.semaphore_signal(barrier, inc=1, device_id=there, device_id_type=MESH)

    def start(copy):
        copy.start()

    def wait(copy):
        copy.wait()

    @pl.when(coarse_rank)
    def _():
        for slot in range(3):
            load_coarse(slot, start)

    @pl.when(jnp.logical_not(coarse_rank))
    def _():
        @pl.loop(0, PARTS)
        def _(part):
            load_part(part, start)

    @pl.loop(jnp.where(coarse_rank, coarse_blocks, 1), blocks)
    def _(step):
        load_step(step, start)

    for side, exists in ((0, has_up), (1, has_down)):

        @pl.when(jnp.logical_not(exists))
        def _(side=side):
            edge = pl.ds(0 if side == 0 else slab + HALO, HALO)
            ext[:, :, edge, :] = jnp.zeros((3, 2, HALO, columns), jnp.float32)

    @pl.when(jnp.logical_not(has_prev))
    def _():
        begin_copies(start)

    def greet():
        friends = sum(jnp.where(e, 1, 0) for e in (has_up, has_down, has_prev, has_next))
        pl.semaphore_wait(barrier, friends)
        for side, exists in ((0, has_up), (1, has_down)):

            @pl.when(exists)
            def _(side=side):
                for c in halos(side):
                    c.start()

    def halo_wait(block):
        for side, edge in ((0, (block == blocks - 1) & has_down), (1, (block == 0) & has_up)):

            @pl.when(edge)
            def _(side=side):
                for c in halos(side):
                    c.wait_recv()

    def strip_compute(block, column, coarse):
        length = BLOCK + 2 * HALO
        span = pl.ds(pl.multiple_of(block * BLOCK, BLOCK), length)
        here = pl.ds(column, LANES)
        begin, one, two = [[ext[f, k, span, here] for k in range(2)] for f in range(3)]
        row = lax.broadcasted_iota(jnp.int32, (length, LANES), 0)
        row = row + (rank * slab + block * BLOCK - HALO)
        along = (row - total // 2).astype(jnp.float32) / (total // 2)
        place = lax.broadcasted_iota(jnp.int32, (1, LANES), 1) + column
        across = (place - columns // 2).astype(jnp.float32) / (columns // 2)
        inside = jnp.where((row >= 0) & (row < total), 1.0, 0.0).astype(jnp.float32)
        real = -diffusion * (along * along + across * across)
        imag = -drift * across
        factor = shear * across
        half_real, half_imag = 1.0 - 0.5 * real, -0.5 * imag
        scale = 1.0 / (half_real * half_real + half_imag * half_imag)
        inverse = (half_real * scale, -half_imag * scale)
        sum_one = weighted(first_weights, (begin, one, two))
        sum_two = weighted(second_weights, (begin, one, two))
        moved = times(real, imag, [s - 0.5 * o for s, o in zip(sum_one, one)])
        turned = coupled(factor, sum_one)
        inner = [begin[k] + moved[k] + turned[k] for k in range(2)]
        node_one = [inside * f for f in times(*inverse, inner)]
        moved = times(real, imag, [s - 0.5 * o for s, o in zip(sum_two, two)])
        turned = coupled(
            factor, [sum_two[k] + 0.5 * (node_one[k] - one[k]) for k in range(2)]
        )
        inner = [node_one[k] + moved[k] + turned[k] for k in range(2)]
        node_two = times(*inverse, inner)
        own = slice(HALO, HALO + BLOCK)
        rows = rows_of(block)
        if not coarse:
            for k in range(2):
                nodes_out[0, k, rows, here] = node_one[k][own]
                nodes_out[1, k, rows, here] = node_two[k][own]
            return
        mean = weighted(whole_weights, (begin, node_one, node_two))
        moved = times(real, imag, [mean[k] - node_two[k] for k in range(2)])
        turned = coupled(factor, mean)
        offset = [moved[k] + turned[k] for k in range(2)]
        step_real, step_imag = 1.0 - real, -imag
        scale = 1.0 / (step_real * step_real + step_imag * step_imag)
        grown = (step_real * scale, -step_imag * scale)
        offset = times(*grown, offset)
        local = pl.ds(pl.multiple_of(block * BLOCK - coarse_start, BLOCK), BLOCK)
        inner_here = pl.ds(pl.multiple_of(column - low_column, LANES), LANES)
        for k in range(2):
            gain[k, local, inner_here] = grown[k][own]
            shift[k, local, inner_here] = offset[k][own]
            kept = node_one[k] - 0.5 * (begin[k] + node_two[k])
            nodes_out[0, k, rows, here] = kept[own]

        @pl.when(jnp.logical_not(has_prev))
        def _():
            for k in range(2):
                start_out[k, rows, here] = begin[k][own]

    def coarse_compute(step):
        block = block_of(step)
        halo_wait(block)

        @pl.loop(0, CX // LANES)
        def _(index):
            strip_compute(block, pl.multiple_of(low_column + index * LANES, LANES), True)

    def relay(low, high):
        @pl.loop(low, high)
        def _(step):
            @pl.when(has_prev)
            def _():
                relay_copy(step).wait_recv()

            block = block_of(step)
            rows = rows_of(block)
            local = pl.ds(pl.multiple_of(block * BLOCK - coarse_start, BLOCK), BLOCK)
            here = pl.ds(low_column, CX)
            begin = [start_out[k, rows, here] for k in range(2)]
            grown = times(gain[0, local, :], gain[1, local, :], begin)
            finish = [grown[k] + shift[k, local, :] for k in range(2)]
            for k in range(2):
                nodes_out[1, k, rows, here] = finish[k]

            @pl.when(has_next)
            def _():
                relay_copy(step).start()

            for k in range(2):
                nodes_out[0, k, rows, here] += 0.5 * (begin[k] + finish[k])

    units = PARTS * blocks
    never = blocks + 1
    turn = jnp.where(coarse_rank, jnp.minimum(TURN * tm, blocks), never)
    early = jnp.where(coarse_rank, jnp.minimum(tm // 2, turn), blocks)

    @pl.when(coarse_rank)
    def _():
        greet()
        load_coarse(0, wait)

        @pl.loop(0, coarse_blocks - 1)
        def _(step):
            coarse_compute(step)

    strips = columns // LANES // PARTS

    @pl.loop(0, blocks + 1)
    def _(step):
        @pl.when(step == turn)
        def _():
            relay(0, coarse_blocks - 1)

        @pl.when(coarse_rank & (step == jnp.minimum(turn, coarse_blocks - 1)))
        def _():
            coarse_compute(coarse_blocks - 1)

        @pl.when(step == turn)
        def _():
            relay(coarse_blocks - 1, coarse_blocks)
            send(PARTS * early, PARTS * turn)

        @pl.when(step < blocks)
        def _():
            block = block_of(step)
            in_coarse = coarse_rank & (step < coarse_blocks)

            @pl.when(step >= jnp.where(coarse_rank, coarse_blocks, 1))
            def _():
                load_step(step, wait)
                halo_wait(block)

            @pl.when(coarse_rank & (step == 0))
            def _():
                load_coarse(1, wait)
                load_coarse(2, wait)

            @pl.loop(0, PARTS)
            def _(part):
                @pl.when(jnp.logical_not(coarse_rank) & (step == 0))
                def _():
                    load_part(part, wait)

                @pl.loop(0, strips)
                def _(index):
                    low = (part * strips + index) * LANES

                    @pl.when(
                        jnp.logical_not(in_coarse & (low >= low_column) & (low < low_column + CX))
                    )
                    def _():
                        strip_compute(block, pl.multiple_of(low, LANES), False)

                unit = PARTS * step + part

                @pl.when(jnp.logical_not(coarse_rank) & (unit == 0))
                def _():
                    greet()

                @pl.when((step < early) | (step >= turn))
                def _():
                    send(unit, unit + 1)

    @pl.when(jnp.logical_not(has_prev))
    def _():
        begin_copies(wait)

    for side, exists in ((0, has_up), (1, has_down)):

        @pl.when(exists)
        def _(side=side):
            for c in halos(side):
                c.wait_send()

    @pl.when(coarse_rank & has_next)
    def _():
        @pl.loop(0, coarse_blocks)
        def _(step):
            relay_copy(step).wait_send()

    @pl.when(has_prev)
    def _():
        @pl.loop(0, units)
        def _(unit):
            bulk(unit, lambda c: c.wait_recv())

    @pl.when(has_next)
    def _():
        @pl.loop(0, units)
        def _(unit):
            bulk(unit, lambda c: c.wait_send())


def write_out(start, nodes, start_hbm, nodes_hbm, sem):
    copies = [
        pltpu.make_async_copy(nodes.at[f, k], nodes_hbm.at[f, k], sem.at[2 * f + k])
        for f in range(2)
        for k in range(2)
    ]
    copies += [pltpu.make_async_copy(start.at[k], start_hbm.at[k], sem.at[4 + k]) for k in range(2)]
    for c in copies:
        c.start()
    for c in copies:
        c.wait()


def body(start_values, node_values):
    slab, columns = start_values.shape[2:]
    peers = lax.axis_size("space")
    coarse_rows = min(slab, max(CX // 2, CX // peers))
    blocks, coarse_blocks = slab // BLOCK, coarse_rows // BLOCK
    hbm = pl.BlockSpec(memory_space=pltpu.HBM)
    vmem = pl.BlockSpec(memory_space=pltpu.VMEM)
    dma = pltpu.SemaphoreType.DMA
    start, nodes = pl.pallas_call(
        kernel,
        out_shape=(
            OUT((2, slab, columns), jnp.float32),
            OUT((2, 2, slab, columns), jnp.float32),
        ),
        in_specs=[hbm, hbm],
        out_specs=(vmem, vmem),
        scratch_shapes=[
            pltpu.VMEM((3, 2, slab + 2 * HALO, columns), jnp.float32),
            pltpu.VMEM((2, coarse_rows, CX), jnp.float32),
            pltpu.VMEM((2, coarse_rows, CX), jnp.float32),
            dma((2, PARTS + blocks)),
            dma((3,)),
            dma((2, 2)),
            dma((2, 2)),
            dma((PARTS * blocks,)),
            dma((PARTS * blocks,)),
            dma((coarse_blocks,)),
            dma((coarse_blocks,)),
        ],
        compiler_params=pltpu.CompilerParams(
            collective_id=0, has_side_effects=True, vmem_limit_bytes=56 * 1024 * 1024
        ),
    )(start_values[0], node_values[0])
    start, nodes = pl.pallas_call(
        write_out,
        out_shape=(
            jax.ShapeDtypeStruct(start.shape, jnp.float32),
            jax.ShapeDtypeStruct(nodes.shape, jnp.float32),
        ),
        in_specs=[pl.BlockSpec(memory_space=pl.ANY)] * 2,
        out_specs=(hbm, hbm),
        scratch_shapes=[dma((6,))],
        compiler_params=pltpu.CompilerParams(vmem_limit_bytes=2 * 1024 * 1024),
    )(start, nodes)
    return (start[None], nodes[None])


OUT = pltpu.VMEM


def solution(mesh):
    in_specs = (P("tm", None, "space", None), P("tm", None, None, "space", None))
    out_specs = (P("tm", None, "space", None), P("tm", None, None, "space", None))
    return jax.shard_map(body, mesh=mesh, in_specs=in_specs, out_specs=out_specs, check_vma=False)
```

```python
import jax
import jax.numpy as jnp
from jax import lax
from jax.experimental import pallas as pl
from jax.experimental.pallas import tpu as pltpu
from jax.sharding import PartitionSpec as P

CX = 256

diffusion = 1.5
drift = 0.8
shear = 0.6
first_weights = (5.0 / 24.0, 1.0 / 3.0, -1.0 / 24.0)
second_weights = (-1.0 / 24.0, 1.0 / 3.0, 5.0 / 24.0)
whole_weights = (1.0 / 6.0, 2.0 / 3.0, 1.0 / 6.0)

MESH = pl.DeviceIdType.MESH
HALO = 8
BLOCK = 32
PARTS = 4
TURN = 3
LANES = 128


def weighted(weights, fields):
    return [sum(w * f[k] for w, f in zip(weights, fields)) for k in range(2)]


def times(real, imag, field):
    return [real * field[0] - imag * field[1], real * field[1] + imag * field[0]]


def coupled(factor, field):
    length = field[0].shape[0]
    sums = [pltpu.roll(f, 1, 0) + pltpu.roll(f, length - 1, 0) for f in field]
    return [factor * sums[1], -factor * sums[0]]


def kernel(
    begin_hbm,
    nodes_hbm,
    start_out,
    nodes_out,
    ext,
    gain,
    shift,
    load_sem,
    start_sem,
    halo_send,
    halo_recv,
    bulk_send,
    bulk_recv,
    relay_send,
    relay_recv,
):
    slab, columns = begin_hbm.shape[1:]
    peers, count = lax.axis_size("space"), lax.axis_size("tm")
    rows_total = slab * peers
    tm, rank = lax.axis_index("tm"), lax.axis_index("space")
    has_prev, has_next = tm > 0, tm < count - 1
    has_up, has_down = rank > 0, rank < peers - 1
    blocks = slab // BLOCK
    low_row = rows_total // 2 - CX // 2
    low_column = columns // 2 - CX // 2
    coarse_rows = gain.shape[1]
    coarse_blocks = coarse_rows // BLOCK
    inward = min(HALO, slab - coarse_rows)
    coarse_rank = (rank * slab < low_row + CX) & (rank * slab + slab > low_row)
    lower = rank < peers // 2
    coarse_start = jnp.clip(low_row - rank * slab, 0, slab - coarse_rows)
    coarse_block = coarse_start // BLOCK
    first = jnp.where(
        coarse_rank,
        jnp.where(lower, coarse_block, blocks - coarse_block - coarse_blocks),
        0,
    )

    def block_of(step):
        index = jnp.where(step < blocks - first, first + step, blocks - 1 - step)
        return jnp.where(lower, index, blocks - 1 - index)

    def rows_of(block):
        return pl.ds(pl.multiple_of(block * BLOCK, BLOCK), BLOCK)

    def load(slot, top, height, left, width):
        top, left = pl.multiple_of(top, HALO), pl.multiple_of(left, LANES)
        source, here = pl.ds(top, height), pl.ds(left, width)
        target = pl.ds(pl.multiple_of(top + HALO, HALO), height)
        pltpu.make_async_copy(
            begin_hbm.at[:, source, here], ext.at[0, :, target, here], load_sem.at[slot]
        ).start()
        pltpu.make_async_copy(
            nodes_hbm.at[:, :, source, here], ext.at[1:3, :, target, here], load_sem.at[slot]
        ).start()

    def loaded(slot, height, width):
        part = ext.at[:, :, pl.ds(0, height), pl.ds(0, width)]
        pltpu.make_async_copy(part, part, load_sem.at[slot]).wait()

    side_rows = coarse_rows + inward
    first_rows, width = BLOCK + HALO, columns // PARTS
    rest_rows = slab - first_rows - BLOCK

    def load_coarse_rank():
        top = jnp.where(lower, slab - side_rows, 0)
        load(0, top, side_rows, low_column, CX)
        load(1, top, side_rows, 0, low_column)
        load(1, top, side_rows, low_column + CX, low_column)
        if slab > side_rows:
            load(2, jnp.where(lower, 0, side_rows), slab - side_rows, 0, columns)

    def load_other_rank():
        @pl.loop(0, PARTS)
        def _(part):
            load(part, jnp.where(lower, 0, slab - first_rows), first_rows, part * width, width)

        load(PARTS, jnp.where(lower, first_rows, rest_rows), BLOCK, 0, columns)
        load(PARTS + 1, jnp.where(lower, slab - rest_rows, 0), rest_rows, 0, columns)

    def begin_copies():
        def copy(top, height, left, width):
            place = (slice(None), pl.ds(pl.multiple_of(top, HALO), height), pl.ds(left, width))
            pltpu.make_async_copy(begin_hbm.at[place], start_out.at[place], start_sem).start()

        @pl.when(coarse_rank)
        def _():
            copy(coarse_start, coarse_rows, 0, low_column)
            copy(coarse_start, coarse_rows, low_column + CX, low_column)
            if slab > coarse_rows:
                top = jnp.where(lower, 0, coarse_rows)
                copy(top, slab - coarse_rows, 0, columns)

        @pl.when(jnp.logical_not(coarse_rank))
        def _():
            copy(0, slab, 0, columns)

    def halo_start(side):
        source = pl.ds(0 if side == 0 else slab - HALO, HALO)
        target = pl.ds(slab + HALO if side == 0 else 0, HALO)
        for slot, left, extent in (
            (0, low_column, CX),
            (1, 0, low_column),
            (1, low_column + CX, low_column),
        ):
            here = pl.ds(left, extent)
            for there_from, there_to in (
                (begin_hbm.at[:, source, here], ext.at[0, :, target, here]),
                (nodes_hbm.at[:, :, source, here], ext.at[1:3, :, target, here]),
            ):
                pltpu.make_async_remote_copy(
                    there_from,
                    there_to,
                    halo_send.at[side],
                    halo_recv.at[side, slot],
                    device_id={"space": rank - 1 if side == 0 else rank + 1},
                    device_id_type=MESH,
                ).start()

    def halo_wait(block, slot):
        for side, edge in ((0, (block == blocks - 1) & has_down), (1, (block == 0) & has_up)):

            @pl.when(edge)
            def _(side=side):
                part = ext.at[:, :, pl.ds(0, HALO), pl.ds(0, CX if slot == 0 else columns - CX)]
                pltpu.make_async_copy(part, part, halo_recv.at[side, slot]).wait()

    following = {"tm": tm + 1}

    def relay_copy(step):
        place = (slice(None), rows_of(block_of(step)), pl.ds(low_column, CX))
        return pltpu.make_async_remote_copy(
            nodes_out.at[(1,) + place],
            start_out.at[place],
            relay_send,
            relay_recv.at[step],
            device_id=following,
            device_id_type=MESH,
        )

    def bulk(unit):
        step, part = unit // PARTS, unit % PARTS
        block = block_of(step)
        strip = coarse_rank & (step < coarse_blocks)

        def copy(left, width):
            place = (slice(None), rows_of(block), pl.ds(pl.multiple_of(left, LANES), width))
            pltpu.make_async_remote_copy(
                nodes_out.at[(1,) + place],
                start_out.at[place],
                bulk_send,
                bulk_recv,
                device_id=following,
                device_id_type=MESH,
            ).start()

        @pl.when(strip & (part >= PARTS - 2))
        def _():
            copy((part - (PARTS - 2)) * (low_column + CX), low_column)

        quick = (step == 0) & jnp.logical_not(coarse_rank)

        @pl.when(quick)
        def _():
            copy(part * (columns // PARTS), columns // PARTS)

        @pl.when(jnp.logical_not(quick | strip) & (part == PARTS - 1))
        def _():
            copy(0, columns)

    def send(low, high):
        @pl.when(has_next)
        def _():
            @pl.loop(low, high)
            def _(unit):
                bulk(unit)

    barrier = pltpu.get_barrier_semaphore()
    for there, exists in (
        ({"space": rank - 1}, has_up),
        ({"space": rank + 1}, has_down),
        ({"tm": tm - 1}, has_prev),
        ({"tm": tm + 1}, has_next),
    ):

        @pl.when(exists)
        def _(there=there):
            pl.semaphore_signal(barrier, inc=1, device_id=there, device_id_type=MESH)

    pl.when(coarse_rank)(load_coarse_rank)
    pl.when(jnp.logical_not(coarse_rank))(load_other_rank)

    for side, exists in ((0, has_up), (1, has_down)):

        @pl.when(jnp.logical_not(exists))
        def _(side=side):
            edge = pl.ds(0 if side == 0 else slab + HALO, HALO)
            ext[:, :, edge, :] = jnp.zeros((3, 2, HALO, columns), jnp.float32)

    pl.when(jnp.logical_not(has_prev))(begin_copies)

    def greet():
        friends = sum(jnp.where(e, 1, 0) for e in (has_up, has_down, has_prev, has_next))
        pl.semaphore_wait(barrier, friends)
        for side, exists in ((0, has_up), (1, has_down)):

            @pl.when(exists)
            def _(side=side):
                halo_start(side)

    def strip_compute(block, column, coarse):
        length = BLOCK + 2 * HALO
        span = pl.ds(pl.multiple_of(block * BLOCK, BLOCK), length)
        here = pl.ds(column, LANES)
        begin, one, two = [[ext[f, k, span, here] for k in range(2)] for f in range(3)]
        row = lax.broadcasted_iota(jnp.int32, (length, LANES), 0)
        row = row + (rank * slab + block * BLOCK - HALO)
        along = (row - rows_total // 2).astype(jnp.float32) / (rows_total // 2)
        place = lax.broadcasted_iota(jnp.int32, (1, LANES), 1) + column
        across = (place - columns // 2).astype(jnp.float32) / (columns // 2)
        inside = jnp.where((row >= 0) & (row < rows_total), 1.0, 0.0).astype(jnp.float32)
        real = -diffusion * (along * along + across * across)
        imag = -drift * across
        factor = shear * across
        half_real, half_imag = 1.0 - 0.5 * real, -0.5 * imag
        scale = 1.0 / (half_real * half_real + half_imag * half_imag)
        inverse = (half_real * scale, -half_imag * scale)
        sum_one = weighted(first_weights, (begin, one, two))
        sum_two = weighted(second_weights, (begin, one, two))
        moved = times(real, imag, [s - 0.5 * o for s, o in zip(sum_one, one)])
        turned = coupled(factor, sum_one)
        inner = [begin[k] + moved[k] + turned[k] for k in range(2)]
        node_one = [inside * f for f in times(*inverse, inner)]
        moved = times(real, imag, [s - 0.5 * o for s, o in zip(sum_two, two)])
        turned = coupled(
            factor, [sum_two[k] + 0.5 * (node_one[k] - one[k]) for k in range(2)]
        )
        inner = [node_one[k] + moved[k] + turned[k] for k in range(2)]
        node_two = times(*inverse, inner)
        own = slice(HALO, HALO + BLOCK)
        rows = rows_of(block)
        if not coarse:
            for k in range(2):
                nodes_out[0, k, rows, here] = node_one[k][own]
                nodes_out[1, k, rows, here] = node_two[k][own]
            return
        mean = weighted(whole_weights, (begin, node_one, node_two))
        moved = times(real, imag, [mean[k] - node_two[k] for k in range(2)])
        turned = coupled(factor, mean)
        offset = [moved[k] + turned[k] for k in range(2)]
        step_real, step_imag = 1.0 - real, -imag
        scale = 1.0 / (step_real * step_real + step_imag * step_imag)
        grown = (step_real * scale, -step_imag * scale)
        offset = times(*grown, offset)
        local = pl.ds(pl.multiple_of(block * BLOCK - coarse_start, BLOCK), BLOCK)
        inner_here = pl.ds(pl.multiple_of(column - low_column, LANES), LANES)
        for k in range(2):
            gain[k, local, inner_here] = grown[k][own]
            shift[k, local, inner_here] = offset[k][own]
            kept = node_one[k] - 0.5 * (begin[k] + node_two[k])
            nodes_out[0, k, rows, here] = kept[own]

        @pl.when(jnp.logical_not(has_prev))
        def _():
            for k in range(2):
                start_out[k, rows, here] = begin[k][own]

    def coarse_compute(step):
        block = block_of(step)
        halo_wait(block, 0)

        @pl.loop(0, CX // LANES)
        def _(index):
            strip_compute(block, pl.multiple_of(low_column + index * LANES, LANES), True)

    def relay(low, high):
        @pl.loop(low, high)
        def _(step):
            @pl.when(has_prev)
            def _():
                relay_copy(step).wait_recv()

            block = block_of(step)
            rows = rows_of(block)
            local = pl.ds(pl.multiple_of(block * BLOCK - coarse_start, BLOCK), BLOCK)
            here = pl.ds(low_column, CX)
            begin = [start_out[k, rows, here] for k in range(2)]
            grown = times(gain[0, local, :], gain[1, local, :], begin)
            finish = [grown[k] + shift[k, local, :] for k in range(2)]
            for k in range(2):
                nodes_out[1, k, rows, here] = finish[k]

            @pl.when(has_next)
            def _():
                relay_copy(step).start()

            for k in range(2):
                nodes_out[0, k, rows, here] += 0.5 * (begin[k] + finish[k])

    never = blocks + 1
    turn = jnp.where(coarse_rank, jnp.minimum(TURN * tm, blocks), never)
    early = jnp.where(coarse_rank, jnp.minimum(tm // 2, turn), blocks)

    @pl.when(coarse_rank)
    def _():
        greet()
        loaded(0, side_rows, CX)

        @pl.loop(0, coarse_blocks - 1)
        def _(step):
            coarse_compute(step)

    strips = columns // LANES // PARTS

    @pl.loop(0, blocks + 1)
    def _(step):
        @pl.when(step == turn)
        def _():
            relay(0, coarse_blocks - 1)

        @pl.when(coarse_rank & (step == jnp.minimum(turn, coarse_blocks - 1)))
        def _():
            coarse_compute(coarse_blocks - 1)

        @pl.when(step == turn)
        def _():
            relay(coarse_blocks - 1, coarse_blocks)
            send(PARTS * early, PARTS * turn)

        @pl.when(step < blocks)
        def _():
            block = block_of(step)
            in_coarse = coarse_rank & (step < coarse_blocks)

            @pl.when(coarse_rank & (step == 0))
            def _():
                loaded(1, side_rows, columns - CX)

            if slab > side_rows:

                @pl.when(coarse_rank & (step == coarse_blocks))
                def _():
                    loaded(2, slab - side_rows, columns)

            for slot, height in ((PARTS, BLOCK), (PARTS + 1, rest_rows)):

                @pl.when(jnp.logical_not(coarse_rank) & (step == slot - PARTS + 1))
                def _(slot=slot, height=height):
                    loaded(slot, height, columns)

            @pl.when(jnp.logical_not(in_coarse))
            def _():
                halo_wait(block, 0)

            halo_wait(block, 1)

            @pl.loop(0, PARTS)
            def _(part):
                @pl.when(jnp.logical_not(coarse_rank) & (step == 0))
                def _():
                    loaded(part, first_rows, width)

                @pl.loop(0, strips)
                def _(index):
                    low = (part * strips + index) * LANES

                    @pl.when(
                        jnp.logical_not(in_coarse & (low >= low_column) & (low < low_column + CX))
                    )
                    def _():
                        strip_compute(block, pl.multiple_of(low, LANES), False)

                unit = PARTS * step + part

                @pl.when(jnp.logical_not(coarse_rank) & (unit == 0))
                def _():
                    greet()

                @pl.when((step < early) | (step >= turn))
                def _():
                    send(unit, unit + 1)

    def total(sem, height, extent):
        part = start_out.at[:, pl.ds(0, height), pl.ds(0, extent)]
        pltpu.make_async_copy(part, part, sem).wait()

    def all_bulk(sem):
        @pl.when(coarse_rank)
        def _():
            total(sem, slab - coarse_rows * CX // columns, columns)

        @pl.when(jnp.logical_not(coarse_rank))
        def _():
            total(sem, slab, columns)

    for side, exists in ((0, has_up), (1, has_down)):

        @pl.when(exists)
        def _(side=side):
            part = ext.at[:, :, pl.ds(0, HALO), :]
            pltpu.make_async_copy(part, part, halo_send.at[side]).wait()

    @pl.when(coarse_rank & has_next)
    def _():
        total(relay_send, coarse_rows, CX)

    @pl.when(jnp.logical_not(has_prev))
    def _():
        all_bulk(start_sem)

    @pl.when(has_prev)
    def _():
        all_bulk(bulk_recv)

    @pl.when(has_next)
    def _():
        all_bulk(bulk_send)


def write_out(start, nodes, start_hbm, nodes_hbm, sem):
    for source, target, which in ((nodes, nodes_hbm, 0), (start, start_hbm, 1)):
        for k in range(source.shape[0]):
            pltpu.make_async_copy(source.at[k], target.at[k], sem.at[which]).start()
    pltpu.make_async_copy(nodes, nodes_hbm, sem.at[0]).wait()
    pltpu.make_async_copy(start, start_hbm, sem.at[1]).wait()


def body(start_values, node_values):
    slab, columns = start_values.shape[2:]
    peers = lax.axis_size("space")
    coarse_rows = min(slab, max(CX // 2, CX // peers))
    coarse_blocks = coarse_rows // BLOCK
    hbm = pl.BlockSpec(memory_space=pltpu.HBM)
    vmem = pl.BlockSpec(memory_space=pltpu.VMEM)
    dma = pltpu.SemaphoreType.DMA
    start, nodes = pl.pallas_call(
        kernel,
        out_shape=(
            OUT((2, slab, columns), jnp.float32),
            OUT((2, 2, slab, columns), jnp.float32),
        ),
        in_specs=[hbm, hbm],
        out_specs=(vmem, vmem),
        scratch_shapes=[
            pltpu.VMEM((3, 2, slab + 2 * HALO, columns), jnp.float32),
            pltpu.VMEM((2, coarse_rows, CX), jnp.float32),
            pltpu.VMEM((2, coarse_rows, CX), jnp.float32),
            dma((PARTS + 2,)),
            dma,
            dma((2,)),
            dma((2, 2)),
            dma,
            dma,
            dma,
            dma((coarse_blocks,)),
        ],
        compiler_params=pltpu.CompilerParams(
            collective_id=0, has_side_effects=True, vmem_limit_bytes=56 * 1024 * 1024
        ),
    )(start_values[0], node_values[0])
    start, nodes = pl.pallas_call(
        write_out,
        out_shape=(
            jax.ShapeDtypeStruct(start.shape, jnp.float32),
            jax.ShapeDtypeStruct(nodes.shape, jnp.float32),
        ),
        in_specs=[pl.BlockSpec(memory_space=pl.ANY)] * 2,
        out_specs=(hbm, hbm),
        scratch_shapes=[dma((2,))],
        compiler_params=pltpu.CompilerParams(vmem_limit_bytes=2 * 1024 * 1024),
    )(start, nodes)
    return (start[None], nodes[None])


OUT = pltpu.VMEM


def solution(mesh):
    in_specs = (P("tm", None, "space", None), P("tm", None, None, "space", None))
    out_specs = (P("tm", None, "space", None), P("tm", None, None, "space", None))
    return jax.shard_map(body, mesh=mesh, in_specs=in_specs, out_specs=out_specs, check_vma=False)
```

```python
import functools

import jax
import jax.numpy as jnp
from jax import lax
from jax.experimental import pallas as pl
from jax.experimental.pallas import tpu as pltpu
from jax.sharding import PartitionSpec as P

CX = 256

diffusion = 1.5
drift = 0.8
shear = 0.6
first_weights = (5.0 / 24.0, 1.0 / 3.0, -1.0 / 24.0)
second_weights = (-1.0 / 24.0, 1.0 / 3.0, 5.0 / 24.0)
whole_weights = (1.0 / 6.0, 2.0 / 3.0, 1.0 / 6.0)

MESH = pl.DeviceIdType.MESH
HALO = 8
BLOCK = 32
PARTS = 4
LATE = 4
TURN = 2
EARLY = 3
PIECES = 4
LANES = 128


def weighted(weights, fields):
    return [sum(w * f[k] for w, f in zip(weights, fields)) for k in range(2)]


def times(real, imag, field):
    return [real * field[0] - imag * field[1], real * field[1] + imag * field[0]]


def coupled(factor, field):
    length = field[0].shape[0]
    sums = [pltpu.roll(f, 1, 0) + pltpu.roll(f, length - 1, 0) for f in field]
    return [factor * sums[1], -factor * sums[0]]


def late(tm):
    return tm >= LATE


def kernel(
    begin_hbm,
    nodes_hbm,
    start_out,
    nodes_out,
    ext,
    gain,
    shift,
    load_sem,
    start_sem,
    halo_send,
    halo_recv,
    bulk_send,
    bulk_recv,
    relay_send,
    relay_recv,
):
    slab, columns = begin_hbm.shape[1:]
    peers, count = lax.axis_size("space"), lax.axis_size("tm")
    rows_total = slab * peers
    tm, rank = lax.axis_index("tm"), lax.axis_index("space")
    has_prev, has_next = tm > 0, tm < count - 1
    has_up, has_down = rank > 0, rank < peers - 1
    blocks = slab // BLOCK
    low_row = rows_total // 2 - CX // 2
    low_column = columns // 2 - CX // 2
    coarse_rows = gain.shape[1]
    coarse_blocks = coarse_rows // BLOCK
    inward = min(HALO, slab - coarse_rows)
    coarse_rank = (rank * slab < low_row + CX) & (rank * slab + slab > low_row)
    lower = rank < peers // 2
    coarse_start = jnp.clip(low_row - rank * slab, 0, slab - coarse_rows)
    coarse_block = coarse_start // BLOCK
    first = jnp.where(
        coarse_rank,
        jnp.where(lower, coarse_block, blocks - coarse_block - coarse_blocks),
        0,
    )

    def block_of(step):
        index = jnp.where(step < blocks - first, first + step, blocks - 1 - step)
        return jnp.where(lower, index, blocks - 1 - index)

    def rows_of(block):
        return pl.ds(pl.multiple_of(block * BLOCK, BLOCK), BLOCK)

    def load(slot, top, height, left, width):
        top, left = pl.multiple_of(top, HALO), pl.multiple_of(left, LANES)
        source, here = pl.ds(top, height), pl.ds(left, width)
        target = pl.ds(pl.multiple_of(top + HALO, HALO), height)
        pltpu.make_async_copy(
            begin_hbm.at[:, source, here], ext.at[0, :, target, here], load_sem.at[slot]
        ).start()
        pltpu.make_async_copy(
            nodes_hbm.at[:, :, source, here], ext.at[1:3, :, target, here], load_sem.at[slot]
        ).start()

    def loaded(slot, height, width):
        part = ext.at[:, :, pl.ds(0, height), pl.ds(0, width)]
        pltpu.make_async_copy(part, part, load_sem.at[slot]).wait()

    side_rows = coarse_rows + inward
    first_rows, width = BLOCK + HALO, columns // PARTS
    rest_rows = slab - first_rows - BLOCK

    def load_coarse_rank():
        top = jnp.where(lower, slab - side_rows, 0)
        load(0, top, side_rows, low_column, CX)
        load(1, top, side_rows, 0, low_column)
        load(1, top, side_rows, low_column + CX, low_column)
        if slab > side_rows:
            load(2, jnp.where(lower, 0, side_rows), slab - side_rows, 0, columns)

    def load_other_rank():
        @pl.loop(0, PARTS)
        def _(part):
            load(part, jnp.where(lower, 0, slab - first_rows), first_rows, part * width, width)

        load(PARTS, jnp.where(lower, first_rows, rest_rows), BLOCK, 0, columns)
        load(PARTS + 1, jnp.where(lower, slab - rest_rows, 0), rest_rows, 0, columns)

    def begin_copies():
        def copy(top, height, left, width):
            place = (slice(None), pl.ds(pl.multiple_of(top, HALO), height), pl.ds(left, width))
            pltpu.make_async_copy(begin_hbm.at[place], start_out.at[place], start_sem).start()

        @pl.when(coarse_rank)
        def _():
            copy(coarse_start, coarse_rows, 0, low_column)
            copy(coarse_start, coarse_rows, low_column + CX, low_column)
            if slab > coarse_rows:
                top = jnp.where(lower, 0, coarse_rows)
                copy(top, slab - coarse_rows, 0, columns)

        @pl.when(jnp.logical_not(coarse_rank))
        def _():
            copy(0, slab, 0, columns)

    def halo_start(side, slot, sources):
        target = pl.ds(slab + HALO if side == 0 else 0, HALO)
        for left, extent in (
            ((low_column, CX),)
            if slot == 0
            else ((0, low_column), (low_column + CX, low_column))
        ):
            here = pl.ds(left, extent)
            for source, place in zip(sources, (0, slice(1, 3))):
                pltpu.make_async_remote_copy(
                    source.at[..., here],
                    ext.at[place, :, target, here],
                    halo_send.at[side],
                    halo_recv.at[side, slot],
                    device_id={"space": rank - 1 if side == 0 else rank + 1},
                    device_id_type=MESH,
                ).start()

    def halo_exchange(slots, loaded_edge):
        for side, exists in ((0, has_up), (1, has_down)):
            edge = pl.ds(0 if side == 0 else slab - HALO, HALO)
            held = pl.ds(HALO if side == 0 else slab, HALO)
            inner = coarse_rank & (lower if side == 1 else jnp.logical_not(lower))
            for slot in slots:
                fit = inner if loaded_edge else jnp.logical_not(inner)
                fit = exists if slot == 1 else exists & fit
                sources = (
                    (ext.at[0, :, held, :], ext.at[1:3, :, held, :])
                    if loaded_edge
                    else (begin_hbm.at[:, edge, :], nodes_hbm.at[:, :, edge, :])
                )

                @pl.when(fit)
                def _(side=side, slot=slot, sources=sources):
                    halo_start(side, slot, sources)

    def halo_wait(block, slot):
        for side, edge in ((0, (block == blocks - 1) & has_down), (1, (block == 0) & has_up)):

            @pl.when(edge)
            def _(side=side):
                part = ext.at[:, :, pl.ds(0, HALO), pl.ds(0, CX if slot == 0 else columns - CX)]
                pltpu.make_async_copy(part, part, halo_recv.at[side, slot]).wait()

    following = {"tm": tm + 1}

    def relay_rows(step, origin):
        top = block_of(step // PIECES) * BLOCK + step % PIECES * (BLOCK // PIECES) - origin
        return pl.ds(pl.multiple_of(top, HALO), BLOCK // PIECES)

    def relay_copy(step):
        place = (slice(None), relay_rows(step, 0), pl.ds(low_column, CX))
        return pltpu.make_async_remote_copy(
            nodes_out.at[(1,) + place],
            start_out.at[place],
            relay_send,
            relay_recv.at[step],
            device_id=following,
            device_id_type=MESH,
        )

    def bulk(unit):
        step, part = unit // PARTS, unit % PARTS
        block = block_of(step)
        strip = coarse_rank & (step < coarse_blocks)

        def copy(left, width):
            place = (slice(None), rows_of(block), pl.ds(pl.multiple_of(left, LANES), width))
            pltpu.make_async_remote_copy(
                nodes_out.at[(1,) + place],
                start_out.at[place],
                bulk_send,
                bulk_recv,
                device_id=following,
                device_id_type=MESH,
            ).start()

        @pl.when(strip & (part >= PARTS - 2))
        def _():
            copy((part - (PARTS - 2)) * (low_column + CX), low_column)

        quick = (step == 0) & jnp.logical_not(coarse_rank)

        @pl.when(quick)
        def _():
            copy(part * (columns // PARTS), columns // PARTS)

        @pl.when(jnp.logical_not(quick | coarse_rank) & (part == PARTS - 1))
        def _():
            copy(0, columns)

    def send(step, low, high):
        held = coarse_rank & late(tm) & (step == coarse_blocks - 1)

        @pl.when(has_next & jnp.logical_not(held))
        def _():
            @pl.loop(low, high)
            def _(part):
                bulk(PARTS * step + part)

    barrier = pltpu.get_barrier_semaphore()
    for there, exists in (
        ({"space": rank - 1}, has_up),
        ({"space": rank + 1}, has_down),
        ({"tm": tm - 1}, has_prev),
        ({"tm": tm + 1}, has_next),
    ):

        @pl.when(exists)
        def _(there=there):
            pl.semaphore_signal(barrier, inc=1, device_id=there, device_id_type=MESH)

    pl.when(coarse_rank)(load_coarse_rank)
    pl.when(jnp.logical_not(coarse_rank))(load_other_rank)

    for side, exists in ((0, has_up), (1, has_down)):

        @pl.when(jnp.logical_not(exists))
        def _(side=side):
            edge = pl.ds(0 if side == 0 else slab + HALO, HALO)
            ext[:, :, edge, :] = jnp.zeros((3, 2, HALO, columns), jnp.float32)

    pl.when(jnp.logical_not(has_prev))(begin_copies)

    def greet():
        friends = sum(jnp.where(e, 1, 0) for e in (has_up, has_down, has_prev, has_next))
        pl.semaphore_wait(barrier, friends)
    def strip_compute(block, column, coarse):
        length = BLOCK + 2 * HALO
        span = pl.ds(pl.multiple_of(block * BLOCK, BLOCK), length)
        here = pl.ds(column, LANES)
        begin, one, two = [[ext[f, k, span, here] for k in range(2)] for f in range(3)]
        row = lax.broadcasted_iota(jnp.int32, (length, LANES), 0)
        row = row + (rank * slab + block * BLOCK - HALO)
        along = (row - rows_total // 2).astype(jnp.float32) / (rows_total // 2)
        place = lax.broadcasted_iota(jnp.int32, (1, LANES), 1) + column
        across = (place - columns // 2).astype(jnp.float32) / (columns // 2)
        inside = jnp.where((row >= 0) & (row < rows_total), 1.0, 0.0).astype(jnp.float32)
        real = -diffusion * (along * along + across * across)
        imag = -drift * across
        factor = shear * across
        half_real, half_imag = 1.0 - 0.5 * real, -0.5 * imag
        scale = 1.0 / (half_real * half_real + half_imag * half_imag)
        inverse = (half_real * scale, -half_imag * scale)
        sum_one = weighted(first_weights, (begin, one, two))
        sum_two = weighted(second_weights, (begin, one, two))
        moved = times(real, imag, [s - 0.5 * o for s, o in zip(sum_one, one)])
        turned = coupled(factor, sum_one)
        inner = [begin[k] + moved[k] + turned[k] for k in range(2)]
        node_one = [inside * f for f in times(*inverse, inner)]
        moved = times(real, imag, [s - 0.5 * o for s, o in zip(sum_two, two)])
        turned = coupled(
            factor, [sum_two[k] + 0.5 * (node_one[k] - one[k]) for k in range(2)]
        )
        inner = [node_one[k] + moved[k] + turned[k] for k in range(2)]
        node_two = times(*inverse, inner)
        own = slice(HALO, HALO + BLOCK)
        rows = rows_of(block)
        if not coarse:
            for k in range(2):
                nodes_out[0, k, rows, here] = node_one[k][own]
                nodes_out[1, k, rows, here] = node_two[k][own]
            return
        mean = weighted(whole_weights, (begin, node_one, node_two))
        moved = times(real, imag, [mean[k] - node_two[k] for k in range(2)])
        turned = coupled(factor, mean)
        offset = [moved[k] + turned[k] for k in range(2)]
        step_real, step_imag = 1.0 - real, -imag
        scale = 1.0 / (step_real * step_real + step_imag * step_imag)
        grown = (step_real * scale, -step_imag * scale)
        offset = times(*grown, offset)
        local = pl.ds(pl.multiple_of(block * BLOCK - coarse_start, BLOCK), BLOCK)
        inner_here = pl.ds(pl.multiple_of(column - low_column, LANES), LANES)
        for k in range(2):
            gain[k, local, inner_here] = grown[k][own]
            shift[k, local, inner_here] = offset[k][own]
            kept = node_one[k] - 0.5 * (begin[k] + node_two[k])
            nodes_out[0, k, rows, here] = kept[own]

        @pl.when(jnp.logical_not(has_prev))
        def _():
            for k in range(2):
                start_out[k, rows, here] = begin[k][own]

    def coarse_compute(step):
        block = block_of(step)
        halo_wait(block, 0)

        @pl.loop(0, CX // LANES)
        def _(index):
            strip_compute(block, pl.multiple_of(low_column + index * LANES, LANES), True)

    def relay(low, high):
        @pl.loop(low, high)
        def _(step):
            @pl.when(has_prev)
            def _():
                relay_copy(step).wait_recv()

            rows, local = relay_rows(step, 0), relay_rows(step, coarse_start)
            here = pl.ds(low_column, CX)
            begin = [start_out[k, rows, here] for k in range(2)]
            grown = times(gain[0, local, :], gain[1, local, :], begin)
            finish = [grown[k] + shift[k, local, :] for k in range(2)]
            for k in range(2):
                nodes_out[1, k, rows, here] = finish[k]

            @pl.when(has_next)
            def _():
                relay_copy(step).start()

            for k in range(2):
                nodes_out[0, k, rows, here] += 0.5 * (begin[k] + finish[k])

    never = blocks + 1
    turn = jnp.where(coarse_rank, jnp.minimum(TURN * tm, blocks), never)
    early = jnp.where(coarse_rank, jnp.minimum(EARLY * tm // 4, turn), blocks)

    @pl.when(coarse_rank)
    def _():
        greet()
        loaded(0, side_rows, CX)
        halo_exchange((0,), True)
        halo_exchange((0, 1), False)

        @pl.loop(0, coarse_blocks - 1)
        def _(step):
            coarse_compute(step)

    strips = columns // LANES // PARTS

    def step_at(index):
        later = jnp.where(index == blocks - 1, coarse_blocks - 1, index + 1)
        return jnp.where(coarse_rank & (index >= coarse_blocks - 1), later, index)

    @pl.loop(0, blocks + 1)
    def _(index):
        @pl.when(index == turn)
        def _():
            relay(0, PIECES * (coarse_blocks - 1))

        @pl.when(coarse_rank & (index == jnp.minimum(turn, coarse_blocks - 1)))
        def _():
            coarse_compute(coarse_blocks - 1)

        @pl.when(index == turn)
        def _():
            relay(PIECES * (coarse_blocks - 1), PIECES * coarse_blocks)

            @pl.loop(early, turn)
            def _(position):
                send(step_at(position), 0, PARTS)

        @pl.when(index < blocks)
        def _():
            step = step_at(index)
            block = block_of(step)
            in_coarse = coarse_rank & (step < coarse_blocks)

            @pl.when(coarse_rank & (index == 0))
            def _():
                loaded(1, side_rows, columns - CX)

            if slab > side_rows:

                @pl.when(coarse_rank & (index == coarse_blocks - 1))
                def _():
                    loaded(2, slab - side_rows, columns)

            for slot, height in ((PARTS, BLOCK), (PARTS + 1, rest_rows)):

                @pl.when(jnp.logical_not(coarse_rank) & (step == slot - PARTS + 1))
                def _(slot=slot, height=height):
                    loaded(slot, height, columns)

            @pl.when(jnp.logical_not(in_coarse))
            def _():
                halo_wait(block, 0)

            halo_wait(block, 1)

            @pl.loop(0, PARTS)
            def _(part):
                @pl.when(jnp.logical_not(coarse_rank) & (step == 0))
                def _():
                    loaded(part, first_rows, width)

                @pl.loop(0, strips)
                def _(strip):
                    low = (part * strips + strip) * LANES

                    @pl.when(
                        jnp.logical_not(in_coarse & (low >= low_column) & (low < low_column + CX))
                    )
                    def _():
                        strip_compute(block, pl.multiple_of(low, LANES), False)

                @pl.when(jnp.logical_not(coarse_rank) & (step == 0) & (part == 0))
                def _():
                    greet()
                    halo_exchange((0, 1), False)

                @pl.when((index < early) | (index >= turn))
                def _():
                    send(step, part, part + 1)

    def total(sem, height, extent):
        part = start_out.at[:, pl.ds(0, height), pl.ds(0, extent)]
        pltpu.make_async_copy(part, part, sem).wait()

    def all_bulk(sem, rows, lately):
        for short in (False, True):

            @pl.when(coarse_rank & (lately == short))
            def _(short=short):
                extent = rows - BLOCK if short else rows
                narrow = coarse_rows - BLOCK if short else coarse_rows
                total(sem, extent - narrow * CX // columns, columns)

        @pl.when(jnp.logical_not(coarse_rank))
        def _():
            total(sem, slab, columns)

    for side, exists in ((0, has_up), (1, has_down)):

        @pl.when(exists)
        def _(side=side):
            part = ext.at[:, :, pl.ds(0, HALO), :]
            pltpu.make_async_copy(part, part, halo_send.at[side]).wait()

    @pl.when(coarse_rank & has_next)
    def _():
        total(relay_send, coarse_rows, CX)

    @pl.when(jnp.logical_not(has_prev))
    def _():
        all_bulk(start_sem, slab, tm < 0)

    @pl.when(has_prev)
    def _():
        all_bulk(bulk_recv, coarse_rows, late(tm - 1))

    @pl.when(has_next)
    def _():
        all_bulk(bulk_send, coarse_rows, late(tm))


def place_of(slab, columns, coarse_rows):
    peers, rank = lax.axis_size("space"), lax.axis_index("space")
    low_row = slab * peers // 2 - CX // 2
    coarse_rank = (rank * slab < low_row + CX) & (rank * slab + slab > low_row)
    coarse_start = jnp.clip(low_row - rank * slab, 0, slab - coarse_rows)
    lower = rank < peers // 2
    other, edge = jnp.where(lower, 0, coarse_rows), jnp.where(lower, slab - BLOCK, 0)
    return coarse_rank, coarse_start, pl.multiple_of(other, HALO), pl.multiple_of(edge, HALO)


def sides(columns):
    width = columns // 2 - CX // 2
    return pl.ds(0, width), pl.ds(columns - width, width)


def write_out(coarse_rows, start, nodes, start_hbm, nodes_hbm, _, sem):
    slab, columns = start.shape[1:]
    coarse_rank, coarse_start, _, _ = place_of(slab, columns, coarse_rows)
    partly = coarse_rank & (lax.axis_index("tm") > 0)
    for k in range(2):
        pltpu.make_async_copy(nodes.at[k], nodes_hbm.at[k], sem.at[0]).start()

    def copy(top, height, act):
        here = (slice(None), pl.ds(pl.multiple_of(top, HALO), height), slice(None))
        act(pltpu.make_async_copy(start.at[here], start_hbm.at[here], sem.at[1]))

    for act in (lambda c: c.start(), lambda c: c.wait()):

        @pl.when(partly)
        def _(act=act):
            copy(coarse_start, coarse_rows, act)

        @pl.when(jnp.logical_not(partly))
        def _(act=act):
            copy(0, slab, act)

    pltpu.make_async_copy(nodes, nodes_hbm, sem.at[0]).wait()


def send_rest(coarse_rows, nodes, _, rest_out, send_sem, recv_sem):
    slab, columns = nodes.shape[2:]
    coarse_rank, _, other, edge = place_of(slab, columns, coarse_rows)
    tm, count = lax.axis_index("tm"), lax.axis_size("tm")
    has_prev, has_next = coarse_rank & (tm > 0), coarse_rank & (tm < count - 1)
    others = slab - coarse_rows
    barrier = pltpu.get_barrier_semaphore()

    def send(source, target):
        pltpu.make_async_remote_copy(
            source,
            target,
            send_sem,
            recv_sem,
            device_id={"tm": tm + 1},
            device_id_type=MESH,
        ).start()

    def total(sem, lately):
        for short in (False, True):

            @pl.when(lately == short)
            def _(short=short):
                rows = others + (BLOCK - BLOCK * CX // columns if short else 0)
                part = rest_out.at[:, pl.ds(0, rows), :]
                pltpu.make_async_copy(part, part, sem).wait()

    @pl.when(has_prev)
    def _():
        pl.semaphore_signal(barrier, inc=1, device_id={"tm": tm - 1}, device_id_type=MESH)

    @pl.when(has_next)
    def _():
        pl.semaphore_wait(barrier, 1)

        @pl.when(late(tm))
        def _():
            for side in sides(columns):
                send(
                    nodes.at[1, :, pl.ds(edge, BLOCK), side],
                    rest_out.at[:, pl.ds(others, BLOCK), side],
                )

        send(nodes.at[1, :, pl.ds(other, others), :], rest_out.at[:, pl.ds(0, others), :])

    @pl.when(has_prev)
    def _():
        total(recv_sem, late(tm - 1))

    @pl.when(has_next)
    def _():
        total(send_sem, late(tm))


def write_rest(coarse_rows, rest, _, start_hbm, sem):
    slab, columns = start_hbm.shape[1:]
    coarse_rank, _, other, edge = place_of(slab, columns, coarse_rows)
    tm, others = lax.axis_index("tm"), slab - coarse_rows

    @pl.when(coarse_rank & (tm > 0))
    def _():
        whole = pltpu.make_async_copy(
            rest.at[:, pl.ds(0, others), :], start_hbm.at[:, pl.ds(other, others), :], sem.at[0]
        )
        strips = [
            pltpu.make_async_copy(
                rest.at[:, pl.ds(others, BLOCK), side],
                start_hbm.at[:, pl.ds(edge, BLOCK), side],
                sem.at[1 + index],
            )
            for index, side in enumerate(sides(columns))
        ]
        whole.start()
        for act in (lambda c: c.start(), lambda c: c.wait()):

            @pl.when(late(tm - 1))
            def _(act=act):
                for strip in strips:
                    act(strip)

        whole.wait()


def body(start_values, node_values):
    slab, columns = start_values.shape[2:]
    peers = lax.axis_size("space")
    coarse_rows = min(slab, max(CX // 2, CX // peers))
    coarse_blocks = coarse_rows // BLOCK
    hbm = pl.BlockSpec(memory_space=pltpu.HBM)
    vmem = pl.BlockSpec(memory_space=pltpu.VMEM)
    anywhere = pl.BlockSpec(memory_space=pl.ANY)
    dma = pltpu.SemaphoreType.DMA
    start, nodes = pl.pallas_call(
        kernel,
        out_shape=(
            OUT((2, slab, columns), jnp.float32),
            OUT((2, 2, slab, columns), jnp.float32),
        ),
        in_specs=[hbm, hbm],
        out_specs=(vmem, vmem),
        scratch_shapes=[
            pltpu.VMEM((3, 2, slab + 2 * HALO, columns), jnp.float32),
            pltpu.VMEM((2, coarse_rows, CX), jnp.float32),
            pltpu.VMEM((2, coarse_rows, CX), jnp.float32),
            dma((PARTS + 2,)),
            dma,
            dma((2,)),
            dma((2, 2)),
            dma,
            dma,
            dma,
            dma((PIECES * coarse_blocks,)),
        ],
        compiler_params=pltpu.CompilerParams(
            collective_id=0, has_side_effects=True, vmem_limit_bytes=56 * 1024 * 1024
        ),
    )(start_values[0], node_values[0])
    start_hbm, nodes_hbm, written = pl.pallas_call(
        functools.partial(write_out, coarse_rows),
        out_shape=(
            jax.ShapeDtypeStruct(start.shape, jnp.float32),
            jax.ShapeDtypeStruct(nodes.shape, jnp.float32),
            OUT((8, LANES), jnp.float32),
        ),
        in_specs=[anywhere, anywhere],
        out_specs=(hbm, hbm, vmem),
        scratch_shapes=[dma((2,))],
        compiler_params=pltpu.CompilerParams(vmem_limit_bytes=2 * 1024 * 1024),
    )(start, nodes)
    if slab > coarse_rows:
        rest = pl.pallas_call(
            functools.partial(send_rest, coarse_rows),
            out_shape=OUT((2, slab - coarse_rows + BLOCK, columns), jnp.float32),
            in_specs=[anywhere, anywhere],
            out_specs=vmem,
            scratch_shapes=[dma, dma],
            compiler_params=pltpu.CompilerParams(
                collective_id=1, has_side_effects=True, vmem_limit_bytes=4 * 1024 * 1024
            ),
        )(nodes, written)
        start_hbm = pl.pallas_call(
            functools.partial(write_rest, coarse_rows),
            out_shape=jax.ShapeDtypeStruct(start.shape, jnp.float32),
            in_specs=[anywhere, hbm],
            out_specs=hbm,
            scratch_shapes=[dma((3,))],
            input_output_aliases={1: 0},
            compiler_params=pltpu.CompilerParams(vmem_limit_bytes=2 * 1024 * 1024),
        )(rest, start_hbm)
    return (start_hbm[None], nodes_hbm[None])


OUT = pltpu.VMEM


def solution(mesh):
    in_specs = (P("tm", None, "space", None), P("tm", None, None, "space", None))
    out_specs = (P("tm", None, "space", None), P("tm", None, None, "space", None))
    return jax.shard_map(body, mesh=mesh, in_specs=in_specs, out_specs=out_specs, check_vma=False)
```

```python
import functools

import jax
import jax.numpy as jnp
from jax import lax
from jax.experimental import pallas as pl
from jax.experimental.pallas import tpu as pltpu
from jax.sharding import PartitionSpec as P

CX = 256

diffusion = 1.5
drift = 0.8
shear = 0.6
first_weights = (5.0 / 24.0, 1.0 / 3.0, -1.0 / 24.0)
second_weights = (-1.0 / 24.0, 1.0 / 3.0, 5.0 / 24.0)
whole_weights = (1.0 / 6.0, 2.0 / 3.0, 1.0 / 6.0)

MESH = pl.DeviceIdType.MESH
HALO = 8
BLOCK = 32
PARTS = 4
LATE = 4
DETOURS = 3
DETOUR_ROWS = 16
TURN = 2
EARLY = 3
PIECES = 4
LANES = 128


def weighted(weights, fields):
    return [sum(w * f[k] for w, f in zip(weights, fields)) for k in range(2)]


def times(real, imag, field):
    return [real * field[0] - imag * field[1], real * field[1] + imag * field[0]]


def coupled(factor, field):
    length = field[0].shape[0]
    sums = [pltpu.roll(f, 1, 0) + pltpu.roll(f, length - 1, 0) for f in field]
    return [factor * sums[1], -factor * sums[0]]


def late(tm):
    return tm >= LATE


def kernel(
    begin_hbm,
    nodes_hbm,
    start_out,
    nodes_out,
    ext,
    gain,
    shift,
    load_sem,
    start_sem,
    halo_send,
    halo_recv,
    bulk_send,
    bulk_recv,
    relay_send,
    relay_recv,
    transit,
    transit_recv,
    forward_send,
    below,
    above,
):
    slab, columns = begin_hbm.shape[1:]
    peers, count = lax.axis_size("space"), lax.axis_size("tm")
    rows_total = slab * peers
    tm, rank = lax.axis_index("tm"), lax.axis_index("space")
    has_prev, has_next = tm > 0, tm < count - 1
    has_up, has_down = rank > 0, rank < peers - 1
    blocks = slab // BLOCK
    low_row = rows_total // 2 - CX // 2
    low_column = columns // 2 - CX // 2
    coarse_rows = gain.shape[1]
    coarse_blocks = coarse_rows // BLOCK
    inward = min(HALO, slab - coarse_rows)
    coarse_rank = (rank * slab < low_row + CX) & (rank * slab + slab > low_row)
    lower = rank < peers // 2
    coarse_start = jnp.clip(low_row - rank * slab, 0, slab - coarse_rows)
    coarse_block = coarse_start // BLOCK
    first = jnp.where(
        coarse_rank,
        jnp.where(lower, coarse_block, blocks - coarse_block - coarse_blocks),
        0,
    )

    def block_of(step):
        index = jnp.where(step < blocks - first, first + step, blocks - 1 - step)
        return jnp.where(lower, index, blocks - 1 - index)

    def rows_of(block):
        return pl.ds(pl.multiple_of(block * BLOCK, BLOCK), BLOCK)

    def load(slot, top, height, left, width):
        top, left = pl.multiple_of(top, HALO), pl.multiple_of(left, LANES)
        source, here = pl.ds(top, height), pl.ds(left, width)
        target = pl.ds(pl.multiple_of(top + HALO, HALO), height)
        pltpu.make_async_copy(
            begin_hbm.at[:, source, here], ext.at[0, :, target, here], load_sem.at[slot]
        ).start()
        pltpu.make_async_copy(
            nodes_hbm.at[:, :, source, here], ext.at[1:3, :, target, here], load_sem.at[slot]
        ).start()

    def loaded(slot, height, width):
        part = ext.at[:, :, pl.ds(0, height), pl.ds(0, width)]
        pltpu.make_async_copy(part, part, load_sem.at[slot]).wait()

    side_rows = coarse_rows + inward
    head_rows = BLOCK + 2 * HALO if inward else 0
    first_rows, width = BLOCK + HALO, columns // PARTS
    rest_rows = slab - first_rows - BLOCK

    def load_coarse_rank():
        top = jnp.where(lower, slab - side_rows, 0)
        if head_rows:
            load(3, jnp.where(lower, top, side_rows - head_rows), head_rows, 0, low_column)
        load(0, top, side_rows, low_column, CX)
        rest = jnp.where(lower, top + head_rows, 0)
        load(1, rest, side_rows - head_rows, 0, low_column)
        load(1, top, side_rows, low_column + CX, low_column)
        if slab > side_rows:
            load(2, jnp.where(lower, 0, side_rows), slab - side_rows, 0, columns)

    def load_other_rank():
        @pl.loop(0, PARTS)
        def _(part):
            load(part, jnp.where(lower, 0, slab - first_rows), first_rows, part * width, width)

        load(PARTS, jnp.where(lower, first_rows, rest_rows), BLOCK, 0, columns)
        load(PARTS + 1, jnp.where(lower, slab - rest_rows, 0), rest_rows, 0, columns)

    def begin_copies():
        def copy(top, height, left, width):
            place = (slice(None), pl.ds(pl.multiple_of(top, HALO), height), pl.ds(left, width))
            pltpu.make_async_copy(begin_hbm.at[place], start_out.at[place], start_sem).start()

        @pl.when(coarse_rank)
        def _():
            copy(coarse_start, coarse_rows, 0, low_column)
            copy(coarse_start, coarse_rows, low_column + CX, low_column)
            if slab > coarse_rows:
                top = jnp.where(lower, 0, coarse_rows)
                copy(top, slab - coarse_rows, 0, columns)

        @pl.when(jnp.logical_not(coarse_rank))
        def _():
            copy(0, slab, 0, columns)

    def halo_start(side, slot, sources):
        target = pl.ds(slab + HALO if side == 0 else 0, HALO)
        for left, extent in (
            ((low_column, CX),)
            if slot == 0
            else ((0, low_column), (low_column + CX, low_column))
        ):
            here = pl.ds(left, extent)
            for source, place in zip(sources, (0, slice(1, 3))):
                pltpu.make_async_remote_copy(
                    source.at[..., here],
                    ext.at[place, :, target, here],
                    halo_send.at[side],
                    halo_recv.at[side, slot],
                    device_id={"space": rank - 1 if side == 0 else rank + 1},
                    device_id_type=MESH,
                ).start()

    def halo_exchange(slots, loaded_edge):
        for side, exists in ((0, has_up), (1, has_down)):
            edge = pl.ds(0 if side == 0 else slab - HALO, HALO)
            held = pl.ds(HALO if side == 0 else slab, HALO)
            inner = coarse_rank & (lower if side == 1 else jnp.logical_not(lower))
            for slot in slots:
                fit = inner if loaded_edge else jnp.logical_not(inner)
                fit = exists if slot == 1 else exists & fit
                sources = (
                    (ext.at[0, :, held, :], ext.at[1:3, :, held, :])
                    if loaded_edge
                    else (begin_hbm.at[:, edge, :], nodes_hbm.at[:, :, edge, :])
                )

                @pl.when(fit)
                def _(side=side, slot=slot, sources=sources):
                    halo_start(side, slot, sources)

    def halo_wait(block, slot):
        for side, edge in ((0, (block == blocks - 1) & has_down), (1, (block == 0) & has_up)):

            @pl.when(edge)
            def _(side=side):
                part = ext.at[:, :, pl.ds(0, HALO), pl.ds(0, CX if slot == 0 else columns - CX)]
                pltpu.make_async_copy(part, part, halo_recv.at[side, slot]).wait()

    following = {"tm": tm + 1}

    def relay_rows(step, origin):
        top = block_of(step // PIECES) * BLOCK + step % PIECES * (BLOCK // PIECES) - origin
        return pl.ds(pl.multiple_of(top, HALO), BLOCK // PIECES)

    def relay_copy(step):
        place = (slice(None), relay_rows(step, 0), pl.ds(low_column, CX))
        return pltpu.make_async_remote_copy(
            nodes_out.at[(1,) + place],
            start_out.at[place],
            relay_send,
            relay_recv.at[step],
            device_id=following,
            device_id_type=MESH,
        )

    detours = min(DETOURS, (count - 1) // 2)
    taking_part = jnp.logical_not(coarse_rank) & (tm <= 2 * detours)
    detoured = taking_part & (tm % 2 == 1)
    detour_rows = transit.shape[2]

    def detour_place():
        top = pl.multiple_of(block_of(blocks - 1) * BLOCK, BLOCK)
        return slice(None), pl.ds(top, detour_rows), slice(None)

    def detour():
        for sign, met, ends in ((1, below, (tm == 0, tm == 2 * detours)), (-1, above, (tm == 2 * detours, tm == 0))):

            @pl.when(jnp.logical_not(ends[0]))
            def _(met=met):
                pl.semaphore_wait(met, 1)

            @pl.when(jnp.logical_not(ends[1]))
            def _(met=met, sign=sign):
                pl.semaphore_signal(
                    met, inc=1, device_id={"tm": tm + sign}, device_id_type=MESH
                )

        slot = tm // 2
        place = detour_place()

        @pl.when(detoured)
        def _():
            pltpu.make_async_remote_copy(
                nodes_out.at[(1,) + place],
                transit.at[slot],
                bulk_send,
                transit_recv.at[slot],
                device_id={"tm": tm - tm},
                device_id_type=MESH,
            ).start()

        @pl.when(tm == 0)
        def _():
            for slot in range(detours):
                pltpu.make_async_copy(transit.at[slot], transit.at[slot], transit_recv.at[slot]).wait()
                pltpu.make_async_remote_copy(
                    transit.at[slot],
                    start_out.at[place],
                    forward_send,
                    bulk_recv,
                    device_id={"tm": tm + 2 * slot + 2},
                    device_id_type=MESH,
                ).start()
            pltpu.make_async_copy(transit, transit, forward_send).wait()

    def bulk_copy(block, left, width, top=0):
        rows = pl.ds(pl.multiple_of(block * BLOCK + top, HALO), BLOCK - top)
        place = (slice(None), rows, pl.ds(pl.multiple_of(left, LANES), width))
        pltpu.make_async_remote_copy(
            nodes_out.at[(1,) + place],
            start_out.at[place],
            bulk_send,
            bulk_recv,
            device_id=following,
            device_id_type=MESH,
        ).start()

    def bulk(unit):
        step, part = unit // PARTS, unit % PARTS
        block = block_of(step)
        strip = coarse_rank & (step < coarse_blocks)
        sent = (step == 0) & (part == PARTS - 2) & (head_rows > 0)

        def copy(left, width):
            bulk_copy(block, left, width)

        @pl.when(strip & (part >= PARTS - 2) & jnp.logical_not(sent))
        def _():
            copy((part - (PARTS - 2)) * (low_column + CX), low_column)

        quick = (step == 0) & jnp.logical_not(coarse_rank)

        @pl.when(quick)
        def _():
            copy(part * (columns // PARTS), columns // PARTS)

        whole = jnp.logical_not(quick | coarse_rank) & (part == PARTS - 1)
        short = detoured & (step == blocks - 1)

        @pl.when(whole & jnp.logical_not(short))
        def _():
            copy(0, columns)

        @pl.when(whole & short)
        def _():
            bulk_copy(block, 0, columns, detour_rows)

    def send(step, low, high):
        held = coarse_rank & late(tm) & (step == coarse_blocks - 1)

        @pl.when(has_next & jnp.logical_not(held))
        def _():
            @pl.loop(low, high)
            def _(part):
                bulk(PARTS * step + part)

    barrier = pltpu.get_barrier_semaphore()
    for there, exists in (
        ({"space": rank - 1}, has_up),
        ({"space": rank + 1}, has_down),
        ({"tm": tm - 1}, has_prev),
        ({"tm": tm + 1}, has_next),
    ):

        @pl.when(exists)
        def _(there=there):
            pl.semaphore_signal(barrier, inc=1, device_id=there, device_id_type=MESH)

    pl.when(coarse_rank)(load_coarse_rank)
    pl.when(jnp.logical_not(coarse_rank))(load_other_rank)

    for side, exists in ((0, has_up), (1, has_down)):

        @pl.when(jnp.logical_not(exists))
        def _(side=side):
            edge = pl.ds(0 if side == 0 else slab + HALO, HALO)
            ext[:, :, edge, :] = jnp.zeros((3, 2, HALO, columns), jnp.float32)

    pl.when(jnp.logical_not(has_prev))(begin_copies)

    def greet():
        friends = sum(jnp.where(e, 1, 0) for e in (has_up, has_down, has_prev, has_next))
        pl.semaphore_wait(barrier, friends)
    def strip_compute(block, column, coarse):
        length = BLOCK + 2 * HALO
        span = pl.ds(pl.multiple_of(block * BLOCK, BLOCK), length)
        here = pl.ds(column, LANES)
        begin, one, two = [[ext[f, k, span, here] for k in range(2)] for f in range(3)]
        row = lax.broadcasted_iota(jnp.int32, (length, LANES), 0)
        row = row + (rank * slab + block * BLOCK - HALO)
        along = (row - rows_total // 2).astype(jnp.float32) / (rows_total // 2)
        place = lax.broadcasted_iota(jnp.int32, (1, LANES), 1) + column
        across = (place - columns // 2).astype(jnp.float32) / (columns // 2)
        inside = jnp.where((row >= 0) & (row < rows_total), 1.0, 0.0).astype(jnp.float32)
        real = -diffusion * (along * along + across * across)
        imag = -drift * across
        factor = shear * across
        half_real, half_imag = 1.0 - 0.5 * real, -0.5 * imag
        scale = 1.0 / (half_real * half_real + half_imag * half_imag)
        inverse = (half_real * scale, -half_imag * scale)
        sum_one = weighted(first_weights, (begin, one, two))
        sum_two = weighted(second_weights, (begin, one, two))
        moved = times(real, imag, [s - 0.5 * o for s, o in zip(sum_one, one)])
        turned = coupled(factor, sum_one)
        inner = [begin[k] + moved[k] + turned[k] for k in range(2)]
        node_one = [inside * f for f in times(*inverse, inner)]
        moved = times(real, imag, [s - 0.5 * o for s, o in zip(sum_two, two)])
        turned = coupled(
            factor, [sum_two[k] + 0.5 * (node_one[k] - one[k]) for k in range(2)]
        )
        inner = [node_one[k] + moved[k] + turned[k] for k in range(2)]
        node_two = times(*inverse, inner)
        own = slice(HALO, HALO + BLOCK)
        rows = rows_of(block)
        if not coarse:
            for k in range(2):
                nodes_out[0, k, rows, here] = node_one[k][own]
                nodes_out[1, k, rows, here] = node_two[k][own]
            return
        mean = weighted(whole_weights, (begin, node_one, node_two))
        moved = times(real, imag, [mean[k] - node_two[k] for k in range(2)])
        turned = coupled(factor, mean)
        offset = [moved[k] + turned[k] for k in range(2)]
        step_real, step_imag = 1.0 - real, -imag
        scale = 1.0 / (step_real * step_real + step_imag * step_imag)
        grown = (step_real * scale, -step_imag * scale)
        offset = times(*grown, offset)
        local = pl.ds(pl.multiple_of(block * BLOCK - coarse_start, BLOCK), BLOCK)
        inner_here = pl.ds(pl.multiple_of(column - low_column, LANES), LANES)
        for k in range(2):
            gain[k, local, inner_here] = grown[k][own]
            shift[k, local, inner_here] = offset[k][own]
            kept = node_one[k] - 0.5 * (begin[k] + node_two[k])
            nodes_out[0, k, rows, here] = kept[own]

        @pl.when(jnp.logical_not(has_prev))
        def _():
            for k in range(2):
                start_out[k, rows, here] = begin[k][own]

    def coarse_compute(step):
        block = block_of(step)
        halo_wait(block, 0)

        @pl.loop(0, CX // LANES)
        def _(index):
            strip_compute(block, pl.multiple_of(low_column + index * LANES, LANES), True)

    def relay(low, high):
        @pl.loop(low, high)
        def _(step):
            @pl.when(has_prev)
            def _():
                relay_copy(step).wait_recv()

            rows, local = relay_rows(step, 0), relay_rows(step, coarse_start)
            here = pl.ds(low_column, CX)
            begin = [start_out[k, rows, here] for k in range(2)]
            grown = times(gain[0, local, :], gain[1, local, :], begin)
            finish = [grown[k] + shift[k, local, :] for k in range(2)]
            for k in range(2):
                nodes_out[1, k, rows, here] = finish[k]

            @pl.when(has_next)
            def _():
                relay_copy(step).start()

            for k in range(2):
                nodes_out[0, k, rows, here] += 0.5 * (begin[k] + finish[k])

    never = blocks + 1
    turn = jnp.where(coarse_rank, jnp.minimum(TURN * tm, blocks), never)
    early = jnp.where(coarse_rank, jnp.minimum(EARLY * tm // 4, turn), blocks)

    @pl.when(coarse_rank)
    def _():
        if head_rows:
            loaded(3, head_rows, low_column)

            @pl.loop(0, low_column // LANES)
            def _(strip):
                left = pl.multiple_of(strip * LANES, LANES)
                strip_compute(block_of(0), left, False)
                pl.when(strip == 0)(greet)

                @pl.when(has_next)
                def _():
                    bulk_copy(block_of(0), left, LANES)
        else:
            greet()
        loaded(0, side_rows, CX)
        halo_exchange((0,), True)
        halo_exchange((0, 1), False)

        @pl.loop(0, coarse_blocks - 1)
        def _(step):
            coarse_compute(step)

    strips = columns // LANES // PARTS

    def step_at(index):
        later = jnp.where(index == blocks - 1, coarse_blocks - 1, index + 1)
        return jnp.where(coarse_rank & (index >= coarse_blocks - 1), later, index)

    @pl.loop(0, blocks + 1)
    def _(index):
        @pl.when(index == turn)
        def _():
            relay(0, PIECES * (coarse_blocks - 1))

        @pl.when(coarse_rank & (index == jnp.minimum(turn, coarse_blocks - 1)))
        def _():
            coarse_compute(coarse_blocks - 1)

        @pl.when(index == turn)
        def _():
            relay(PIECES * (coarse_blocks - 1), PIECES * coarse_blocks)

            @pl.loop(early, turn)
            def _(position):
                send(step_at(position), 0, PARTS)

        @pl.when(index < blocks)
        def _():
            step = step_at(index)
            block = block_of(step)
            in_coarse = coarse_rank & (step < coarse_blocks)

            @pl.when(coarse_rank & (index == 0))
            def _():
                if head_rows:
                    loaded(1, 2 * side_rows - head_rows, low_column)
                else:
                    loaded(1, side_rows, columns - CX)

            if slab > side_rows:

                @pl.when(coarse_rank & (index == coarse_blocks - 1))
                def _():
                    loaded(2, slab - side_rows, columns)

            for slot, height in ((PARTS, BLOCK), (PARTS + 1, rest_rows)):

                @pl.when(jnp.logical_not(coarse_rank) & (step == slot - PARTS + 1))
                def _(slot=slot, height=height):
                    loaded(slot, height, columns)

            @pl.when(jnp.logical_not(in_coarse))
            def _():
                halo_wait(block, 0)

            halo_wait(block, 1)

            @pl.loop(0, PARTS)
            def _(part):
                @pl.when(jnp.logical_not(coarse_rank) & (step == 0))
                def _():
                    loaded(part, first_rows, width)

                @pl.loop(0, strips)
                def _(strip):
                    low = (part * strips + strip) * LANES

                    begun = in_coarse & (step == 0) & (low < low_column) & (head_rows > 0)
                    kept = in_coarse & (low >= low_column) & (low < low_column + CX)

                    @pl.when(jnp.logical_not(begun | kept))
                    def _():
                        strip_compute(block, pl.multiple_of(low, LANES), False)

                @pl.when(jnp.logical_not(coarse_rank) & (step == 0) & (part == 0))
                def _():
                    greet()
                    halo_exchange((0, 1), False)

                @pl.when((index < early) | (index >= turn))
                def _():
                    send(step, part, part + 1)

    if detours:
        pl.when(taking_part)(detour)

    def total(sem, height, extent):
        part = start_out.at[:, pl.ds(0, height), pl.ds(0, extent)]
        pltpu.make_async_copy(part, part, sem).wait()

    def all_bulk(sem, rows, lately):
        for short in (False, True):

            @pl.when(coarse_rank & (lately == short))
            def _(short=short):
                extent = rows - BLOCK if short else rows
                narrow = coarse_rows - BLOCK if short else coarse_rows
                total(sem, extent - narrow * CX // columns, columns)

        @pl.when(jnp.logical_not(coarse_rank))
        def _():
            total(sem, slab, columns)

    for side, exists in ((0, has_up), (1, has_down)):

        @pl.when(exists)
        def _(side=side):
            part = ext.at[:, :, pl.ds(0, HALO), :]
            pltpu.make_async_copy(part, part, halo_send.at[side]).wait()

    @pl.when(coarse_rank & has_next)
    def _():
        total(relay_send, coarse_rows, CX)

    @pl.when(jnp.logical_not(has_prev))
    def _():
        all_bulk(start_sem, slab, tm < 0)

    @pl.when(has_prev)
    def _():
        all_bulk(bulk_recv, coarse_rows, late(tm - 1))

    @pl.when(has_next)
    def _():
        all_bulk(bulk_send, coarse_rows, late(tm))


def place_of(slab, columns, coarse_rows):
    peers, rank = lax.axis_size("space"), lax.axis_index("space")
    low_row = slab * peers // 2 - CX // 2
    coarse_rank = (rank * slab < low_row + CX) & (rank * slab + slab > low_row)
    coarse_start = jnp.clip(low_row - rank * slab, 0, slab - coarse_rows)
    lower = rank < peers // 2
    other, edge = jnp.where(lower, 0, coarse_rows), jnp.where(lower, slab - BLOCK, 0)
    return coarse_rank, coarse_start, pl.multiple_of(other, HALO), pl.multiple_of(edge, HALO)


def sides(columns):
    width = columns // 2 - CX // 2
    return pl.ds(0, width), pl.ds(columns - width, width)


def write_out(coarse_rows, start, nodes, start_hbm, nodes_hbm, _, sem):
    slab, columns = start.shape[1:]
    coarse_rank, coarse_start, _, _ = place_of(slab, columns, coarse_rows)
    partly = coarse_rank & (lax.axis_index("tm") > 0)
    for k in range(2):
        pltpu.make_async_copy(nodes.at[k], nodes_hbm.at[k], sem.at[0]).start()

    def copy(top, height, act):
        here = (slice(None), pl.ds(pl.multiple_of(top, HALO), height), slice(None))
        act(pltpu.make_async_copy(start.at[here], start_hbm.at[here], sem.at[1]))

    for act in (lambda c: c.start(), lambda c: c.wait()):

        @pl.when(partly)
        def _(act=act):
            copy(coarse_start, coarse_rows, act)

        @pl.when(jnp.logical_not(partly))
        def _(act=act):
            copy(0, slab, act)

    pltpu.make_async_copy(nodes, nodes_hbm, sem.at[0]).wait()


def send_rest(coarse_rows, nodes, _, rest_out, send_sem, recv_sem):
    slab, columns = nodes.shape[2:]
    coarse_rank, _, other, edge = place_of(slab, columns, coarse_rows)
    tm, count = lax.axis_index("tm"), lax.axis_size("tm")
    has_prev, has_next = coarse_rank & (tm > 0), coarse_rank & (tm < count - 1)
    others = slab - coarse_rows
    barrier = pltpu.get_barrier_semaphore()

    def send(source, target):
        pltpu.make_async_remote_copy(
            source,
            target,
            send_sem,
            recv_sem,
            device_id={"tm": tm + 1},
            device_id_type=MESH,
        ).start()

    def total(sem, lately):
        for short in (False, True):

            @pl.when(lately == short)
            def _(short=short):
                rows = others + (BLOCK - BLOCK * CX // columns if short else 0)
                part = rest_out.at[:, pl.ds(0, rows), :]
                pltpu.make_async_copy(part, part, sem).wait()

    @pl.when(has_prev)
    def _():
        pl.semaphore_signal(barrier, inc=1, device_id={"tm": tm - 1}, device_id_type=MESH)

    @pl.when(has_next)
    def _():
        pl.semaphore_wait(barrier, 1)

        @pl.when(late(tm))
        def _():
            for side in sides(columns):
                send(
                    nodes.at[1, :, pl.ds(edge, BLOCK), side],
                    rest_out.at[:, pl.ds(others, BLOCK), side],
                )

        send(nodes.at[1, :, pl.ds(other, others), :], rest_out.at[:, pl.ds(0, others), :])

    @pl.when(has_prev)
    def _():
        total(recv_sem, late(tm - 1))

    @pl.when(has_next)
    def _():
        total(send_sem, late(tm))


def write_rest(coarse_rows, rest, _, start_hbm, sem):
    slab, columns = start_hbm.shape[1:]
    coarse_rank, _, other, edge = place_of(slab, columns, coarse_rows)
    tm, others = lax.axis_index("tm"), slab - coarse_rows

    @pl.when(coarse_rank & (tm > 0))
    def _():
        whole = pltpu.make_async_copy(
            rest.at[:, pl.ds(0, others), :], start_hbm.at[:, pl.ds(other, others), :], sem.at[0]
        )
        strips = [
            pltpu.make_async_copy(
                rest.at[:, pl.ds(others, BLOCK), side],
                start_hbm.at[:, pl.ds(edge, BLOCK), side],
                sem.at[1 + index],
            )
            for index, side in enumerate(sides(columns))
        ]
        whole.start()
        for act in (lambda c: c.start(), lambda c: c.wait()):

            @pl.when(late(tm - 1))
            def _(act=act):
                for strip in strips:
                    act(strip)

        whole.wait()


def body(start_values, node_values):
    slab, columns = start_values.shape[2:]
    peers = lax.axis_size("space")
    coarse_rows = min(slab, max(CX // 2, CX // peers))
    coarse_blocks = coarse_rows // BLOCK
    slots = max(1, min(DETOURS, (lax.axis_size("tm") - 1) // 2))
    hbm = pl.BlockSpec(memory_space=pltpu.HBM)
    vmem = pl.BlockSpec(memory_space=pltpu.VMEM)
    anywhere = pl.BlockSpec(memory_space=pl.ANY)
    dma = pltpu.SemaphoreType.DMA
    start, nodes = pl.pallas_call(
        kernel,
        out_shape=(
            OUT((2, slab, columns), jnp.float32),
            OUT((2, 2, slab, columns), jnp.float32),
        ),
        in_specs=[hbm, hbm],
        out_specs=(vmem, vmem),
        scratch_shapes=[
            pltpu.VMEM((3, 2, slab + 2 * HALO, columns), jnp.float32),
            pltpu.VMEM((2, coarse_rows, CX), jnp.float32),
            pltpu.VMEM((2, coarse_rows, CX), jnp.float32),
            dma((PARTS + 2,)),
            dma,
            dma((2,)),
            dma((2, 2)),
            dma,
            dma,
            dma,
            dma((PIECES * coarse_blocks,)),
            pltpu.VMEM((slots, 2, DETOUR_ROWS, columns), jnp.float32),
            dma((slots,)),
            dma,
            pltpu.SemaphoreType.REGULAR,
            pltpu.SemaphoreType.REGULAR,
        ],
        compiler_params=pltpu.CompilerParams(
            collective_id=0, has_side_effects=True, vmem_limit_bytes=56 * 1024 * 1024
        ),
    )(start_values[0], node_values[0])
    start_hbm, nodes_hbm, written = pl.pallas_call(
        functools.partial(write_out, coarse_rows),
        out_shape=(
            jax.ShapeDtypeStruct(start.shape, jnp.float32),
            jax.ShapeDtypeStruct(nodes.shape, jnp.float32),
            OUT((8, LANES), jnp.float32),
        ),
        in_specs=[anywhere, anywhere],
        out_specs=(hbm, hbm, vmem),
        scratch_shapes=[dma((2,))],
        compiler_params=pltpu.CompilerParams(vmem_limit_bytes=2 * 1024 * 1024),
    )(start, nodes)
    if slab > coarse_rows:
        rest = pl.pallas_call(
            functools.partial(send_rest, coarse_rows),
            out_shape=OUT((2, slab - coarse_rows + BLOCK, columns), jnp.float32),
            in_specs=[anywhere, anywhere],
            out_specs=vmem,
            scratch_shapes=[dma, dma],
            compiler_params=pltpu.CompilerParams(
                collective_id=1, has_side_effects=True, vmem_limit_bytes=4 * 1024 * 1024
            ),
        )(nodes, written)
        start_hbm = pl.pallas_call(
            functools.partial(write_rest, coarse_rows),
            out_shape=jax.ShapeDtypeStruct(start.shape, jnp.float32),
            in_specs=[anywhere, hbm],
            out_specs=hbm,
            scratch_shapes=[dma((3,))],
            input_output_aliases={1: 0},
            compiler_params=pltpu.CompilerParams(vmem_limit_bytes=2 * 1024 * 1024),
        )(rest, start_hbm)
    return (start_hbm[None], nodes_hbm[None])


OUT = pltpu.VMEM


def solution(mesh):
    in_specs = (P("tm", None, "space", None), P("tm", None, None, "space", None))
    out_specs = (P("tm", None, "space", None), P("tm", None, None, "space", None))
    return jax.shard_map(body, mesh=mesh, in_specs=in_specs, out_specs=out_specs, check_vma=False)
```

```python
import functools

import jax
import jax.numpy as jnp
from jax import lax
from jax.experimental import pallas as pl
from jax.experimental.pallas import tpu as pltpu
from jax.sharding import PartitionSpec as P

CX = 256

diffusion = 1.5
drift = 0.8
shear = 0.6
first_weights = (5.0 / 24.0, 1.0 / 3.0, -1.0 / 24.0)
second_weights = (-1.0 / 24.0, 1.0 / 3.0, 5.0 / 24.0)
whole_weights = (1.0 / 6.0, 2.0 / 3.0, 1.0 / 6.0)

MESH = pl.DeviceIdType.MESH
HALO = 8
BLOCK = 32
PARTS = 4
DEFER = 5
WRITES = 2
DETOURS = 3
DETOUR_ROWS = 16
TURN = 2
EARLY = 3
PIECES = 4
LANES = 128


def weighted(weights, fields):
    return [sum(w * f[k] for w, f in zip(weights, fields)) for k in range(2)]


def times(real, imag, field):
    return [real * field[0] - imag * field[1], real * field[1] + imag * field[0]]


def coupled(factor, field):
    length = field[0].shape[0]
    sums = [pltpu.roll(f, 1, 0) + pltpu.roll(f, length - 1, 0) for f in field]
    return [factor * sums[1], -factor * sums[0]]


def defers(tm, slab, coarse_rows):
    return tm < DEFER if slab > coarse_rows else tm < 0


def kernel(
    begin_hbm,
    nodes_hbm,
    start_out,
    nodes_out,
    ext,
    gain,
    shift,
    load_sem,
    halo_send,
    halo_recv,
    bulk_send,
    bulk_recv,
    relay_send,
    relay_recv,
    transit,
    transit_recv,
    below,
    above,
    answer,
):
    slab, columns = begin_hbm.shape[1:]
    peers, count = lax.axis_size("space"), lax.axis_size("tm")
    rows_total = slab * peers
    tm, rank = lax.axis_index("tm"), lax.axis_index("space")
    has_prev, has_next = tm > 0, tm < count - 1
    has_up, has_down = rank > 0, rank < peers - 1
    blocks = slab // BLOCK
    low_row = rows_total // 2 - CX // 2
    low_column = columns // 2 - CX // 2
    coarse_rows = gain.shape[1]
    coarse_blocks = coarse_rows // BLOCK
    inward = min(HALO, slab - coarse_rows)
    coarse_rank = (rank * slab < low_row + CX) & (rank * slab + slab > low_row)
    lower = rank < peers // 2
    coarse_start = jnp.clip(low_row - rank * slab, 0, slab - coarse_rows)
    coarse_block = coarse_start // BLOCK
    first = jnp.where(
        coarse_rank,
        jnp.where(lower, coarse_block, blocks - coarse_block - coarse_blocks),
        0,
    )

    def block_of(step):
        index = jnp.where(step < blocks - first, first + step, blocks - 1 - step)
        return jnp.where(lower, index, blocks - 1 - index)

    def rows_of(block):
        return pl.ds(pl.multiple_of(block * BLOCK, BLOCK), BLOCK)

    def load(slot, top, height, left, width):
        top, left = pl.multiple_of(top, HALO), pl.multiple_of(left, LANES)
        source, here = pl.ds(top, height), pl.ds(left, width)
        target = pl.ds(pl.multiple_of(top + HALO, HALO), height)
        pltpu.make_async_copy(
            begin_hbm.at[:, source, here], ext.at[0, :, target, here], load_sem.at[slot]
        ).start()
        pltpu.make_async_copy(
            nodes_hbm.at[:, :, source, here], ext.at[1:3, :, target, here], load_sem.at[slot]
        ).start()

    def loaded(slot, height, width):
        part = ext.at[:, :, pl.ds(0, height), pl.ds(0, width)]
        pltpu.make_async_copy(part, part, load_sem.at[slot]).wait()

    side_rows = coarse_rows + inward
    head_rows = BLOCK + 2 * HALO if inward else 0
    first_rows, width = BLOCK + HALO, columns // PARTS
    rest_rows = slab - first_rows - BLOCK

    def load_first():
        top = jnp.where(lower, slab - side_rows, 0)
        if head_rows:
            load(3, jnp.where(lower, top, side_rows - head_rows), head_rows, 0, LANES)
        else:
            load(0, top, side_rows, low_column, CX)

    def load_coarse_rank():
        top = jnp.where(lower, slab - side_rows, 0)
        if head_rows:
            first_top = jnp.where(lower, top, side_rows - head_rows)
            load(4, first_top, head_rows, LANES, low_column - LANES)
            load(0, top, side_rows, low_column, CX)
        rest = jnp.where(lower, top + head_rows, 0)
        load(1, rest, side_rows - head_rows, 0, low_column)
        load(1, top, side_rows, low_column + CX, low_column)
        if slab > side_rows:
            load(2, jnp.where(lower, 0, side_rows), slab - side_rows, 0, columns)

    def load_part(part):
        load(part, jnp.where(lower, 0, slab - first_rows), first_rows, part * width, width)

    def load_other_rank():
        pl.loop(1, PARTS)(load_part)

        load(PARTS, jnp.where(lower, first_rows, rest_rows), BLOCK, 0, columns)
        load(PARTS + 1, jnp.where(lower, slab - rest_rows, 0), rest_rows, 0, columns)

    def begin_copies():
        def copy(top, height, left, width):
            place = (slice(None), pl.ds(pl.multiple_of(top, HALO), height), pl.ds(left, width))
            pltpu.make_async_copy(begin_hbm.at[place], start_out.at[place], bulk_recv).start()

        @pl.when(coarse_rank)
        def _():
            copy(coarse_start, coarse_rows, 0, low_column)
            copy(coarse_start, coarse_rows, low_column + CX, low_column)
            if slab > coarse_rows:
                top = jnp.where(lower, 0, coarse_rows)
                copy(top, slab - coarse_rows, 0, columns)

        @pl.when(jnp.logical_not(coarse_rank))
        def _():
            copy(0, slab, 0, columns)

    def halo_start(side, slot, sources):
        target = pl.ds(slab + HALO if side == 0 else 0, HALO)
        for left, extent in (
            ((low_column, CX),)
            if slot == 0
            else ((0, low_column), (low_column + CX, low_column))
        ):
            here = pl.ds(left, extent)
            for source, place in zip(sources, (0, slice(1, 3))):
                pltpu.make_async_remote_copy(
                    source.at[..., here],
                    ext.at[place, :, target, here],
                    halo_send.at[side],
                    halo_recv.at[side, slot],
                    device_id={"space": rank - 1 if side == 0 else rank + 1},
                    device_id_type=MESH,
                ).start()

    def answered():
        @pl.when(has_down)
        def _():
            pl.semaphore_wait(answer, 1)

    def halo_exchange(slots, loaded_edge):
        for side, exists in ((0, has_up), (1, has_down)):
            edge = pl.ds(0 if side == 0 else slab - HALO, HALO)
            held = pl.ds(HALO if side == 0 else slab, HALO)
            inner = coarse_rank & (lower if side == 1 else jnp.logical_not(lower))
            for slot in slots:
                fit = inner if loaded_edge else jnp.logical_not(inner)
                fit = exists if slot == 1 else exists & fit
                sources = (
                    (ext.at[0, :, held, :], ext.at[1:3, :, held, :])
                    if loaded_edge
                    else (begin_hbm.at[:, edge, :], nodes_hbm.at[:, :, edge, :])
                )

                @pl.when(fit)
                def _(side=side, slot=slot, sources=sources):
                    halo_start(side, slot, sources)

    def halo_wait(block, slot):
        for side, edge in ((0, (block == blocks - 1) & has_down), (1, (block == 0) & has_up)):

            @pl.when(edge)
            def _(side=side):
                part = ext.at[:, :, pl.ds(0, HALO), pl.ds(0, CX if slot == 0 else columns - CX)]
                pltpu.make_async_copy(part, part, halo_recv.at[side, slot]).wait()

    following = {"tm": tm + 1}

    def deferred(tm):
        return defers(tm, slab, coarse_rows)

    def relay_rows(step, origin):
        top = block_of(step // PIECES) * BLOCK + step % PIECES * (BLOCK // PIECES) - origin
        return pl.ds(pl.multiple_of(top, HALO), BLOCK // PIECES)

    def relay_copy(step):
        place = (slice(None), relay_rows(step, 0), pl.ds(low_column, CX))
        return pltpu.make_async_remote_copy(
            nodes_out.at[(1,) + place],
            start_out.at[place],
            relay_send,
            relay_recv.at[step],
            device_id=following,
            device_id_type=MESH,
        )

    detours = min(DETOURS, (count - 1) // 2)
    taking_part = jnp.logical_not(coarse_rank) & (tm <= 2 * detours)
    detoured = taking_part & (tm % 2 == 1)
    detour_rows = transit.shape[2]

    def detour_place():
        top = pl.multiple_of(block_of(blocks - 1) * BLOCK, BLOCK)
        return slice(None), pl.ds(top, detour_rows), slice(None)

    def detour():
        for sign, met, ends in ((1, below, (tm == 0, tm == 2 * detours)), (-1, above, (tm == 2 * detours, tm == 0))):

            @pl.when(jnp.logical_not(ends[0]))
            def _(met=met):
                pl.semaphore_wait(met, 1)

            @pl.when(jnp.logical_not(ends[1]))
            def _(met=met, sign=sign):
                pl.semaphore_signal(
                    met, inc=1, device_id={"tm": tm + sign}, device_id_type=MESH
                )

        slot = tm // 2
        place = detour_place()

        @pl.when(detoured)
        def _():
            pltpu.make_async_remote_copy(
                nodes_out.at[(1,) + place],
                transit.at[slot],
                bulk_send,
                transit_recv,
                device_id={"tm": tm - tm},
                device_id_type=MESH,
            ).start()

        @pl.when(tm == 0)
        def _():
            pltpu.make_async_copy(transit, transit, transit_recv).wait()
            for slot in range(detours):
                pltpu.make_async_remote_copy(
                    transit.at[slot],
                    start_out.at[place],
                    relay_send,
                    bulk_recv,
                    device_id={"tm": tm + 2 * slot + 2},
                    device_id_type=MESH,
                ).start()
            pltpu.make_async_copy(transit, transit, relay_send).wait()

    def bulk_copy(block, left, width, top=0):
        rows = pl.ds(pl.multiple_of(block * BLOCK + top, HALO), BLOCK - top)
        place = (slice(None), rows, pl.ds(pl.multiple_of(left, LANES), width))
        pltpu.make_async_remote_copy(
            nodes_out.at[(1,) + place],
            start_out.at[place],
            bulk_send,
            bulk_recv,
            device_id=following,
            device_id_type=MESH,
        ).start()

    def bulk(unit):
        step, part = unit // PARTS, unit % PARTS
        block = block_of(step)
        strip = coarse_rank & (step < coarse_blocks)
        sent = (step == 0) & (part == PARTS - 2) & (head_rows > 0)

        def copy(left, width):
            bulk_copy(block, left, width)

        @pl.when(strip & (part >= PARTS - 2) & jnp.logical_not(sent))
        def _():
            copy((part - (PARTS - 2)) * (low_column + CX), low_column)

        quick = (step == 0) & jnp.logical_not(coarse_rank)

        @pl.when(quick)
        def _():
            copy(part * (columns // PARTS), columns // PARTS)

        whole = jnp.logical_not(quick | coarse_rank) & (part == PARTS - 1)
        short = detoured & (step == blocks - 1)

        @pl.when(whole & jnp.logical_not(short))
        def _():
            copy(0, columns)

        @pl.when(whole & short)
        def _():
            bulk_copy(block, 0, columns, detour_rows)

    def send(step, low, high):
        held = coarse_rank & deferred(tm) & (step == coarse_blocks - 1)

        @pl.when(has_next & jnp.logical_not(held))
        def _():
            @pl.loop(low, high)
            def _(part):
                bulk(PARTS * step + part)

    pl.when(coarse_rank)(load_first)

    @pl.when(jnp.logical_not(coarse_rank))
    def _():
        load_part(0)

    barrier = pltpu.get_barrier_semaphore()
    for there, exists in (
        ({"tm": tm - 1}, has_prev),
        ({"space": rank + 1}, has_down),
    ):

        @pl.when(exists)
        def _(there=there):
            pl.semaphore_signal(barrier, inc=1, device_id=there, device_id_type=MESH)

    pl.when(coarse_rank)(load_coarse_rank)
    pl.when(jnp.logical_not(coarse_rank))(load_other_rank)

    for side, exists in ((0, has_up), (1, has_down)):

        @pl.when(jnp.logical_not(exists))
        def _(side=side):
            edge = pl.ds(0 if side == 0 else slab + HALO, HALO)
            ext[:, :, edge, :] = jnp.zeros((3, 2, HALO, columns), jnp.float32)

    pl.when(jnp.logical_not(has_prev))(begin_copies)

    def greet():
        friends = jnp.where(has_up, 1, 0) + jnp.where(has_next, 1, 0)

        @pl.when(friends > 0)
        def _():
            pl.semaphore_wait(barrier, friends)

        @pl.when(has_up)
        def _():
            pl.semaphore_signal(
                answer, inc=1, device_id={"space": rank - 1}, device_id_type=MESH
            )
    def strip_compute(block, column, coarse):
        length = BLOCK + 2 * HALO
        span = pl.ds(pl.multiple_of(block * BLOCK, BLOCK), length)
        here = pl.ds(column, LANES)
        begin, one, two = [[ext[f, k, span, here] for k in range(2)] for f in range(3)]
        row = lax.broadcasted_iota(jnp.int32, (length, LANES), 0)
        row = row + (rank * slab + block * BLOCK - HALO)
        along = (row - rows_total // 2).astype(jnp.float32) / (rows_total // 2)
        place = lax.broadcasted_iota(jnp.int32, (1, LANES), 1) + column
        across = (place - columns // 2).astype(jnp.float32) / (columns // 2)
        inside = jnp.where((row >= 0) & (row < rows_total), 1.0, 0.0).astype(jnp.float32)
        real = -diffusion * (along * along + across * across)
        imag = -drift * across
        factor = shear * across
        half_real, half_imag = 1.0 - 0.5 * real, -0.5 * imag
        scale = 1.0 / (half_real * half_real + half_imag * half_imag)
        inverse = (half_real * scale, -half_imag * scale)
        sum_one = weighted(first_weights, (begin, one, two))
        sum_two = weighted(second_weights, (begin, one, two))
        moved = times(real, imag, [s - 0.5 * o for s, o in zip(sum_one, one)])
        turned = coupled(factor, sum_one)
        inner = [begin[k] + moved[k] + turned[k] for k in range(2)]
        node_one = [inside * f for f in times(*inverse, inner)]
        moved = times(real, imag, [s - 0.5 * o for s, o in zip(sum_two, two)])
        turned = coupled(
            factor, [sum_two[k] + 0.5 * (node_one[k] - one[k]) for k in range(2)]
        )
        inner = [node_one[k] + moved[k] + turned[k] for k in range(2)]
        node_two = times(*inverse, inner)
        own = slice(HALO, HALO + BLOCK)
        rows = rows_of(block)
        if not coarse:
            for k in range(2):
                nodes_out[0, k, rows, here] = node_one[k][own]
                nodes_out[1, k, rows, here] = node_two[k][own]
            return
        mean = weighted(whole_weights, (begin, node_one, node_two))
        moved = times(real, imag, [mean[k] - node_two[k] for k in range(2)])
        turned = coupled(factor, mean)
        offset = [moved[k] + turned[k] for k in range(2)]
        step_real, step_imag = 1.0 - real, -imag
        scale = 1.0 / (step_real * step_real + step_imag * step_imag)
        grown = (step_real * scale, -step_imag * scale)
        offset = times(*grown, offset)
        local = pl.ds(pl.multiple_of(block * BLOCK - coarse_start, BLOCK), BLOCK)
        inner_here = pl.ds(pl.multiple_of(column - low_column, LANES), LANES)
        for k in range(2):
            gain[k, local, inner_here] = grown[k][own]
            shift[k, local, inner_here] = offset[k][own]
            kept = node_one[k] - 0.5 * (begin[k] + node_two[k])
            nodes_out[0, k, rows, here] = kept[own]

        @pl.when(jnp.logical_not(has_prev))
        def _():
            for k in range(2):
                start_out[k, rows, here] = begin[k][own]

    def coarse_compute(step):
        block = block_of(step)
        halo_wait(block, 0)

        @pl.loop(0, CX // LANES)
        def _(index):
            strip_compute(block, pl.multiple_of(low_column + index * LANES, LANES), True)

    def relay(low, high):
        @pl.loop(low, high)
        def _(step):
            @pl.when(has_prev)
            def _():
                relay_copy(step).wait_recv()

            rows, local = relay_rows(step, 0), relay_rows(step, coarse_start)
            here = pl.ds(low_column, CX)
            begin = [start_out[k, rows, here] for k in range(2)]
            grown = times(gain[0, local, :], gain[1, local, :], begin)
            finish = [grown[k] + shift[k, local, :] for k in range(2)]
            for k in range(2):
                nodes_out[1, k, rows, here] = finish[k]

            @pl.when(has_next)
            def _():
                relay_copy(step).start()

            for k in range(2):
                nodes_out[0, k, rows, here] += 0.5 * (begin[k] + finish[k])

    never = blocks + 1
    turn = jnp.where(coarse_rank, jnp.minimum(TURN * tm, blocks), never)
    early = jnp.where(coarse_rank, jnp.where(deferred(tm), jnp.minimum(EARLY * tm // 4, turn), turn), blocks)

    @pl.when(coarse_rank)
    def _():
        if head_rows:
            loaded(3, head_rows, LANES)

            @pl.loop(0, low_column // LANES)
            def _(strip):
                left = pl.multiple_of(strip * LANES, LANES)
                strip_compute(block_of(0), left, False)
                pl.when(strip == 0)(greet)

                @pl.when(has_next)
                def _():
                    bulk_copy(block_of(0), left, LANES)

                @pl.when(strip == 0)
                def _():
                    loaded(4, head_rows, low_column - LANES)
        else:
            greet()
        loaded(0, side_rows, CX)
        answered()
        halo_exchange((0,), True)
        halo_exchange((0, 1), False)

        @pl.loop(0, coarse_blocks - 1)
        def _(step):
            coarse_compute(step)

    strips = columns // LANES // PARTS

    def step_at(index):
        later = jnp.where(index == blocks - 1, coarse_blocks - 1, index + 1)
        return jnp.where(coarse_rank & (index >= coarse_blocks - 1), later, index)

    @pl.loop(0, blocks + 1)
    def _(index):
        @pl.when(index == turn)
        def _():
            relay(0, PIECES * (coarse_blocks - 1))

        @pl.when(coarse_rank & (index == jnp.minimum(turn, coarse_blocks - 1)))
        def _():
            coarse_compute(coarse_blocks - 1)

        @pl.when(index == turn)
        def _():
            relay(PIECES * (coarse_blocks - 1), PIECES * coarse_blocks)

            @pl.loop(early, turn)
            def _(position):
                send(step_at(position), 0, PARTS)

        @pl.when(index < blocks)
        def _():
            step = step_at(index)
            block = block_of(step)
            in_coarse = coarse_rank & (step < coarse_blocks)

            @pl.when(coarse_rank & (index == 0))
            def _():
                if head_rows:
                    loaded(1, 2 * side_rows - head_rows, low_column)
                else:
                    loaded(1, side_rows, columns - CX)

            if slab > side_rows:

                @pl.when(coarse_rank & (index == coarse_blocks - 1))
                def _():
                    loaded(2, slab - side_rows, columns)

            for slot, height in ((PARTS, BLOCK), (PARTS + 1, rest_rows)):

                @pl.when(jnp.logical_not(coarse_rank) & (step == slot - PARTS + 1))
                def _(slot=slot, height=height):
                    loaded(slot, height, columns)

            @pl.when(jnp.logical_not(in_coarse))
            def _():
                halo_wait(block, 0)

            halo_wait(block, 1)

            @pl.loop(0, PARTS)
            def _(part):
                @pl.when(jnp.logical_not(coarse_rank) & (step == 0))
                def _():
                    loaded(part, first_rows, width)

                @pl.loop(0, strips)
                def _(strip):
                    low = (part * strips + strip) * LANES

                    begun = in_coarse & (step == 0) & (low < low_column) & (head_rows > 0)
                    kept = in_coarse & (low >= low_column) & (low < low_column + CX)

                    @pl.when(jnp.logical_not(begun | kept))
                    def _():
                        strip_compute(block, pl.multiple_of(low, LANES), False)

                @pl.when(jnp.logical_not(coarse_rank) & (step == 0) & (part == 0))
                def _():
                    greet()

                @pl.when(jnp.logical_not(coarse_rank) & (step == 0) & (part == 1))
                def _():
                    answered()
                    halo_exchange((0, 1), False)

                @pl.when((index < early) | (index >= turn))
                def _():
                    send(step, part, part + 1)

    if detours:
        pl.when(taking_part)(detour)

    def total(sem, height, extent):
        part = start_out.at[:, pl.ds(0, height), pl.ds(0, extent)]
        pltpu.make_async_copy(part, part, sem).wait()

    def all_bulk(sem, rows, lately):
        for short in (False, True):

            @pl.when(coarse_rank & (lately == short))
            def _(short=short):
                extent = rows - BLOCK if short else rows
                narrow = coarse_rows - BLOCK if short else coarse_rows
                total(sem, extent - narrow * CX // columns, columns)

        @pl.when(jnp.logical_not(coarse_rank))
        def _():
            total(sem, slab, columns)

    for side, exists in ((0, has_up), (1, has_down)):

        @pl.when(exists)
        def _(side=side):
            part = ext.at[:, :, pl.ds(0, HALO), :]
            pltpu.make_async_copy(part, part, halo_send.at[side]).wait()

    @pl.when(coarse_rank & has_next)
    def _():
        total(relay_send, coarse_rows, CX)

    @pl.when(jnp.logical_not(has_prev))
    def _():
        all_bulk(bulk_recv, slab, tm < 0)

    @pl.when(has_prev)
    def _():
        all_bulk(bulk_recv, coarse_rows, deferred(tm - 1))

    @pl.when(has_next)
    def _():
        all_bulk(bulk_send, coarse_rows, deferred(tm))


def place_of(slab, columns, coarse_rows):
    peers, rank = lax.axis_size("space"), lax.axis_index("space")
    low_row = slab * peers // 2 - CX // 2
    coarse_rank = (rank * slab < low_row + CX) & (rank * slab + slab > low_row)
    coarse_start = jnp.clip(low_row - rank * slab, 0, slab - coarse_rows)
    lower = rank < peers // 2
    other, edge = jnp.where(lower, 0, coarse_rows), jnp.where(lower, slab - BLOCK, 0)
    return coarse_rank, coarse_start, pl.multiple_of(other, HALO), pl.multiple_of(edge, HALO)


def sides(columns):
    width = columns // 2 - CX // 2
    return pl.ds(0, width), pl.ds(columns - width, width)


def write_out(coarse_rows, start, nodes, start_hbm, nodes_hbm, _, sem):
    slab, columns = start.shape[1:]
    coarse_rank, coarse_start, _, _ = place_of(slab, columns, coarse_rows)
    partly = coarse_rank & (lax.axis_index("tm") > 0)
    for part in range(4 * WRITES):
        height = slab // WRITES
        here = (part // 2 % 2, part % 2, pl.ds(part // 4 * height, height))
        pltpu.make_async_copy(nodes.at[here], nodes_hbm.at[here], sem.at[0]).start()

    def copy(top, height, act):
        here = (slice(None), pl.ds(pl.multiple_of(top, HALO), height), slice(None))
        act(pltpu.make_async_copy(start.at[here], start_hbm.at[here], sem.at[1]))

    for act in (lambda c: c.start(), lambda c: c.wait()):

        @pl.when(partly)
        def _(act=act):
            copy(coarse_start, coarse_rows, act)

        @pl.when(jnp.logical_not(partly))
        def _(act=act):
            copy(0, slab, act)

    pltpu.make_async_copy(nodes, nodes_hbm, sem.at[0]).wait()


def send_rest(coarse_rows, nodes, _, rest_out, send_sem, recv_sem):
    slab, columns = nodes.shape[2:]
    coarse_rank, _, other, edge = place_of(slab, columns, coarse_rows)
    tm, count = lax.axis_index("tm"), lax.axis_size("tm")
    has_prev, has_next = coarse_rank & (tm > 0), coarse_rank & (tm < count - 1)
    others = slab - coarse_rows
    barrier = pltpu.get_barrier_semaphore()

    def send(source, target):
        pltpu.make_async_remote_copy(
            source,
            target,
            send_sem,
            recv_sem,
            device_id={"tm": tm + 1},
            device_id_type=MESH,
        ).start()

    def total(sem, lately):
        for short in (False, True):

            @pl.when(lately == short)
            def _(short=short):
                rows = others + (BLOCK - BLOCK * CX // columns if short else 0)
                part = rest_out.at[:, pl.ds(0, rows), :]
                pltpu.make_async_copy(part, part, sem).wait()

    @pl.when(has_prev)
    def _():
        pl.semaphore_signal(barrier, inc=1, device_id={"tm": tm - 1}, device_id_type=MESH)

    @pl.when(has_next)
    def _():
        pl.semaphore_wait(barrier, 1)

        @pl.when(defers(tm, slab, coarse_rows))
        def _():
            for side in sides(columns):
                send(
                    nodes.at[1, :, pl.ds(edge, BLOCK), side],
                    rest_out.at[:, pl.ds(others, BLOCK), side],
                )

        send(nodes.at[1, :, pl.ds(other, others), :], rest_out.at[:, pl.ds(0, others), :])

    @pl.when(has_prev)
    def _():
        total(recv_sem, defers(tm - 1, slab, coarse_rows))

    @pl.when(has_next)
    def _():
        total(send_sem, defers(tm, slab, coarse_rows))


def write_rest(coarse_rows, rest, _, start_hbm, sem):
    slab, columns = start_hbm.shape[1:]
    coarse_rank, _, other, edge = place_of(slab, columns, coarse_rows)
    tm, others = lax.axis_index("tm"), slab - coarse_rows

    @pl.when(coarse_rank & (tm > 0))
    def _():
        whole = pltpu.make_async_copy(
            rest.at[:, pl.ds(0, others), :], start_hbm.at[:, pl.ds(other, others), :], sem.at[0]
        )
        strips = [
            pltpu.make_async_copy(
                rest.at[:, pl.ds(others, BLOCK), side],
                start_hbm.at[:, pl.ds(edge, BLOCK), side],
                sem.at[1 + index],
            )
            for index, side in enumerate(sides(columns))
        ]
        for part in range(2 * WRITES):
            height = others // WRITES
            top = part // 2 * height
            pltpu.make_async_copy(
                rest.at[part % 2, pl.ds(top, height), :],
                start_hbm.at[part % 2, pl.ds(pl.multiple_of(other + top, HALO), height), :],
                sem.at[0],
            ).start()
        for act in (lambda c: c.start(), lambda c: c.wait()):

            @pl.when(defers(tm - 1, slab, coarse_rows))
            def _(act=act):
                for strip in strips:
                    act(strip)

        whole.wait()


def body(start_values, node_values):
    slab, columns = start_values.shape[2:]
    peers = lax.axis_size("space")
    coarse_rows = min(slab, max(CX // 2, CX // peers))
    coarse_blocks = coarse_rows // BLOCK
    slots = max(1, min(DETOURS, (lax.axis_size("tm") - 1) // 2))
    hbm = pl.BlockSpec(memory_space=pltpu.HBM)
    vmem = pl.BlockSpec(memory_space=pltpu.VMEM)
    anywhere = pl.BlockSpec(memory_space=pl.ANY)
    dma = pltpu.SemaphoreType.DMA
    start, nodes = pl.pallas_call(
        kernel,
        out_shape=(
            OUT((2, slab, columns), jnp.float32),
            OUT((2, 2, slab, columns), jnp.float32),
        ),
        in_specs=[hbm, hbm],
        out_specs=(vmem, vmem),
        scratch_shapes=[
            pltpu.VMEM((3, 2, slab + 2 * HALO, columns), jnp.float32),
            pltpu.VMEM((2, coarse_rows, CX), jnp.float32),
            pltpu.VMEM((2, coarse_rows, CX), jnp.float32),
            dma((PARTS + 2,)),
            dma((2,)),
            dma((2, 2)),
            dma,
            dma,
            dma,
            dma((PIECES * coarse_blocks,)),
            pltpu.VMEM((slots, 2, DETOUR_ROWS, columns), jnp.float32),
            dma,
            pltpu.SemaphoreType.REGULAR,
            pltpu.SemaphoreType.REGULAR,
            pltpu.SemaphoreType.REGULAR,
        ],
        compiler_params=pltpu.CompilerParams(
            collective_id=0, has_side_effects=True, vmem_limit_bytes=56 * 1024 * 1024
        ),
    )(start_values[0], node_values[0])
    start_hbm, nodes_hbm, written = pl.pallas_call(
        functools.partial(write_out, coarse_rows),
        out_shape=(
            jax.ShapeDtypeStruct(start.shape, jnp.float32),
            jax.ShapeDtypeStruct(nodes.shape, jnp.float32),
            OUT((8, LANES), jnp.float32),
        ),
        in_specs=[anywhere, anywhere],
        out_specs=(hbm, hbm, vmem),
        scratch_shapes=[dma((2,))],
        compiler_params=pltpu.CompilerParams(vmem_limit_bytes=2 * 1024 * 1024),
    )(start, nodes)
    if slab > coarse_rows:
        rest = pl.pallas_call(
            functools.partial(send_rest, coarse_rows),
            out_shape=OUT((2, slab - coarse_rows + BLOCK, columns), jnp.float32),
            in_specs=[anywhere, anywhere],
            out_specs=vmem,
            scratch_shapes=[dma, dma],
            compiler_params=pltpu.CompilerParams(
                collective_id=1, has_side_effects=True, vmem_limit_bytes=4 * 1024 * 1024
            ),
        )(nodes, written)
        start_hbm = pl.pallas_call(
            functools.partial(write_rest, coarse_rows),
            out_shape=jax.ShapeDtypeStruct(start.shape, jnp.float32),
            in_specs=[anywhere, hbm],
            out_specs=hbm,
            scratch_shapes=[dma((3,))],
            input_output_aliases={1: 0},
            compiler_params=pltpu.CompilerParams(vmem_limit_bytes=2 * 1024 * 1024),
        )(rest, start_hbm)
    return (start_hbm[None], nodes_hbm[None])


OUT = pltpu.VMEM


def solution(mesh):
    in_specs = (P("tm", None, "space", None), P("tm", None, None, "space", None))
    out_specs = (P("tm", None, "space", None), P("tm", None, None, "space", None))
    return jax.shard_map(body, mesh=mesh, in_specs=in_specs, out_specs=out_specs, check_vma=False)
```

```python
import functools

import jax
import jax.numpy as jnp
from jax import lax
from jax.experimental import pallas as pl
from jax.experimental.pallas import tpu as pltpu
from jax.sharding import PartitionSpec as P

CX = 256

diffusion = 1.5
drift = 0.8
shear = 0.6
first_weights = (5.0 / 24.0, 1.0 / 3.0, -1.0 / 24.0)
second_weights = (-1.0 / 24.0, 1.0 / 3.0, 5.0 / 24.0)
whole_weights = (1.0 / 6.0, 2.0 / 3.0, 1.0 / 6.0)

MESH = pl.DeviceIdType.MESH
HALO = 8
BLOCK = 32
PARTS = 4
DEFER = 5
WRITES = 2
DETOURS = 3
DETOUR_ROWS = 16
TURN = 2
EARLY = 3
PIECES = 4
LANES = 128


def weighted(weights, fields):
    return [sum(w * f[k] for w, f in zip(weights, fields)) for k in range(2)]


def times(real, imag, field):
    return [real * field[0] - imag * field[1], real * field[1] + imag * field[0]]


def coupled(factor, field):
    length = field[0].shape[0]
    sums = [pltpu.roll(f, 1, 0) + pltpu.roll(f, length - 1, 0) for f in field]
    return [factor * sums[1], -factor * sums[0]]


def defers(tm, slab, coarse_rows):
    return tm < DEFER if slab > coarse_rows else tm < 0


def kernel(
    begin_hbm,
    nodes_hbm,
    start_out,
    nodes_out,
    ext,
    gain,
    shift,
    load_sem,
    halo_send,
    halo_recv,
    bulk_send,
    bulk_recv,
    relay_send,
    relay_recv,
    transit,
    transit_recv,
    below,
    above,
    answer,
):
    slab, columns = begin_hbm.shape[1:]
    peers, count = lax.axis_size("space"), lax.axis_size("tm")
    rows_total = slab * peers
    tm, rank = lax.axis_index("tm"), lax.axis_index("space")
    has_prev, has_next = tm > 0, tm < count - 1
    has_up, has_down = rank > 0, rank < peers - 1
    blocks = slab // BLOCK
    low_row = rows_total // 2 - CX // 2
    low_column = columns // 2 - CX // 2
    coarse_rows = gain.shape[1]
    coarse_blocks = coarse_rows // BLOCK
    inward = min(HALO, slab - coarse_rows)
    coarse_rank = (rank * slab < low_row + CX) & (rank * slab + slab > low_row)
    lower = rank < peers // 2
    coarse_start = jnp.clip(low_row - rank * slab, 0, slab - coarse_rows)
    coarse_block = coarse_start // BLOCK
    first = jnp.where(
        coarse_rank,
        jnp.where(lower, coarse_block, blocks - coarse_block - coarse_blocks),
        0,
    )

    def block_of(step):
        index = jnp.where(step < blocks - first, first + step, blocks - 1 - step)
        return jnp.where(lower, index, blocks - 1 - index)

    def rows_of(block):
        return pl.ds(pl.multiple_of(block * BLOCK, BLOCK), BLOCK)

    def load(slot, top, height, left, width):
        top, left = pl.multiple_of(top, HALO), pl.multiple_of(left, LANES)
        source, here = pl.ds(top, height), pl.ds(left, width)
        target = pl.ds(pl.multiple_of(top + HALO, HALO), height)
        pltpu.make_async_copy(
            begin_hbm.at[:, source, here], ext.at[0, :, target, here], load_sem.at[slot]
        ).start()
        pltpu.make_async_copy(
            nodes_hbm.at[:, :, source, here], ext.at[1:3, :, target, here], load_sem.at[slot]
        ).start()

    def loaded(slot, height, width):
        part = ext.at[:, :, pl.ds(0, height), pl.ds(0, width)]
        pltpu.make_async_copy(part, part, load_sem.at[slot]).wait()

    side_rows = coarse_rows + inward
    head_rows = BLOCK + 2 * HALO if inward else 0
    first_rows, width = BLOCK + HALO, columns // PARTS
    rest_rows = slab - first_rows - BLOCK

    def load_first():
        top = jnp.where(lower, slab - side_rows, 0)
        if head_rows:
            load(3, jnp.where(lower, top, side_rows - head_rows), head_rows, 0, LANES)
        else:
            load(0, top, side_rows, low_column, CX)

    def load_coarse_rank():
        top = jnp.where(lower, slab - side_rows, 0)
        if head_rows:
            first_top = jnp.where(lower, top, side_rows - head_rows)
            load(4, first_top, head_rows, LANES, low_column - LANES)
            load(0, top, side_rows, low_column, CX)
        rest = jnp.where(lower, top + head_rows, 0)
        load(1, rest, side_rows - head_rows, 0, low_column)
        load(1, top, side_rows, low_column + CX, low_column)
        if slab > side_rows:
            load(2, jnp.where(lower, 0, side_rows), slab - side_rows, 0, columns)

    def load_part(part):
        load(part, jnp.where(lower, 0, slab - first_rows), first_rows, part * width, width)

    def load_other_rank():
        pl.loop(1, PARTS)(load_part)

        load(PARTS, jnp.where(lower, first_rows, rest_rows), BLOCK, 0, columns)
        load(PARTS + 1, jnp.where(lower, slab - rest_rows, 0), rest_rows, 0, columns)

    def begin_copies():
        def copy(top, height, left, width):
            place = (slice(None), pl.ds(pl.multiple_of(top, HALO), height), pl.ds(left, width))
            pltpu.make_async_copy(begin_hbm.at[place], start_out.at[place], bulk_recv).start()

        @pl.when(coarse_rank)
        def _():
            copy(coarse_start, coarse_rows, 0, low_column)
            copy(coarse_start, coarse_rows, low_column + CX, low_column)
            if slab > coarse_rows:
                top = jnp.where(lower, 0, coarse_rows)
                copy(top, slab - coarse_rows, 0, columns)

        @pl.when(jnp.logical_not(coarse_rank))
        def _():
            copy(0, slab, 0, columns)

    def halo_start(side, slot, sources):
        target = pl.ds(slab + HALO if side == 0 else 0, HALO)
        for left, extent in (
            ((low_column, CX),)
            if slot == 0
            else ((0, low_column), (low_column + CX, low_column))
        ):
            here = pl.ds(left, extent)
            for source, place in zip(sources, (0, slice(1, 3))):
                pltpu.make_async_remote_copy(
                    source.at[..., here],
                    ext.at[place, :, target, here],
                    halo_send.at[side],
                    halo_recv.at[side, slot],
                    device_id={"space": rank - 1 if side == 0 else rank + 1},
                    device_id_type=MESH,
                ).start()

    def answered():
        @pl.when(has_down)
        def _():
            pl.semaphore_wait(answer, 1)

    def halo_exchange(slots, loaded_edge):
        for side, exists in ((0, has_up), (1, has_down)):
            edge = pl.ds(0 if side == 0 else slab - HALO, HALO)
            held = pl.ds(HALO if side == 0 else slab, HALO)
            inner = coarse_rank & (lower if side == 1 else jnp.logical_not(lower))
            for slot in slots:
                fit = inner if loaded_edge else jnp.logical_not(inner)
                fit = exists if slot == 1 else exists & fit
                sources = (
                    (ext.at[0, :, held, :], ext.at[1:3, :, held, :])
                    if loaded_edge
                    else (begin_hbm.at[:, edge, :], nodes_hbm.at[:, :, edge, :])
                )

                @pl.when(fit)
                def _(side=side, slot=slot, sources=sources):
                    halo_start(side, slot, sources)

    def halo_wait(block, slot):
        for side, edge in ((0, (block == blocks - 1) & has_down), (1, (block == 0) & has_up)):

            @pl.when(edge)
            def _(side=side):
                part = ext.at[:, :, pl.ds(0, HALO), pl.ds(0, CX if slot == 0 else columns - CX)]
                pltpu.make_async_copy(part, part, halo_recv.at[side, slot]).wait()

    following = {"tm": tm + 1}

    def deferred(tm):
        return defers(tm, slab, coarse_rows)

    def relay_rows(step, origin):
        top = block_of(step // PIECES) * BLOCK + step % PIECES * (BLOCK // PIECES) - origin
        return pl.ds(pl.multiple_of(top, HALO), BLOCK // PIECES)

    def relay_copy(step):
        place = (slice(None), relay_rows(step, 0), pl.ds(low_column, CX))
        return pltpu.make_async_remote_copy(
            nodes_out.at[(1,) + place],
            start_out.at[place],
            relay_send,
            relay_recv.at[step],
            device_id=following,
            device_id_type=MESH,
        )

    detours = min(DETOURS, (count - 1) // 2)
    taking_part = jnp.logical_not(coarse_rank) & (tm <= 2 * detours)
    detoured = taking_part & (tm % 2 == 1)
    detour_rows = transit.shape[2]

    def detour_place():
        top = pl.multiple_of(block_of(blocks - 1) * BLOCK, BLOCK)
        return slice(None), pl.ds(top, detour_rows), slice(None)

    def detour():
        for sign, met, ends in ((1, below, (tm == 0, tm == 2 * detours)), (-1, above, (tm == 2 * detours, tm == 0))):

            @pl.when(jnp.logical_not(ends[0]))
            def _(met=met):
                pl.semaphore_wait(met, 1)

            @pl.when(jnp.logical_not(ends[1]))
            def _(met=met, sign=sign):
                pl.semaphore_signal(
                    met, inc=1, device_id={"tm": tm + sign}, device_id_type=MESH
                )

        slot = tm // 2
        place = detour_place()

        @pl.when(detoured)
        def _():
            pltpu.make_async_remote_copy(
                nodes_out.at[(1,) + place],
                transit.at[slot],
                bulk_send,
                transit_recv,
                device_id={"tm": tm - tm},
                device_id_type=MESH,
            ).start()

        @pl.when(tm == 0)
        def _():
            pltpu.make_async_copy(transit, transit, transit_recv).wait()
            for slot in range(detours):
                pltpu.make_async_remote_copy(
                    transit.at[slot],
                    start_out.at[place],
                    relay_send,
                    bulk_recv,
                    device_id={"tm": tm + 2 * slot + 2},
                    device_id_type=MESH,
                ).start()
            pltpu.make_async_copy(transit, transit, relay_send).wait()

    def bulk_copy(block, left, width, top=0):
        rows = pl.ds(pl.multiple_of(block * BLOCK + top, HALO), BLOCK - top)
        place = (slice(None), rows, pl.ds(pl.multiple_of(left, LANES), width))
        pltpu.make_async_remote_copy(
            nodes_out.at[(1,) + place],
            start_out.at[place],
            bulk_send,
            bulk_recv,
            device_id=following,
            device_id_type=MESH,
        ).start()

    def bulk(unit):
        step, part = unit // PARTS, unit % PARTS
        block = block_of(step)
        strip = coarse_rank & (step < coarse_blocks)
        sent = (step == 0) & (part == PARTS - 2) & (head_rows > 0)

        def copy(left, width):
            bulk_copy(block, left, width)

        @pl.when(strip & (part >= PARTS - 2) & jnp.logical_not(sent))
        def _():
            copy((part - (PARTS - 2)) * (low_column + CX), low_column)

        quick = (step == 0) & jnp.logical_not(coarse_rank)

        @pl.when(quick)
        def _():
            copy(part * (columns // PARTS), columns // PARTS)

        whole = jnp.logical_not(quick | coarse_rank) & (part == PARTS - 1)
        short = detoured & (step == blocks - 1)

        @pl.when(whole & jnp.logical_not(short))
        def _():
            copy(0, columns)

        @pl.when(whole & short)
        def _():
            bulk_copy(block, 0, columns, detour_rows)

    def send(step, low, high):
        held = coarse_rank & deferred(tm) & (step == coarse_blocks - 1)

        @pl.when(has_next & jnp.logical_not(held))
        def _():
            @pl.loop(low, high)
            def _(part):
                bulk(PARTS * step + part)

    pl.when(coarse_rank)(load_first)

    @pl.when(jnp.logical_not(coarse_rank))
    def _():
        load_part(0)

    barrier = pltpu.get_barrier_semaphore()
    for there, exists in (
        ({"tm": tm - 1}, has_prev),
        ({"space": rank + 1}, has_down),
    ):

        @pl.when(exists)
        def _(there=there):
            pl.semaphore_signal(barrier, inc=1, device_id=there, device_id_type=MESH)

    pl.when(coarse_rank)(load_coarse_rank)
    pl.when(jnp.logical_not(coarse_rank))(load_other_rank)

    for side, exists in ((0, has_up), (1, has_down)):

        @pl.when(jnp.logical_not(exists))
        def _(side=side):
            edge = pl.ds(0 if side == 0 else slab + HALO, HALO)
            ext[:, :, edge, :] = jnp.zeros((3, 2, HALO, columns), jnp.float32)

    pl.when(jnp.logical_not(has_prev))(begin_copies)

    def greet():
        friends = jnp.where(has_up, 1, 0) + jnp.where(has_next, 1, 0)

        @pl.when(friends > 0)
        def _():
            pl.semaphore_wait(barrier, friends)

        @pl.when(has_up)
        def _():
            pl.semaphore_signal(
                answer, inc=1, device_id={"space": rank - 1}, device_id_type=MESH
            )
    def strip_compute(block, column, coarse):
        length = BLOCK + 2 * HALO
        span = pl.ds(pl.multiple_of(block * BLOCK, BLOCK), length)
        here = pl.ds(column, LANES)
        begin, one, two = [[ext[f, k, span, here] for k in range(2)] for f in range(3)]
        row = lax.broadcasted_iota(jnp.int32, (length, LANES), 0)
        row = row + (rank * slab + block * BLOCK - HALO)
        along = (row - rows_total // 2).astype(jnp.float32) / (rows_total // 2)
        place = lax.broadcasted_iota(jnp.int32, (1, LANES), 1) + column
        across = (place - columns // 2).astype(jnp.float32) / (columns // 2)
        inside = jnp.where((row >= 0) & (row < rows_total), 1.0, 0.0).astype(jnp.float32)
        real = -diffusion * (along * along + across * across)
        imag = -drift * across
        factor = shear * across
        half_real, half_imag = 1.0 - 0.5 * real, -0.5 * imag
        scale = 1.0 / (half_real * half_real + half_imag * half_imag)
        inverse = (half_real * scale, -half_imag * scale)
        sum_one = weighted(first_weights, (begin, one, two))
        sum_two = weighted(second_weights, (begin, one, two))
        moved = times(real, imag, [s - 0.5 * o for s, o in zip(sum_one, one)])
        turned = coupled(factor, sum_one)
        inner = [begin[k] + moved[k] + turned[k] for k in range(2)]
        node_one = [inside * f for f in times(*inverse, inner)]
        moved = times(real, imag, [s - 0.5 * o for s, o in zip(sum_two, two)])
        turned = coupled(
            factor, [sum_two[k] + 0.5 * (node_one[k] - one[k]) for k in range(2)]
        )
        inner = [node_one[k] + moved[k] + turned[k] for k in range(2)]
        node_two = times(*inverse, inner)
        own = slice(HALO, HALO + BLOCK)
        rows = rows_of(block)
        if not coarse:
            for k in range(2):
                nodes_out[0, k, rows, here] = node_one[k][own]
                nodes_out[1, k, rows, here] = node_two[k][own]
            return
        mean = weighted(whole_weights, (begin, node_one, node_two))
        moved = times(real, imag, [mean[k] - node_two[k] for k in range(2)])
        turned = coupled(factor, mean)
        offset = [moved[k] + turned[k] for k in range(2)]
        step_real, step_imag = 1.0 - real, -imag
        scale = 1.0 / (step_real * step_real + step_imag * step_imag)
        grown = (step_real * scale, -step_imag * scale)
        offset = times(*grown, offset)
        local = pl.ds(pl.multiple_of(block * BLOCK - coarse_start, BLOCK), BLOCK)
        inner_here = pl.ds(pl.multiple_of(column - low_column, LANES), LANES)
        for k in range(2):
            gain[k, local, inner_here] = grown[k][own]
            shift[k, local, inner_here] = offset[k][own]
            kept = node_one[k] - 0.5 * (begin[k] + node_two[k])
            nodes_out[0, k, rows, here] = kept[own]

        @pl.when(jnp.logical_not(has_prev))
        def _():
            for k in range(2):
                start_out[k, rows, here] = begin[k][own]

    def coarse_compute(step):
        block = block_of(step)
        halo_wait(block, 0)

        @pl.loop(0, CX // LANES)
        def _(index):
            strip_compute(block, pl.multiple_of(low_column + index * LANES, LANES), True)

    def relay(low, high):
        @pl.loop(low, high)
        def _(step):
            @pl.when(has_prev)
            def _():
                relay_copy(step).wait_recv()

            rows, local = relay_rows(step, 0), relay_rows(step, coarse_start)
            here = pl.ds(low_column, CX)
            begin = [start_out[k, rows, here] for k in range(2)]
            grown = times(gain[0, local, :], gain[1, local, :], begin)
            finish = [grown[k] + shift[k, local, :] for k in range(2)]
            for k in range(2):
                nodes_out[1, k, rows, here] = finish[k]

            @pl.when(has_next)
            def _():
                relay_copy(step).start()

            for k in range(2):
                nodes_out[0, k, rows, here] += 0.5 * (begin[k] + finish[k])

    never = blocks + 1
    turn = jnp.where(coarse_rank, jnp.minimum(TURN * tm, blocks), never)
    early = jnp.where(coarse_rank, jnp.where(deferred(tm), jnp.minimum(EARLY * tm // 4, turn), turn), blocks)

    @pl.when(coarse_rank)
    def _():
        if head_rows:
            loaded(3, head_rows, LANES)

            @pl.loop(0, low_column // LANES)
            def _(strip):
                left = pl.multiple_of(strip * LANES, LANES)
                strip_compute(block_of(0), left, False)
                pl.when(strip == 0)(greet)

                @pl.when(has_next)
                def _():
                    bulk_copy(block_of(0), left, LANES)

                @pl.when(strip == 0)
                def _():
                    loaded(4, head_rows, low_column - LANES)
        else:
            greet()
        loaded(0, side_rows, CX)
        answered()
        halo_exchange((0,), True)
        halo_exchange((0, 1), False)

        @pl.loop(0, coarse_blocks - 1)
        def _(step):
            coarse_compute(step)

    greets_first = low_row // slab > 1
    other_rank = jnp.logical_not(coarse_rank)

    if greets_first:

        @pl.when(other_rank)
        def _():
            greet()
            answered()
            halo_exchange((0, 1), False)

    strips = columns // LANES // PARTS

    def step_at(index):
        later = jnp.where(index == blocks - 1, coarse_blocks - 1, index + 1)
        return jnp.where(coarse_rank & (index >= coarse_blocks - 1), later, index)

    @pl.loop(0, blocks + 1)
    def _(index):
        @pl.when(index == turn)
        def _():
            relay(0, PIECES * (coarse_blocks - 1))

        @pl.when(coarse_rank & (index == jnp.minimum(turn, coarse_blocks - 1)))
        def _():
            coarse_compute(coarse_blocks - 1)

        @pl.when(index == turn)
        def _():
            relay(PIECES * (coarse_blocks - 1), PIECES * coarse_blocks)

            @pl.loop(early, turn)
            def _(position):
                send(step_at(position), 0, PARTS)

        @pl.when(index < blocks)
        def _():
            step = step_at(index)
            block = block_of(step)
            in_coarse = coarse_rank & (step < coarse_blocks)

            @pl.when(coarse_rank & (index == 0))
            def _():
                if head_rows:
                    loaded(1, 2 * side_rows - head_rows, low_column)
                else:
                    loaded(1, side_rows, columns - CX)

            if slab > side_rows:

                @pl.when(coarse_rank & (index == coarse_blocks - 1))
                def _():
                    loaded(2, slab - side_rows, columns)

            for slot, height in ((PARTS, BLOCK), (PARTS + 1, rest_rows)):

                @pl.when(jnp.logical_not(coarse_rank) & (step == slot - PARTS + 1))
                def _(slot=slot, height=height):
                    loaded(slot, height, columns)

            @pl.when(jnp.logical_not(in_coarse))
            def _():
                halo_wait(block, 0)

            halo_wait(block, 1)

            @pl.loop(0, PARTS)
            def _(part):
                @pl.when(jnp.logical_not(coarse_rank) & (step == 0))
                def _():
                    loaded(part, first_rows, width)

                @pl.loop(0, strips)
                def _(strip):
                    low = (part * strips + strip) * LANES

                    begun = in_coarse & (step == 0) & (low < low_column) & (head_rows > 0)
                    kept = in_coarse & (low >= low_column) & (low < low_column + CX)

                    @pl.when(jnp.logical_not(begun | kept))
                    def _():
                        strip_compute(block, pl.multiple_of(low, LANES), False)

                if not greets_first:
                    pl.when(other_rank & (step == 0) & (part == 0))(greet)

                    @pl.when(other_rank & (step == 0) & (part == 1))
                    def _():
                        answered()
                        halo_exchange((0, 1), False)

                @pl.when((index < early) | (index >= turn))
                def _():
                    send(step, part, part + 1)

    if detours:
        pl.when(taking_part)(detour)

    def total(sem, height, extent):
        part = start_out.at[:, pl.ds(0, height), pl.ds(0, extent)]
        pltpu.make_async_copy(part, part, sem).wait()

    def all_bulk(sem, rows, lately):
        for short in (False, True):

            @pl.when(coarse_rank & (lately == short))
            def _(short=short):
                extent = rows - BLOCK if short else rows
                narrow = coarse_rows - BLOCK if short else coarse_rows
                total(sem, extent - narrow * CX // columns, columns)

        @pl.when(jnp.logical_not(coarse_rank))
        def _():
            total(sem, slab, columns)

    for side, exists in ((0, has_up), (1, has_down)):

        @pl.when(exists)
        def _(side=side):
            part = ext.at[:, :, pl.ds(0, HALO), :]
            pltpu.make_async_copy(part, part, halo_send.at[side]).wait()

    @pl.when(coarse_rank & has_next)
    def _():
        total(relay_send, coarse_rows, CX)

    @pl.when(jnp.logical_not(has_prev))
    def _():
        all_bulk(bulk_recv, slab, tm < 0)

    @pl.when(has_prev)
    def _():
        all_bulk(bulk_recv, coarse_rows, deferred(tm - 1))

    @pl.when(has_next)
    def _():
        all_bulk(bulk_send, coarse_rows, deferred(tm))


def place_of(slab, columns, coarse_rows):
    peers, rank = lax.axis_size("space"), lax.axis_index("space")
    low_row = slab * peers // 2 - CX // 2
    coarse_rank = (rank * slab < low_row + CX) & (rank * slab + slab > low_row)
    coarse_start = jnp.clip(low_row - rank * slab, 0, slab - coarse_rows)
    lower = rank < peers // 2
    other, edge = jnp.where(lower, 0, coarse_rows), jnp.where(lower, slab - BLOCK, 0)
    return coarse_rank, coarse_start, pl.multiple_of(other, HALO), pl.multiple_of(edge, HALO)


def sides(columns):
    width = columns // 2 - CX // 2
    return pl.ds(0, width), pl.ds(columns - width, width)


def write_out(coarse_rows, start, nodes, start_hbm, nodes_hbm, _, sem):
    slab, columns = start.shape[1:]
    coarse_rank, coarse_start, _, _ = place_of(slab, columns, coarse_rows)
    partly = coarse_rank & (lax.axis_index("tm") > 0)
    for part in range(4 * WRITES):
        height = slab // WRITES
        here = (part // 2 % 2, part % 2, pl.ds(part // 4 * height, height))
        pltpu.make_async_copy(nodes.at[here], nodes_hbm.at[here], sem.at[0]).start()

    def copy(top, height, act):
        here = (slice(None), pl.ds(pl.multiple_of(top, HALO), height), slice(None))
        act(pltpu.make_async_copy(start.at[here], start_hbm.at[here], sem.at[1]))

    for act in (lambda c: c.start(), lambda c: c.wait()):

        @pl.when(partly)
        def _(act=act):
            copy(coarse_start, coarse_rows, act)

        @pl.when(jnp.logical_not(partly))
        def _(act=act):
            copy(0, slab, act)

    pltpu.make_async_copy(nodes, nodes_hbm, sem.at[0]).wait()


def send_rest(coarse_rows, nodes, _, rest_out, send_sem, recv_sem):
    slab, columns = nodes.shape[2:]
    coarse_rank, _, other, edge = place_of(slab, columns, coarse_rows)
    tm, count = lax.axis_index("tm"), lax.axis_size("tm")
    has_prev, has_next = coarse_rank & (tm > 0), coarse_rank & (tm < count - 1)
    others = slab - coarse_rows
    barrier = pltpu.get_barrier_semaphore()

    def send(source, target):
        pltpu.make_async_remote_copy(
            source,
            target,
            send_sem,
            recv_sem,
            device_id={"tm": tm + 1},
            device_id_type=MESH,
        ).start()

    def total(sem, lately):
        for short in (False, True):

            @pl.when(lately == short)
            def _(short=short):
                rows = others + (BLOCK - BLOCK * CX // columns if short else 0)
                part = rest_out.at[:, pl.ds(0, rows), :]
                pltpu.make_async_copy(part, part, sem).wait()

    @pl.when(has_prev)
    def _():
        pl.semaphore_signal(barrier, inc=1, device_id={"tm": tm - 1}, device_id_type=MESH)

    @pl.when(has_next)
    def _():
        pl.semaphore_wait(barrier, 1)

        @pl.when(defers(tm, slab, coarse_rows))
        def _():
            for side in sides(columns):
                send(
                    nodes.at[1, :, pl.ds(edge, BLOCK), side],
                    rest_out.at[:, pl.ds(others, BLOCK), side],
                )

        send(nodes.at[1, :, pl.ds(other, others), :], rest_out.at[:, pl.ds(0, others), :])

    @pl.when(has_prev)
    def _():
        total(recv_sem, defers(tm - 1, slab, coarse_rows))

    @pl.when(has_next)
    def _():
        total(send_sem, defers(tm, slab, coarse_rows))


def write_rest(coarse_rows, rest, _, start_hbm, sem):
    slab, columns = start_hbm.shape[1:]
    coarse_rank, _, other, edge = place_of(slab, columns, coarse_rows)
    tm, others = lax.axis_index("tm"), slab - coarse_rows

    @pl.when(coarse_rank & (tm > 0))
    def _():
        whole = pltpu.make_async_copy(
            rest.at[:, pl.ds(0, others), :], start_hbm.at[:, pl.ds(other, others), :], sem.at[0]
        )
        strips = [
            pltpu.make_async_copy(
                rest.at[:, pl.ds(others, BLOCK), side],
                start_hbm.at[:, pl.ds(edge, BLOCK), side],
                sem.at[1 + index],
            )
            for index, side in enumerate(sides(columns))
        ]
        for part in range(2 * WRITES):
            height = others // WRITES
            top = part // 2 * height
            pltpu.make_async_copy(
                rest.at[part % 2, pl.ds(top, height), :],
                start_hbm.at[part % 2, pl.ds(pl.multiple_of(other + top, HALO), height), :],
                sem.at[0],
            ).start()
        for act in (lambda c: c.start(), lambda c: c.wait()):

            @pl.when(defers(tm - 1, slab, coarse_rows))
            def _(act=act):
                for strip in strips:
                    act(strip)

        whole.wait()


def body(start_values, node_values):
    slab, columns = start_values.shape[2:]
    peers = lax.axis_size("space")
    coarse_rows = min(slab, max(CX // 2, CX // peers))
    coarse_blocks = coarse_rows // BLOCK
    slots = max(1, min(DETOURS, (lax.axis_size("tm") - 1) // 2))
    hbm = pl.BlockSpec(memory_space=pltpu.HBM)
    vmem = pl.BlockSpec(memory_space=pltpu.VMEM)
    anywhere = pl.BlockSpec(memory_space=pl.ANY)
    dma = pltpu.SemaphoreType.DMA
    start, nodes = pl.pallas_call(
        kernel,
        out_shape=(
            OUT((2, slab, columns), jnp.float32),
            OUT((2, 2, slab, columns), jnp.float32),
        ),
        in_specs=[hbm, hbm],
        out_specs=(vmem, vmem),
        scratch_shapes=[
            pltpu.VMEM((3, 2, slab + 2 * HALO, columns), jnp.float32),
            pltpu.VMEM((2, coarse_rows, CX), jnp.float32),
            pltpu.VMEM((2, coarse_rows, CX), jnp.float32),
            dma((PARTS + 2,)),
            dma((2,)),
            dma((2, 2)),
            dma,
            dma,
            dma,
            dma((PIECES * coarse_blocks,)),
            pltpu.VMEM((slots, 2, DETOUR_ROWS, columns), jnp.float32),
            dma,
            pltpu.SemaphoreType.REGULAR,
            pltpu.SemaphoreType.REGULAR,
            pltpu.SemaphoreType.REGULAR,
        ],
        compiler_params=pltpu.CompilerParams(
            collective_id=0, has_side_effects=True, vmem_limit_bytes=56 * 1024 * 1024
        ),
    )(start_values[0], node_values[0])
    start_hbm, nodes_hbm, written = pl.pallas_call(
        functools.partial(write_out, coarse_rows),
        out_shape=(
            jax.ShapeDtypeStruct(start.shape, jnp.float32),
            jax.ShapeDtypeStruct(nodes.shape, jnp.float32),
            OUT((8, LANES), jnp.float32),
        ),
        in_specs=[anywhere, anywhere],
        out_specs=(hbm, hbm, vmem),
        scratch_shapes=[dma((2,))],
        compiler_params=pltpu.CompilerParams(vmem_limit_bytes=2 * 1024 * 1024),
    )(start, nodes)
    if slab > coarse_rows:
        rest = pl.pallas_call(
            functools.partial(send_rest, coarse_rows),
            out_shape=OUT((2, slab - coarse_rows + BLOCK, columns), jnp.float32),
            in_specs=[anywhere, anywhere],
            out_specs=vmem,
            scratch_shapes=[dma, dma],
            compiler_params=pltpu.CompilerParams(
                collective_id=1, has_side_effects=True, vmem_limit_bytes=4 * 1024 * 1024
            ),
        )(nodes, written)
        start_hbm = pl.pallas_call(
            functools.partial(write_rest, coarse_rows),
            out_shape=jax.ShapeDtypeStruct(start.shape, jnp.float32),
            in_specs=[anywhere, hbm],
            out_specs=hbm,
            scratch_shapes=[dma((3,))],
            input_output_aliases={1: 0},
            compiler_params=pltpu.CompilerParams(vmem_limit_bytes=2 * 1024 * 1024),
        )(rest, start_hbm)
    return (start_hbm[None], nodes_hbm[None])


OUT = pltpu.VMEM


def solution(mesh):
    in_specs = (P("tm", None, "space", None), P("tm", None, None, "space", None))
    out_specs = (P("tm", None, "space", None), P("tm", None, None, "space", None))
    return jax.shard_map(body, mesh=mesh, in_specs=in_specs, out_specs=out_specs, check_vma=False)
```

```python
import functools

import jax
import jax.numpy as jnp
from jax import lax
from jax.experimental import pallas as pl
from jax.experimental.pallas import tpu as pltpu
from jax.sharding import PartitionSpec as P

CX = 256

diffusion = 1.5
drift = 0.8
shear = 0.6
first_weights = (5.0 / 24.0, 1.0 / 3.0, -1.0 / 24.0)
second_weights = (-1.0 / 24.0, 1.0 / 3.0, 5.0 / 24.0)
whole_weights = (1.0 / 6.0, 2.0 / 3.0, 1.0 / 6.0)

MESH = pl.DeviceIdType.MESH
HALO = 8
BLOCK = 32
PARTS = 4
DEFER = 5
WRITES = 2
DETOURS = 3
DETOUR_ROWS = 16
TURN = 2
EARLY = 3
PIECES = 4
LANES = 128


def weighted(weights, fields):
    return [sum(w * f[k] for w, f in zip(weights, fields)) for k in range(2)]


def times(real, imag, field):
    return [real * field[0] - imag * field[1], real * field[1] + imag * field[0]]


def coupled(factor, field):
    length = field[0].shape[0]
    sums = [pltpu.roll(f, 1, 0) + pltpu.roll(f, length - 1, 0) for f in field]
    return [factor * sums[1], -factor * sums[0]]


def defers(tm, slab, coarse_rows):
    return tm < DEFER if slab > coarse_rows else tm < 0


def kernel(
    begin_hbm,
    nodes_hbm,
    start_out,
    nodes_out,
    ext,
    gain,
    shift,
    load_sem,
    halo_send,
    halo_recv,
    bulk_send,
    bulk_recv,
    relay_send,
    relay_recv,
    transit,
    transit_recv,
    below,
    above,
    answer,
):
    slab, columns = begin_hbm.shape[1:]
    peers, count = lax.axis_size("space"), lax.axis_size("tm")
    rows_total = slab * peers
    tm, rank = lax.axis_index("tm"), lax.axis_index("space")
    has_prev, has_next = tm > 0, tm < count - 1
    has_up, has_down = rank > 0, rank < peers - 1
    blocks = slab // BLOCK
    low_row = rows_total // 2 - CX // 2
    low_column = columns // 2 - CX // 2
    coarse_rows = gain.shape[1]
    coarse_blocks = coarse_rows // BLOCK
    inward = min(HALO, slab - coarse_rows)
    coarse_rank = (rank * slab < low_row + CX) & (rank * slab + slab > low_row)
    lower = rank < peers // 2
    coarse_start = jnp.clip(low_row - rank * slab, 0, slab - coarse_rows)
    coarse_block = coarse_start // BLOCK
    first = jnp.where(
        coarse_rank,
        jnp.where(lower, coarse_block, blocks - coarse_block - coarse_blocks),
        0,
    )

    def block_of(step):
        index = jnp.where(step < blocks - first, first + step, blocks - 1 - step)
        return jnp.where(lower, index, blocks - 1 - index)

    def rows_of(block):
        return pl.ds(pl.multiple_of(block * BLOCK, BLOCK), BLOCK)

    def load(slot, top, height, left, width):
        top, left = pl.multiple_of(top, HALO), pl.multiple_of(left, LANES)
        source, here = pl.ds(top, height), pl.ds(left, width)
        target = pl.ds(pl.multiple_of(top + HALO, HALO), height)
        pltpu.make_async_copy(
            begin_hbm.at[:, source, here], ext.at[0, :, target, here], load_sem.at[slot]
        ).start()
        pltpu.make_async_copy(
            nodes_hbm.at[:, :, source, here], ext.at[1:3, :, target, here], load_sem.at[slot]
        ).start()

    def loaded(slot, height, width):
        part = ext.at[:, :, pl.ds(0, height), pl.ds(0, width)]
        pltpu.make_async_copy(part, part, load_sem.at[slot]).wait()

    side_rows = coarse_rows + inward
    head_rows = BLOCK + 2 * HALO if inward else 0
    first_rows, width = BLOCK + HALO, columns // 2
    rest_rows = slab - first_rows - BLOCK

    def load_first():
        top = jnp.where(lower, slab - side_rows, 0)
        if head_rows:
            load(3, jnp.where(lower, top, side_rows - head_rows), head_rows, 0, low_column)
        else:
            load(0, top, side_rows, low_column, CX)

    def load_coarse_rank():
        top = jnp.where(lower, slab - side_rows, 0)
        if head_rows:
            load(0, top, side_rows, low_column, CX)
        rest = jnp.where(lower, top + head_rows, 0)
        load(1, rest, side_rows - head_rows, 0, low_column)
        load(1, top, side_rows, low_column + CX, low_column)
        if slab > side_rows:
            load(2, jnp.where(lower, 0, side_rows), slab - side_rows, 0, columns)

    def load_part(part):
        load(part, jnp.where(lower, 0, slab - first_rows), first_rows, part * width, width)

    def load_other_rank():
        load_part(1)

        load(2, jnp.where(lower, first_rows, rest_rows), BLOCK, 0, columns)
        load(3, jnp.where(lower, slab - rest_rows, 0), rest_rows, 0, columns)

    def begin_copies():
        def copy(top, height, left, width):
            place = (slice(None), pl.ds(pl.multiple_of(top, HALO), height), pl.ds(left, width))
            pltpu.make_async_copy(begin_hbm.at[place], start_out.at[place], bulk_recv).start()

        @pl.when(coarse_rank)
        def _():
            copy(coarse_start, coarse_rows, 0, low_column)
            copy(coarse_start, coarse_rows, low_column + CX, low_column)
            if slab > coarse_rows:
                top = jnp.where(lower, 0, coarse_rows)
                copy(top, slab - coarse_rows, 0, columns)

        @pl.when(jnp.logical_not(coarse_rank))
        def _():
            copy(0, slab, 0, columns)

    def halo_start(side, slot, sources):
        target = pl.ds(slab + HALO if side == 0 else 0, HALO)
        for left, extent in (
            ((low_column, CX),)
            if slot == 0
            else ((0, low_column), (low_column + CX, low_column))
        ):
            here = pl.ds(left, extent)
            for source, place in zip(sources, (0, slice(1, 3))):
                pltpu.make_async_remote_copy(
                    source.at[..., here],
                    ext.at[place, :, target, here],
                    halo_send.at[side],
                    halo_recv.at[side, slot],
                    device_id={"space": rank - 1 if side == 0 else rank + 1},
                    device_id_type=MESH,
                ).start()

    def answered():
        @pl.when(has_down)
        def _():
            pl.semaphore_wait(answer, 1)

    def halo_exchange(slots, loaded_edge):
        for side, exists in ((0, has_up), (1, has_down)):
            edge = pl.ds(0 if side == 0 else slab - HALO, HALO)
            held = pl.ds(HALO if side == 0 else slab, HALO)
            inner = coarse_rank & (lower if side == 1 else jnp.logical_not(lower))
            for slot in slots:
                fit = inner if loaded_edge else jnp.logical_not(inner)
                fit = exists if slot == 1 else exists & fit
                sources = (
                    (ext.at[0, :, held, :], ext.at[1:3, :, held, :])
                    if loaded_edge
                    else (begin_hbm.at[:, edge, :], nodes_hbm.at[:, :, edge, :])
                )

                @pl.when(fit)
                def _(side=side, slot=slot, sources=sources):
                    halo_start(side, slot, sources)

    def halo_wait(block, slot):
        for side, edge in ((0, (block == blocks - 1) & has_down), (1, (block == 0) & has_up)):

            @pl.when(edge)
            def _(side=side):
                part = ext.at[:, :, pl.ds(0, HALO), pl.ds(0, CX if slot == 0 else columns - CX)]
                pltpu.make_async_copy(part, part, halo_recv.at[side, slot]).wait()

    following = {"tm": tm + 1}

    def deferred(tm):
        return defers(tm, slab, coarse_rows)

    def relay_rows(step, origin):
        top = block_of(step // PIECES) * BLOCK + step % PIECES * (BLOCK // PIECES) - origin
        return pl.ds(pl.multiple_of(top, HALO), BLOCK // PIECES)

    def relay_copy(step):
        place = (slice(None), relay_rows(step, 0), pl.ds(low_column, CX))
        return pltpu.make_async_remote_copy(
            nodes_out.at[(1,) + place],
            start_out.at[place],
            relay_send,
            relay_recv.at[step],
            device_id=following,
            device_id_type=MESH,
        )

    detours = min(DETOURS, (count - 1) // 2)
    taking_part = jnp.logical_not(coarse_rank) & (tm <= 2 * detours)
    detoured = taking_part & (tm % 2 == 1)
    detour_rows = transit.shape[2]

    def detour_place():
        top = pl.multiple_of(block_of(blocks - 1) * BLOCK, BLOCK)
        return slice(None), pl.ds(top, detour_rows), slice(None)

    def detour():
        for sign, met, ends in ((1, below, (tm == 0, tm == 2 * detours)), (-1, above, (tm == 2 * detours, tm == 0))):

            @pl.when(jnp.logical_not(ends[0]))
            def _(met=met):
                pl.semaphore_wait(met, 1)

            @pl.when(jnp.logical_not(ends[1]))
            def _(met=met, sign=sign):
                pl.semaphore_signal(
                    met, inc=1, device_id={"tm": tm + sign}, device_id_type=MESH
                )

        slot = tm // 2
        place = detour_place()

        @pl.when(detoured)
        def _():
            pltpu.make_async_remote_copy(
                nodes_out.at[(1,) + place],
                transit.at[slot],
                bulk_send,
                transit_recv,
                device_id={"tm": tm - tm},
                device_id_type=MESH,
            ).start()

        @pl.when(tm == 0)
        def _():
            pltpu.make_async_copy(transit, transit, transit_recv).wait()
            for slot in range(detours):
                pltpu.make_async_remote_copy(
                    transit.at[slot],
                    start_out.at[place],
                    relay_send,
                    bulk_recv,
                    device_id={"tm": tm + 2 * slot + 2},
                    device_id_type=MESH,
                ).start()
            pltpu.make_async_copy(transit, transit, relay_send).wait()

    def bulk_copy(block, left, width, top=0):
        rows = pl.ds(pl.multiple_of(block * BLOCK + top, HALO), BLOCK - top)
        place = (slice(None), rows, pl.ds(pl.multiple_of(left, LANES), width))
        pltpu.make_async_remote_copy(
            nodes_out.at[(1,) + place],
            start_out.at[place],
            bulk_send,
            bulk_recv,
            device_id=following,
            device_id_type=MESH,
        ).start()

    def bulk(unit):
        step, part = unit // PARTS, unit % PARTS
        block = block_of(step)
        strip = coarse_rank & (step < coarse_blocks)
        sent = (step == 0) & (part == PARTS - 2) & (head_rows > 0)

        def copy(left, width):
            bulk_copy(block, left, width)

        @pl.when(strip & (part >= PARTS - 2) & jnp.logical_not(sent))
        def _():
            copy((part - (PARTS - 2)) * (low_column + CX), low_column)

        quick = (step == 0) & jnp.logical_not(coarse_rank)

        @pl.when(quick)
        def _():
            copy(part * (columns // PARTS), columns // PARTS)

        whole = jnp.logical_not(quick | coarse_rank) & (part == PARTS - 1)
        short = detoured & (step == blocks - 1)

        @pl.when(whole & jnp.logical_not(short))
        def _():
            copy(0, columns)

        @pl.when(whole & short)
        def _():
            bulk_copy(block, 0, columns, detour_rows)

    def send(step, low, high):
        held = coarse_rank & deferred(tm) & (step == coarse_blocks - 1)

        @pl.when(has_next & jnp.logical_not(held))
        def _():
            @pl.loop(low, high)
            def _(part):
                bulk(PARTS * step + part)

    barrier = pltpu.get_barrier_semaphore()
    for there, exists in (
        ({"tm": tm - 1}, has_prev),
        ({"space": rank + 1}, has_down),
    ):

        @pl.when(exists)
        def _(there=there):
            pl.semaphore_signal(barrier, inc=1, device_id=there, device_id_type=MESH)

    pl.when(coarse_rank)(load_first)

    @pl.when(jnp.logical_not(coarse_rank))
    def _():
        load_part(0)

    pl.when(coarse_rank)(load_coarse_rank)
    pl.when(jnp.logical_not(coarse_rank))(load_other_rank)

    for side, exists in ((0, has_up), (1, has_down)):

        @pl.when(jnp.logical_not(exists))
        def _(side=side):
            edge = pl.ds(0 if side == 0 else slab + HALO, HALO)
            ext[:, :, edge, :] = jnp.zeros((3, 2, HALO, columns), jnp.float32)

    pl.when(jnp.logical_not(has_prev))(begin_copies)

    def greet():
        friends = jnp.where(has_up, 1, 0) + jnp.where(has_next, 1, 0)

        @pl.when(friends > 0)
        def _():
            pl.semaphore_wait(barrier, friends)

        @pl.when(has_up)
        def _():
            pl.semaphore_signal(
                answer, inc=1, device_id={"space": rank - 1}, device_id_type=MESH
            )
    def strip_compute(block, column, coarse):
        length = BLOCK + 2 * HALO
        span = pl.ds(pl.multiple_of(block * BLOCK, BLOCK), length)
        here = pl.ds(column, LANES)
        begin, one, two = [[ext[f, k, span, here] for k in range(2)] for f in range(3)]
        row = lax.broadcasted_iota(jnp.int32, (length, LANES), 0)
        row = row + (rank * slab + block * BLOCK - HALO)
        along = (row - rows_total // 2).astype(jnp.float32) / (rows_total // 2)
        place = lax.broadcasted_iota(jnp.int32, (1, LANES), 1) + column
        across = (place - columns // 2).astype(jnp.float32) / (columns // 2)
        inside = jnp.where((row >= 0) & (row < rows_total), 1.0, 0.0).astype(jnp.float32)
        real = -diffusion * (along * along + across * across)
        imag = -drift * across
        factor = shear * across
        half_real, half_imag = 1.0 - 0.5 * real, -0.5 * imag
        scale = 1.0 / (half_real * half_real + half_imag * half_imag)
        inverse = (half_real * scale, -half_imag * scale)
        sum_one = weighted(first_weights, (begin, one, two))
        sum_two = weighted(second_weights, (begin, one, two))
        moved = times(real, imag, [s - 0.5 * o for s, o in zip(sum_one, one)])
        turned = coupled(factor, sum_one)
        inner = [begin[k] + moved[k] + turned[k] for k in range(2)]
        node_one = [inside * f for f in times(*inverse, inner)]
        moved = times(real, imag, [s - 0.5 * o for s, o in zip(sum_two, two)])
        turned = coupled(
            factor, [sum_two[k] + 0.5 * (node_one[k] - one[k]) for k in range(2)]
        )
        inner = [node_one[k] + moved[k] + turned[k] for k in range(2)]
        node_two = times(*inverse, inner)
        own = slice(HALO, HALO + BLOCK)
        rows = rows_of(block)
        if not coarse:
            for k in range(2):
                nodes_out[0, k, rows, here] = node_one[k][own]
                nodes_out[1, k, rows, here] = node_two[k][own]
            return
        mean = weighted(whole_weights, (begin, node_one, node_two))
        moved = times(real, imag, [mean[k] - node_two[k] for k in range(2)])
        turned = coupled(factor, mean)
        offset = [moved[k] + turned[k] for k in range(2)]
        step_real, step_imag = 1.0 - real, -imag
        scale = 1.0 / (step_real * step_real + step_imag * step_imag)
        grown = (step_real * scale, -step_imag * scale)
        offset = times(*grown, offset)
        local = pl.ds(pl.multiple_of(block * BLOCK - coarse_start, BLOCK), BLOCK)
        inner_here = pl.ds(pl.multiple_of(column - low_column, LANES), LANES)
        for k in range(2):
            gain[k, local, inner_here] = grown[k][own]
            shift[k, local, inner_here] = offset[k][own]
            kept = node_one[k] - 0.5 * (begin[k] + node_two[k])
            nodes_out[0, k, rows, here] = kept[own]

        @pl.when(jnp.logical_not(has_prev))
        def _():
            for k in range(2):
                start_out[k, rows, here] = begin[k][own]

    def coarse_compute(step):
        block = block_of(step)
        halo_wait(block, 0)

        @pl.loop(0, CX // LANES)
        def _(index):
            strip_compute(block, pl.multiple_of(low_column + index * LANES, LANES), True)

    def relay(low, high):
        @pl.loop(low, high)
        def _(step):
            @pl.when(has_prev)
            def _():
                relay_copy(step).wait_recv()

            rows, local = relay_rows(step, 0), relay_rows(step, coarse_start)
            here = pl.ds(low_column, CX)
            begin = [start_out[k, rows, here] for k in range(2)]
            grown = times(gain[0, local, :], gain[1, local, :], begin)
            finish = [grown[k] + shift[k, local, :] for k in range(2)]
            for k in range(2):
                nodes_out[1, k, rows, here] = finish[k]

            @pl.when(has_next)
            def _():
                relay_copy(step).start()

            for k in range(2):
                nodes_out[0, k, rows, here] += 0.5 * (begin[k] + finish[k])

    never = blocks + 1
    turn = jnp.where(coarse_rank, jnp.minimum(TURN * tm, blocks), never)
    early = jnp.where(coarse_rank, jnp.where(deferred(tm), jnp.minimum(EARLY * tm // 4, turn), turn), blocks)

    @pl.when(coarse_rank)
    def _():
        if head_rows:
            loaded(3, head_rows, low_column)

            @pl.loop(0, low_column // LANES)
            def _(strip):
                left = pl.multiple_of(strip * LANES, LANES)
                strip_compute(block_of(0), left, False)
                pl.when(strip == 0)(greet)

                @pl.when(has_next)
                def _():
                    bulk_copy(block_of(0), left, LANES)
        else:
            greet()
        loaded(0, side_rows, CX)
        answered()
        halo_exchange((0,), True)
        halo_exchange((0, 1), False)

        @pl.loop(0, coarse_blocks - 1)
        def _(step):
            coarse_compute(step)

    greets_first = low_row // slab > 1
    other_rank = jnp.logical_not(coarse_rank)

    if greets_first:

        @pl.when(other_rank)
        def _():
            greet()
            answered()
            halo_exchange((0, 1), False)

    strips = columns // LANES // PARTS

    def step_at(index):
        later = jnp.where(index == blocks - 1, coarse_blocks - 1, index + 1)
        return jnp.where(coarse_rank & (index >= coarse_blocks - 1), later, index)

    @pl.loop(0, blocks + 1)
    def _(index):
        @pl.when(index == turn)
        def _():
            relay(0, PIECES * (coarse_blocks - 1))

        @pl.when(coarse_rank & (index == jnp.minimum(turn, coarse_blocks - 1)))
        def _():
            coarse_compute(coarse_blocks - 1)

        @pl.when(index == turn)
        def _():
            relay(PIECES * (coarse_blocks - 1), PIECES * coarse_blocks)

            @pl.loop(early, turn)
            def _(position):
                send(step_at(position), 0, PARTS)

        @pl.when(index < blocks)
        def _():
            step = step_at(index)
            block = block_of(step)
            in_coarse = coarse_rank & (step < coarse_blocks)

            @pl.when(coarse_rank & (index == 0))
            def _():
                if head_rows:
                    loaded(1, 2 * side_rows - head_rows, low_column)
                else:
                    loaded(1, side_rows, columns - CX)

            if slab > side_rows:

                @pl.when(coarse_rank & (index == coarse_blocks - 1))
                def _():
                    loaded(2, slab - side_rows, columns)

            for slot, height in ((2, BLOCK), (3, rest_rows)):

                @pl.when(jnp.logical_not(coarse_rank) & (step == slot - 1))
                def _(slot=slot, height=height):
                    loaded(slot, height, columns)

            @pl.when(jnp.logical_not(in_coarse))
            def _():
                halo_wait(block, 0)

            halo_wait(block, 1)

            @pl.loop(0, PARTS)
            def _(part):
                @pl.when(jnp.logical_not(coarse_rank) & (step == 0) & (part % (PARTS // 2) == 0))
                def _():
                    loaded(part // (PARTS // 2), first_rows, width)

                @pl.loop(0, strips)
                def _(strip):
                    low = (part * strips + strip) * LANES

                    begun = in_coarse & (step == 0) & (low < low_column) & (head_rows > 0)
                    kept = in_coarse & (low >= low_column) & (low < low_column + CX)

                    @pl.when(jnp.logical_not(begun | kept))
                    def _():
                        strip_compute(block, pl.multiple_of(low, LANES), False)

                if not greets_first:
                    pl.when(other_rank & (step == 0) & (part == 0))(greet)

                    @pl.when(other_rank & (step == 0) & (part == 1))
                    def _():
                        answered()
                        halo_exchange((0, 1), False)

                @pl.when((index < early) | (index >= turn))
                def _():
                    send(step, part, part + 1)

    if detours:
        pl.when(taking_part)(detour)

    def total(sem, height, extent):
        part = start_out.at[:, pl.ds(0, height), pl.ds(0, extent)]
        pltpu.make_async_copy(part, part, sem).wait()

    def all_bulk(sem, rows, lately):
        for short in (False, True):

            @pl.when(coarse_rank & (lately == short))
            def _(short=short):
                extent = rows - BLOCK if short else rows
                narrow = coarse_rows - BLOCK if short else coarse_rows
                total(sem, extent - narrow * CX // columns, columns)

        @pl.when(jnp.logical_not(coarse_rank))
        def _():
            total(sem, slab, columns)

    for side, exists in ((0, has_up), (1, has_down)):

        @pl.when(exists)
        def _(side=side):
            part = ext.at[:, :, pl.ds(0, HALO), :]
            pltpu.make_async_copy(part, part, halo_send.at[side]).wait()

    @pl.when(coarse_rank & has_next)
    def _():
        total(relay_send, coarse_rows, CX)

    @pl.when(jnp.logical_not(has_prev))
    def _():
        all_bulk(bulk_recv, slab, tm < 0)

    @pl.when(has_prev)
    def _():
        all_bulk(bulk_recv, coarse_rows, deferred(tm - 1))

    @pl.when(has_next)
    def _():
        all_bulk(bulk_send, coarse_rows, deferred(tm))


def place_of(slab, columns, coarse_rows):
    peers, rank = lax.axis_size("space"), lax.axis_index("space")
    low_row = slab * peers // 2 - CX // 2
    coarse_rank = (rank * slab < low_row + CX) & (rank * slab + slab > low_row)
    coarse_start = jnp.clip(low_row - rank * slab, 0, slab - coarse_rows)
    lower = rank < peers // 2
    other, edge = jnp.where(lower, 0, coarse_rows), jnp.where(lower, slab - BLOCK, 0)
    return coarse_rank, coarse_start, pl.multiple_of(other, HALO), pl.multiple_of(edge, HALO)


def sides(columns):
    width = columns // 2 - CX // 2
    return pl.ds(0, width), pl.ds(columns - width, width)


def write_out(coarse_rows, start, nodes, start_hbm, nodes_hbm, _, sem):
    slab, columns = start.shape[1:]
    coarse_rank, coarse_start, _, _ = place_of(slab, columns, coarse_rows)
    partly = coarse_rank & (lax.axis_index("tm") > 0)
    for part in range(4 * WRITES):
        height = slab // WRITES
        here = (part // 2 % 2, part % 2, pl.ds(part // 4 * height, height))
        pltpu.make_async_copy(nodes.at[here], nodes_hbm.at[here], sem.at[0]).start()

    def copy(top, height, act):
        here = (slice(None), pl.ds(pl.multiple_of(top, HALO), height), slice(None))
        act(pltpu.make_async_copy(start.at[here], start_hbm.at[here], sem.at[1]))

    for act in (lambda c: c.start(), lambda c: c.wait()):

        @pl.when(partly)
        def _(act=act):
            copy(coarse_start, coarse_rows, act)

        @pl.when(jnp.logical_not(partly))
        def _(act=act):
            copy(0, slab, act)

    pltpu.make_async_copy(nodes, nodes_hbm, sem.at[0]).wait()


def send_rest(coarse_rows, nodes, _, rest_out, send_sem, recv_sem):
    slab, columns = nodes.shape[2:]
    coarse_rank, _, other, edge = place_of(slab, columns, coarse_rows)
    tm, count = lax.axis_index("tm"), lax.axis_size("tm")
    has_prev, has_next = coarse_rank & (tm > 0), coarse_rank & (tm < count - 1)
    others = slab - coarse_rows
    barrier = pltpu.get_barrier_semaphore()

    def send(source, target):
        pltpu.make_async_remote_copy(
            source,
            target,
            send_sem,
            recv_sem,
            device_id={"tm": tm + 1},
            device_id_type=MESH,
        ).start()

    def total(sem, lately):
        for short in (False, True):

            @pl.when(lately == short)
            def _(short=short):
                rows = others + (BLOCK - BLOCK * CX // columns if short else 0)
                part = rest_out.at[:, pl.ds(0, rows), :]
                pltpu.make_async_copy(part, part, sem).wait()

    @pl.when(has_prev)
    def _():
        pl.semaphore_signal(barrier, inc=1, device_id={"tm": tm - 1}, device_id_type=MESH)

    @pl.when(has_next)
    def _():
        pl.semaphore_wait(barrier, 1)

        @pl.when(defers(tm, slab, coarse_rows))
        def _():
            for side in sides(columns):
                send(
                    nodes.at[1, :, pl.ds(edge, BLOCK), side],
                    rest_out.at[:, pl.ds(others, BLOCK), side],
                )

        send(nodes.at[1, :, pl.ds(other, others), :], rest_out.at[:, pl.ds(0, others), :])

    @pl.when(has_prev)
    def _():
        total(recv_sem, defers(tm - 1, slab, coarse_rows))

    @pl.when(has_next)
    def _():
        total(send_sem, defers(tm, slab, coarse_rows))


def write_rest(coarse_rows, rest, _, start_hbm, sem):
    slab, columns = start_hbm.shape[1:]
    coarse_rank, _, other, edge = place_of(slab, columns, coarse_rows)
    tm, others = lax.axis_index("tm"), slab - coarse_rows

    @pl.when(coarse_rank & (tm > 0))
    def _():
        whole = pltpu.make_async_copy(
            rest.at[:, pl.ds(0, others), :], start_hbm.at[:, pl.ds(other, others), :], sem.at[0]
        )
        strips = [
            pltpu.make_async_copy(
                rest.at[:, pl.ds(others, BLOCK), side],
                start_hbm.at[:, pl.ds(edge, BLOCK), side],
                sem.at[1 + index],
            )
            for index, side in enumerate(sides(columns))
        ]
        for part in range(2 * WRITES):
            height = others // WRITES
            top = part // 2 * height
            pltpu.make_async_copy(
                rest.at[part % 2, pl.ds(top, height), :],
                start_hbm.at[part % 2, pl.ds(pl.multiple_of(other + top, HALO), height), :],
                sem.at[0],
            ).start()
        for act in (lambda c: c.start(), lambda c: c.wait()):

            @pl.when(defers(tm - 1, slab, coarse_rows))
            def _(act=act):
                for strip in strips:
                    act(strip)

        whole.wait()


def body(start_values, node_values):
    slab, columns = start_values.shape[2:]
    peers = lax.axis_size("space")
    coarse_rows = min(slab, max(CX // 2, CX // peers))
    coarse_blocks = coarse_rows // BLOCK
    slots = max(1, min(DETOURS, (lax.axis_size("tm") - 1) // 2))
    hbm = pl.BlockSpec(memory_space=pltpu.HBM)
    vmem = pl.BlockSpec(memory_space=pltpu.VMEM)
    anywhere = pl.BlockSpec(memory_space=pl.ANY)
    dma = pltpu.SemaphoreType.DMA
    start, nodes = pl.pallas_call(
        kernel,
        out_shape=(
            OUT((2, slab, columns), jnp.float32),
            OUT((2, 2, slab, columns), jnp.float32),
        ),
        in_specs=[hbm, hbm],
        out_specs=(vmem, vmem),
        scratch_shapes=[
            pltpu.VMEM((3, 2, slab + 2 * HALO, columns), jnp.float32),
            pltpu.VMEM((2, coarse_rows, CX), jnp.float32),
            pltpu.VMEM((2, coarse_rows, CX), jnp.float32),
            dma((4,)),
            dma((2,)),
            dma((2, 2)),
            dma,
            dma,
            dma,
            dma((PIECES * coarse_blocks,)),
            pltpu.VMEM((slots, 2, DETOUR_ROWS, columns), jnp.float32),
            dma,
            pltpu.SemaphoreType.REGULAR,
            pltpu.SemaphoreType.REGULAR,
            pltpu.SemaphoreType.REGULAR,
        ],
        compiler_params=pltpu.CompilerParams(
            collective_id=0, has_side_effects=True, vmem_limit_bytes=56 * 1024 * 1024
        ),
    )(start_values[0], node_values[0])
    start_hbm, nodes_hbm, written = pl.pallas_call(
        functools.partial(write_out, coarse_rows),
        out_shape=(
            jax.ShapeDtypeStruct(start.shape, jnp.float32),
            jax.ShapeDtypeStruct(nodes.shape, jnp.float32),
            OUT((8, LANES), jnp.float32),
        ),
        in_specs=[anywhere, anywhere],
        out_specs=(hbm, hbm, vmem),
        scratch_shapes=[dma((2,))],
        compiler_params=pltpu.CompilerParams(vmem_limit_bytes=2 * 1024 * 1024),
    )(start, nodes)
    if slab > coarse_rows:
        rest = pl.pallas_call(
            functools.partial(send_rest, coarse_rows),
            out_shape=OUT((2, slab - coarse_rows + BLOCK, columns), jnp.float32),
            in_specs=[anywhere, anywhere],
            out_specs=vmem,
            scratch_shapes=[dma, dma],
            compiler_params=pltpu.CompilerParams(
                collective_id=1, has_side_effects=True, vmem_limit_bytes=4 * 1024 * 1024
            ),
        )(nodes, written)
        start_hbm = pl.pallas_call(
            functools.partial(write_rest, coarse_rows),
            out_shape=jax.ShapeDtypeStruct(start.shape, jnp.float32),
            in_specs=[anywhere, hbm],
            out_specs=hbm,
            scratch_shapes=[dma((3,))],
            input_output_aliases={1: 0},
            compiler_params=pltpu.CompilerParams(vmem_limit_bytes=2 * 1024 * 1024),
        )(rest, start_hbm)
    return (start_hbm[None], nodes_hbm[None])


OUT = pltpu.VMEM


def solution(mesh):
    in_specs = (P("tm", None, "space", None), P("tm", None, None, "space", None))
    out_specs = (P("tm", None, "space", None), P("tm", None, None, "space", None))
    return jax.shard_map(body, mesh=mesh, in_specs=in_specs, out_specs=out_specs, check_vma=False)
```

```python
import functools

import jax
import jax.numpy as jnp
from jax import lax
from jax.experimental import pallas as pl
from jax.experimental.pallas import tpu as pltpu
from jax.sharding import PartitionSpec as P

CX = 256

diffusion = 1.5
drift = 0.8
shear = 0.6
first_weights = (5.0 / 24.0, 1.0 / 3.0, -1.0 / 24.0)
second_weights = (-1.0 / 24.0, 1.0 / 3.0, 5.0 / 24.0)
whole_weights = (1.0 / 6.0, 2.0 / 3.0, 1.0 / 6.0)

MESH = pl.DeviceIdType.MESH
HALO = 8
BLOCK = 32
PARTS = 4
DEFER = 5
WRITES = 2
DETOURS = 3
DETOUR_ROWS = 24
TURN = 2
EARLY = 3
PIECES = 4
LANES = 128


def weighted(weights, fields):
    return [sum(w * f[k] for w, f in zip(weights, fields)) for k in range(2)]


def times(real, imag, field):
    return [real * field[0] - imag * field[1], real * field[1] + imag * field[0]]


def coupled(factor, field):
    length = field[0].shape[0]
    sums = [pltpu.roll(f, 1, 0) + pltpu.roll(f, length - 1, 0) for f in field]
    return [factor * sums[1], -factor * sums[0]]


def defers(tm, slab, coarse_rows):
    return (tm < DEFER) & (tm > 0) if slab > coarse_rows else tm < 0


def kernel(
    begin_hbm,
    nodes_hbm,
    start_out,
    nodes_out,
    ext,
    gain,
    shift,
    load_sem,
    halo_send,
    halo_recv,
    bulk_send,
    bulk_recv,
    relay_send,
    relay_recv,
    transit,
    transit_recv,
    below,
    above,
    answer,
):
    slab, columns = begin_hbm.shape[1:]
    peers, count = lax.axis_size("space"), lax.axis_size("tm")
    rows_total = slab * peers
    tm, rank = lax.axis_index("tm"), lax.axis_index("space")
    has_prev, has_next = tm > 0, tm < count - 1
    has_up, has_down = rank > 0, rank < peers - 1
    blocks = slab // BLOCK
    low_row = rows_total // 2 - CX // 2
    low_column = columns // 2 - CX // 2
    coarse_rows = gain.shape[1]
    coarse_blocks = coarse_rows // BLOCK
    inward = min(HALO, slab - coarse_rows)
    coarse_rank = (rank * slab < low_row + CX) & (rank * slab + slab > low_row)
    lower = rank < peers // 2
    coarse_start = jnp.clip(low_row - rank * slab, 0, slab - coarse_rows)
    coarse_block = coarse_start // BLOCK
    first = jnp.where(
        coarse_rank,
        jnp.where(lower, coarse_block, blocks - coarse_block - coarse_blocks),
        0,
    )

    def block_of(step):
        index = jnp.where(step < blocks - first, first + step, blocks - 1 - step)
        return jnp.where(lower, index, blocks - 1 - index)

    def rows_of(block):
        return pl.ds(pl.multiple_of(block * BLOCK, BLOCK), BLOCK)

    def load(slot, top, height, left, width):
        top, left = pl.multiple_of(top, HALO), pl.multiple_of(left, LANES)
        source, here = pl.ds(top, height), pl.ds(left, width)
        target = pl.ds(pl.multiple_of(top + HALO, HALO), height)
        pltpu.make_async_copy(
            begin_hbm.at[:, source, here], ext.at[0, :, target, here], load_sem.at[slot]
        ).start()
        pltpu.make_async_copy(
            nodes_hbm.at[:, :, source, here], ext.at[1:3, :, target, here], load_sem.at[slot]
        ).start()

    def loaded(slot, height, width):
        part = ext.at[:, :, pl.ds(0, height), pl.ds(0, width)]
        pltpu.make_async_copy(part, part, load_sem.at[slot]).wait()

    side_rows = coarse_rows + inward
    head_rows = BLOCK + 2 * HALO if inward else 0
    first_rows, width = BLOCK + HALO, columns // 2
    rest_rows = slab - first_rows - BLOCK

    def load_first():
        top = jnp.where(lower, slab - side_rows, 0)
        if head_rows:
            load(3, jnp.where(lower, top, side_rows - head_rows), head_rows, 0, low_column)
        else:
            load(0, top, side_rows, low_column, CX)

    def load_coarse_rank():
        top = jnp.where(lower, slab - side_rows, 0)
        if head_rows:
            load(0, top, side_rows, low_column, CX)
        rest = jnp.where(lower, top + head_rows, 0)
        load(1, rest, side_rows - head_rows, 0, low_column)
        load(1, top, side_rows, low_column + CX, low_column)
        if slab > side_rows:
            load(2, jnp.where(lower, 0, side_rows), slab - side_rows, 0, columns)

    def load_part(part):
        load(part, jnp.where(lower, 0, slab - first_rows), first_rows, part * width, width)

    def load_other_rank():
        load_part(1)

        load(2, jnp.where(lower, first_rows, rest_rows), BLOCK, 0, columns)
        load(3, jnp.where(lower, slab - rest_rows, 0), rest_rows, 0, columns)

    def begin_copies():
        def copy(top, height, left, width):
            place = (slice(None), pl.ds(pl.multiple_of(top, HALO), height), pl.ds(left, width))
            pltpu.make_async_copy(begin_hbm.at[place], start_out.at[place], bulk_recv).start()

        @pl.when(coarse_rank)
        def _():
            copy(coarse_start, coarse_rows, 0, low_column)
            copy(coarse_start, coarse_rows, low_column + CX, low_column)
            if slab > coarse_rows:
                top = jnp.where(lower, 0, coarse_rows)
                copy(top, slab - coarse_rows, 0, columns)

        @pl.when(jnp.logical_not(coarse_rank))
        def _():
            copy(0, slab, 0, columns)

    def halo_start(side, slot, sources):
        target = pl.ds(slab + HALO if side == 0 else 0, HALO)
        for left, extent in (
            ((low_column, CX),)
            if slot == 0
            else ((0, low_column), (low_column + CX, low_column))
        ):
            here = pl.ds(left, extent)
            for source, place in zip(sources, (0, slice(1, 3))):
                pltpu.make_async_remote_copy(
                    source.at[..., here],
                    ext.at[place, :, target, here],
                    halo_send.at[side],
                    halo_recv.at[side, slot],
                    device_id={"space": rank - 1 if side == 0 else rank + 1},
                    device_id_type=MESH,
                ).start()

    def answered():
        @pl.when(has_down)
        def _():
            pl.semaphore_wait(answer, 1)

    def halo_exchange(slots, loaded_edge):
        for side, exists in ((0, has_up), (1, has_down)):
            edge = pl.ds(0 if side == 0 else slab - HALO, HALO)
            held = pl.ds(HALO if side == 0 else slab, HALO)
            inner = coarse_rank & (lower if side == 1 else jnp.logical_not(lower))
            for slot in slots:
                fit = inner if loaded_edge else jnp.logical_not(inner)
                fit = exists if slot == 1 else exists & fit
                sources = (
                    (ext.at[0, :, held, :], ext.at[1:3, :, held, :])
                    if loaded_edge
                    else (begin_hbm.at[:, edge, :], nodes_hbm.at[:, :, edge, :])
                )

                @pl.when(fit)
                def _(side=side, slot=slot, sources=sources):
                    halo_start(side, slot, sources)

    def halo_wait(block, slot):
        for side, edge in ((0, (block == blocks - 1) & has_down), (1, (block == 0) & has_up)):

            @pl.when(edge)
            def _(side=side):
                part = ext.at[:, :, pl.ds(0, HALO), pl.ds(0, CX if slot == 0 else columns - CX)]
                pltpu.make_async_copy(part, part, halo_recv.at[side, slot]).wait()

    following = {"tm": tm + 1}

    def deferred(tm):
        return defers(tm, slab, coarse_rows)

    def relay_rows(step, origin):
        top = block_of(step // PIECES) * BLOCK + step % PIECES * (BLOCK // PIECES) - origin
        return pl.ds(pl.multiple_of(top, HALO), BLOCK // PIECES)

    def relay_copy(step):
        place = (slice(None), relay_rows(step, 0), pl.ds(low_column, CX))
        return pltpu.make_async_remote_copy(
            nodes_out.at[(1,) + place],
            start_out.at[place],
            relay_send,
            relay_recv.at[step],
            device_id=following,
            device_id_type=MESH,
        )

    detours = min(DETOURS, (count - 1) // 2)
    taking_part = jnp.logical_not(coarse_rank) & (tm <= 2 * detours)
    detoured = taking_part & (tm % 2 == 1)
    detour_rows = transit.shape[2]

    def detour_place():
        top = pl.multiple_of(block_of(blocks - 1) * BLOCK, BLOCK)
        return slice(None), pl.ds(top, detour_rows), slice(None)

    def detour():
        for sign, met, ends in ((1, below, (tm == 0, tm == 2 * detours)), (-1, above, (tm == 2 * detours, tm == 0))):

            @pl.when(jnp.logical_not(ends[0]))
            def _(met=met):
                pl.semaphore_wait(met, 1)

            @pl.when(jnp.logical_not(ends[1]))
            def _(met=met, sign=sign):
                pl.semaphore_signal(
                    met, inc=1, device_id={"tm": tm + sign}, device_id_type=MESH
                )

        slot = tm // 2
        place = detour_place()

        @pl.when(detoured)
        def _():
            pltpu.make_async_remote_copy(
                nodes_out.at[(1,) + place],
                transit.at[slot],
                bulk_send,
                transit_recv,
                device_id={"tm": tm - tm},
                device_id_type=MESH,
            ).start()

        @pl.when(tm == 0)
        def _():
            pltpu.make_async_copy(transit, transit, transit_recv).wait()
            for slot in range(detours):
                pltpu.make_async_remote_copy(
                    transit.at[slot],
                    start_out.at[place],
                    relay_send,
                    bulk_recv,
                    device_id={"tm": tm + 2 * slot + 2},
                    device_id_type=MESH,
                ).start()
            pltpu.make_async_copy(transit, transit, relay_send).wait()

    def bulk_copy(block, left, width, top=0):
        rows = pl.ds(pl.multiple_of(block * BLOCK + top, HALO), BLOCK - top)
        place = (slice(None), rows, pl.ds(pl.multiple_of(left, LANES), width))
        pltpu.make_async_remote_copy(
            nodes_out.at[(1,) + place],
            start_out.at[place],
            bulk_send,
            bulk_recv,
            device_id=following,
            device_id_type=MESH,
        ).start()

    def bulk(unit):
        step, part = unit // PARTS, unit % PARTS
        block = block_of(step)
        strip = coarse_rank & (step < coarse_blocks)
        sent = (step == 0) & (part == PARTS - 2) & (head_rows > 0)

        def copy(left, width):
            bulk_copy(block, left, width)

        @pl.when(strip & (part >= PARTS - 2) & jnp.logical_not(sent))
        def _():
            copy((part - (PARTS - 2)) * (low_column + CX), low_column)

        quick = (step == 0) & jnp.logical_not(coarse_rank)

        @pl.when(quick)
        def _():
            copy(part * (columns // PARTS), columns // PARTS)

        whole = jnp.logical_not(quick | coarse_rank) & (part == PARTS - 1)
        short = detoured & (step == blocks - 1)

        @pl.when(whole & jnp.logical_not(short))
        def _():
            copy(0, columns)

        @pl.when(whole & short)
        def _():
            bulk_copy(block, 0, columns, detour_rows)

    def send(step, low, high):
        held = coarse_rank & deferred(tm) & (step == coarse_blocks - 1)

        @pl.when(has_next & jnp.logical_not(held))
        def _():
            @pl.loop(low, high)
            def _(part):
                bulk(PARTS * step + part)

    barrier = pltpu.get_barrier_semaphore()
    for there, exists in (
        ({"tm": tm - 1}, has_prev),
        ({"space": rank + 1}, has_down),
    ):

        @pl.when(exists)
        def _(there=there):
            pl.semaphore_signal(barrier, inc=1, device_id=there, device_id_type=MESH)

    pl.when(coarse_rank)(load_first)

    @pl.when(jnp.logical_not(coarse_rank))
    def _():
        load_part(0)

    pl.when(coarse_rank)(load_coarse_rank)
    pl.when(jnp.logical_not(coarse_rank))(load_other_rank)

    for side, exists in ((0, has_up), (1, has_down)):

        @pl.when(jnp.logical_not(exists))
        def _(side=side):
            edge = pl.ds(0 if side == 0 else slab + HALO, HALO)
            ext[:, :, edge, :] = jnp.zeros((3, 2, HALO, columns), jnp.float32)

    pl.when(jnp.logical_not(has_prev))(begin_copies)

    def greet():
        friends = jnp.where(has_up, 1, 0) + jnp.where(has_next, 1, 0)

        @pl.when(friends > 0)
        def _():
            pl.semaphore_wait(barrier, friends)

        @pl.when(has_up)
        def _():
            pl.semaphore_signal(
                answer, inc=1, device_id={"space": rank - 1}, device_id_type=MESH
            )
    def strip_compute(block, column, coarse):
        length = BLOCK + 2 * HALO
        span = pl.ds(pl.multiple_of(block * BLOCK, BLOCK), length)
        here = pl.ds(column, LANES)
        begin, one, two = [[ext[f, k, span, here] for k in range(2)] for f in range(3)]
        row = lax.broadcasted_iota(jnp.int32, (length, LANES), 0)
        row = row + (rank * slab + block * BLOCK - HALO)
        along = (row - rows_total // 2).astype(jnp.float32) / (rows_total // 2)
        place = lax.broadcasted_iota(jnp.int32, (1, LANES), 1) + column
        across = (place - columns // 2).astype(jnp.float32) / (columns // 2)
        inside = jnp.where((row >= 0) & (row < rows_total), 1.0, 0.0).astype(jnp.float32)
        real = -diffusion * (along * along + across * across)
        imag = -drift * across
        factor = shear * across
        half_real, half_imag = 1.0 - 0.5 * real, -0.5 * imag
        scale = 1.0 / (half_real * half_real + half_imag * half_imag)
        inverse = (half_real * scale, -half_imag * scale)
        sum_one = weighted(first_weights, (begin, one, two))
        sum_two = weighted(second_weights, (begin, one, two))
        moved = times(real, imag, [s - 0.5 * o for s, o in zip(sum_one, one)])
        turned = coupled(factor, sum_one)
        inner = [begin[k] + moved[k] + turned[k] for k in range(2)]
        node_one = [inside * f for f in times(*inverse, inner)]
        moved = times(real, imag, [s - 0.5 * o for s, o in zip(sum_two, two)])
        turned = coupled(
            factor, [sum_two[k] + 0.5 * (node_one[k] - one[k]) for k in range(2)]
        )
        inner = [node_one[k] + moved[k] + turned[k] for k in range(2)]
        node_two = times(*inverse, inner)
        own = slice(HALO, HALO + BLOCK)
        rows = rows_of(block)
        if not coarse:
            for k in range(2):
                nodes_out[0, k, rows, here] = node_one[k][own]
                nodes_out[1, k, rows, here] = node_two[k][own]
            return
        mean = weighted(whole_weights, (begin, node_one, node_two))
        moved = times(real, imag, [mean[k] - node_two[k] for k in range(2)])
        turned = coupled(factor, mean)
        offset = [moved[k] + turned[k] for k in range(2)]
        step_real, step_imag = 1.0 - real, -imag
        scale = 1.0 / (step_real * step_real + step_imag * step_imag)
        grown = (step_real * scale, -step_imag * scale)
        offset = times(*grown, offset)
        local = pl.ds(pl.multiple_of(block * BLOCK - coarse_start, BLOCK), BLOCK)
        inner_here = pl.ds(pl.multiple_of(column - low_column, LANES), LANES)
        for k in range(2):
            gain[k, local, inner_here] = grown[k][own]
            shift[k, local, inner_here] = offset[k][own]
            kept = node_one[k] - 0.5 * (begin[k] + node_two[k])
            nodes_out[0, k, rows, here] = kept[own]

        @pl.when(jnp.logical_not(has_prev))
        def _():
            for k in range(2):
                start_out[k, rows, here] = begin[k][own]

    def coarse_compute(step):
        block = block_of(step)
        halo_wait(block, 0)

        @pl.loop(0, CX // LANES)
        def _(index):
            strip_compute(block, pl.multiple_of(low_column + index * LANES, LANES), True)

    def relay(low, high):
        @pl.loop(low, high)
        def _(step):
            @pl.when(has_prev)
            def _():
                relay_copy(step).wait_recv()

            rows, local = relay_rows(step, 0), relay_rows(step, coarse_start)
            here = pl.ds(low_column, CX)
            begin = [start_out[k, rows, here] for k in range(2)]
            grown = times(gain[0, local, :], gain[1, local, :], begin)
            finish = [grown[k] + shift[k, local, :] for k in range(2)]
            for k in range(2):
                nodes_out[1, k, rows, here] = finish[k]

            @pl.when(has_next)
            def _():
                relay_copy(step).start()

            for k in range(2):
                nodes_out[0, k, rows, here] += 0.5 * (begin[k] + finish[k])

    never = blocks + 1
    turn = jnp.where(coarse_rank, jnp.minimum(TURN * tm, blocks), never)
    early = jnp.where(coarse_rank, jnp.where(tm < DEFER, jnp.minimum(EARLY * tm // 4, turn), turn), blocks)

    @pl.when(coarse_rank)
    def _():
        if head_rows:
            loaded(3, head_rows, low_column)

            @pl.loop(0, low_column // LANES)
            def _(strip):
                left = pl.multiple_of(strip * LANES, LANES)
                strip_compute(block_of(0), left, False)
                pl.when(strip == 0)(greet)

                @pl.when(has_next)
                def _():
                    bulk_copy(block_of(0), left, LANES)
        else:
            greet()
        loaded(0, side_rows, CX)
        answered()
        halo_exchange((0,), True)
        halo_exchange((0, 1), False)

        @pl.loop(0, coarse_blocks - 1)
        def _(step):
            coarse_compute(step)

    greets_first = low_row // slab > 1
    other_rank = jnp.logical_not(coarse_rank)

    if greets_first:

        @pl.when(other_rank)
        def _():
            greet()
            answered()
            halo_exchange((0, 1), False)

    strips = columns // LANES // PARTS

    def step_at(index):
        later = jnp.where(index == blocks - 1, coarse_blocks - 1, index + 1)
        return jnp.where(coarse_rank & (index >= coarse_blocks - 1), later, index)

    @pl.loop(0, blocks + 1)
    def _(index):
        @pl.when(index == turn)
        def _():
            relay(0, PIECES * (coarse_blocks - 1))

        @pl.when(coarse_rank & (index == jnp.minimum(turn, coarse_blocks - 1)))
        def _():
            coarse_compute(coarse_blocks - 1)

        @pl.when(index == turn)
        def _():
            relay(PIECES * (coarse_blocks - 1), PIECES * coarse_blocks)

            @pl.loop(early, turn)
            def _(position):
                send(step_at(position), 0, PARTS)

        @pl.when(index < blocks)
        def _():
            step = step_at(index)
            block = block_of(step)
            in_coarse = coarse_rank & (step < coarse_blocks)

            @pl.when(coarse_rank & (index == 0))
            def _():
                if head_rows:
                    loaded(1, 2 * side_rows - head_rows, low_column)
                else:
                    loaded(1, side_rows, columns - CX)

            if slab > side_rows:

                @pl.when(coarse_rank & (index == coarse_blocks - 1))
                def _():
                    loaded(2, slab - side_rows, columns)

            for slot, height in ((2, BLOCK), (3, rest_rows)):

                @pl.when(jnp.logical_not(coarse_rank) & (step == slot - 1))
                def _(slot=slot, height=height):
                    loaded(slot, height, columns)

            @pl.when(jnp.logical_not(in_coarse))
            def _():
                halo_wait(block, 0)

            halo_wait(block, 1)

            @pl.loop(0, PARTS)
            def _(part):
                @pl.when(jnp.logical_not(coarse_rank) & (step == 0) & (part % (PARTS // 2) == 0))
                def _():
                    loaded(part // (PARTS // 2), first_rows, width)

                @pl.loop(0, strips)
                def _(strip):
                    low = (part * strips + strip) * LANES

                    begun = in_coarse & (step == 0) & (low < low_column) & (head_rows > 0)
                    kept = in_coarse & (low >= low_column) & (low < low_column + CX)

                    @pl.when(jnp.logical_not(begun | kept))
                    def _():
                        strip_compute(block, pl.multiple_of(low, LANES), False)

                if not greets_first:
                    pl.when(other_rank & (step == 0) & (part == 0))(greet)

                    @pl.when(other_rank & (step == 0) & (part == 1))
                    def _():
                        answered()
                        halo_exchange((0, 1), False)

                @pl.when((index < early) | (index >= turn))
                def _():
                    send(step, part, part + 1)

    if detours:
        pl.when(taking_part)(detour)

    def total(sem, height, extent):
        part = start_out.at[:, pl.ds(0, height), pl.ds(0, extent)]
        pltpu.make_async_copy(part, part, sem).wait()

    def all_bulk(sem, rows, lately):
        for short in (False, True):

            @pl.when(coarse_rank & (lately == short))
            def _(short=short):
                extent = rows - BLOCK if short else rows
                narrow = coarse_rows - BLOCK if short else coarse_rows
                total(sem, extent - narrow * CX // columns, columns)

        @pl.when(jnp.logical_not(coarse_rank))
        def _():
            total(sem, slab, columns)

    for side, exists in ((0, has_up), (1, has_down)):

        @pl.when(exists)
        def _(side=side):
            part = ext.at[:, :, pl.ds(0, HALO), :]
            pltpu.make_async_copy(part, part, halo_send.at[side]).wait()

    @pl.when(coarse_rank & has_next)
    def _():
        total(relay_send, coarse_rows, CX)

    @pl.when(jnp.logical_not(has_prev))
    def _():
        all_bulk(bulk_recv, slab, tm < 0)

    @pl.when(has_prev)
    def _():
        all_bulk(bulk_recv, coarse_rows, deferred(tm - 1))

    @pl.when(has_next)
    def _():
        all_bulk(bulk_send, coarse_rows, deferred(tm))


def place_of(slab, columns, coarse_rows):
    peers, rank = lax.axis_size("space"), lax.axis_index("space")
    low_row = slab * peers // 2 - CX // 2
    coarse_rank = (rank * slab < low_row + CX) & (rank * slab + slab > low_row)
    coarse_start = jnp.clip(low_row - rank * slab, 0, slab - coarse_rows)
    lower = rank < peers // 2
    other, edge = jnp.where(lower, 0, coarse_rows), jnp.where(lower, slab - BLOCK, 0)
    return coarse_rank, coarse_start, pl.multiple_of(other, HALO), pl.multiple_of(edge, HALO)


def sides(columns):
    width = columns // 2 - CX // 2
    return pl.ds(0, width), pl.ds(columns - width, width)


def write_out(coarse_rows, start, nodes, start_hbm, nodes_hbm, _, sem):
    slab, columns = start.shape[1:]
    coarse_rank, coarse_start, _, _ = place_of(slab, columns, coarse_rows)
    partly = coarse_rank & (lax.axis_index("tm") > 0)
    for part in range(4 * WRITES):
        height = slab // WRITES
        here = (part // 2 % 2, part % 2, pl.ds(part // 4 * height, height))
        pltpu.make_async_copy(nodes.at[here], nodes_hbm.at[here], sem.at[0]).start()

    def copy(top, height, act):
        here = (slice(None), pl.ds(pl.multiple_of(top, HALO), height), slice(None))
        act(pltpu.make_async_copy(start.at[here], start_hbm.at[here], sem.at[1]))

    for act in (lambda c: c.start(), lambda c: c.wait()):

        @pl.when(partly)
        def _(act=act):
            copy(coarse_start, coarse_rows, act)

        @pl.when(jnp.logical_not(partly))
        def _(act=act):
            copy(0, slab, act)

    pltpu.make_async_copy(nodes, nodes_hbm, sem.at[0]).wait()


def send_rest(coarse_rows, nodes, _, rest_out, send_sem, recv_sem):
    slab, columns = nodes.shape[2:]
    coarse_rank, _, other, edge = place_of(slab, columns, coarse_rows)
    tm, count = lax.axis_index("tm"), lax.axis_size("tm")
    has_prev, has_next = coarse_rank & (tm > 0), coarse_rank & (tm < count - 1)
    others = slab - coarse_rows
    barrier = pltpu.get_barrier_semaphore()

    def send(source, target):
        pltpu.make_async_remote_copy(
            source,
            target,
            send_sem,
            recv_sem,
            device_id={"tm": tm + 1},
            device_id_type=MESH,
        ).start()

    def total(sem, lately):
        for short in (False, True):

            @pl.when(lately == short)
            def _(short=short):
                rows = others + (BLOCK - BLOCK * CX // columns if short else 0)
                part = rest_out.at[:, pl.ds(0, rows), :]
                pltpu.make_async_copy(part, part, sem).wait()

    @pl.when(has_prev)
    def _():
        pl.semaphore_signal(barrier, inc=1, device_id={"tm": tm - 1}, device_id_type=MESH)

    @pl.when(has_next)
    def _():
        pl.semaphore_wait(barrier, 1)

        @pl.when(defers(tm, slab, coarse_rows))
        def _():
            for side in sides(columns):
                send(
                    nodes.at[1, :, pl.ds(edge, BLOCK), side],
                    rest_out.at[:, pl.ds(others, BLOCK), side],
                )

        send(nodes.at[1, :, pl.ds(other, others), :], rest_out.at[:, pl.ds(0, others), :])

    @pl.when(has_prev)
    def _():
        total(recv_sem, defers(tm - 1, slab, coarse_rows))

    @pl.when(has_next)
    def _():
        total(send_sem, defers(tm, slab, coarse_rows))


def write_rest(coarse_rows, rest, _, start_hbm, sem):
    slab, columns = start_hbm.shape[1:]
    coarse_rank, _, other, edge = place_of(slab, columns, coarse_rows)
    tm, others = lax.axis_index("tm"), slab - coarse_rows

    @pl.when(coarse_rank & (tm > 0))
    def _():
        whole = pltpu.make_async_copy(
            rest.at[:, pl.ds(0, others), :], start_hbm.at[:, pl.ds(other, others), :], sem.at[0]
        )
        strips = [
            pltpu.make_async_copy(
                rest.at[:, pl.ds(others, BLOCK), side],
                start_hbm.at[:, pl.ds(edge, BLOCK), side],
                sem.at[1 + index],
            )
            for index, side in enumerate(sides(columns))
        ]
        for part in range(2 * WRITES):
            height = others // WRITES
            top = part // 2 * height
            pltpu.make_async_copy(
                rest.at[part % 2, pl.ds(top, height), :],
                start_hbm.at[part % 2, pl.ds(pl.multiple_of(other + top, HALO), height), :],
                sem.at[0],
            ).start()
        for act in (lambda c: c.start(), lambda c: c.wait()):

            @pl.when(defers(tm - 1, slab, coarse_rows))
            def _(act=act):
                for strip in strips:
                    act(strip)

        whole.wait()


def body(start_values, node_values):
    slab, columns = start_values.shape[2:]
    peers = lax.axis_size("space")
    coarse_rows = min(slab, max(CX // 2, CX // peers))
    coarse_blocks = coarse_rows // BLOCK
    slots = max(1, min(DETOURS, (lax.axis_size("tm") - 1) // 2))
    hbm = pl.BlockSpec(memory_space=pltpu.HBM)
    vmem = pl.BlockSpec(memory_space=pltpu.VMEM)
    anywhere = pl.BlockSpec(memory_space=pl.ANY)
    dma = pltpu.SemaphoreType.DMA
    start, nodes = pl.pallas_call(
        kernel,
        out_shape=(
            OUT((2, slab, columns), jnp.float32),
            OUT((2, 2, slab, columns), jnp.float32),
        ),
        in_specs=[hbm, hbm],
        out_specs=(vmem, vmem),
        scratch_shapes=[
            pltpu.VMEM((3, 2, slab + 2 * HALO, columns), jnp.float32),
            pltpu.VMEM((2, coarse_rows, CX), jnp.float32),
            pltpu.VMEM((2, coarse_rows, CX), jnp.float32),
            dma((4,)),
            dma((2,)),
            dma((2, 2)),
            dma,
            dma,
            dma,
            dma((PIECES * coarse_blocks,)),
            pltpu.VMEM((slots, 2, DETOUR_ROWS, columns), jnp.float32),
            dma,
            pltpu.SemaphoreType.REGULAR,
            pltpu.SemaphoreType.REGULAR,
            pltpu.SemaphoreType.REGULAR,
        ],
        compiler_params=pltpu.CompilerParams(
            collective_id=0, has_side_effects=True, vmem_limit_bytes=56 * 1024 * 1024
        ),
    )(start_values[0], node_values[0])
    start_hbm, nodes_hbm, written = pl.pallas_call(
        functools.partial(write_out, coarse_rows),
        out_shape=(
            jax.ShapeDtypeStruct(start.shape, jnp.float32),
            jax.ShapeDtypeStruct(nodes.shape, jnp.float32),
            OUT((8, LANES), jnp.float32),
        ),
        in_specs=[anywhere, anywhere],
        out_specs=(hbm, hbm, vmem),
        scratch_shapes=[dma((2,))],
        compiler_params=pltpu.CompilerParams(vmem_limit_bytes=2 * 1024 * 1024),
    )(start, nodes)
    if slab > coarse_rows:
        rest = pl.pallas_call(
            functools.partial(send_rest, coarse_rows),
            out_shape=OUT((2, slab - coarse_rows + BLOCK, columns), jnp.float32),
            in_specs=[anywhere, anywhere],
            out_specs=vmem,
            scratch_shapes=[dma, dma],
            compiler_params=pltpu.CompilerParams(
                collective_id=1, has_side_effects=True, vmem_limit_bytes=4 * 1024 * 1024
            ),
        )(nodes, written)
        start_hbm = pl.pallas_call(
            functools.partial(write_rest, coarse_rows),
            out_shape=jax.ShapeDtypeStruct(start.shape, jnp.float32),
            in_specs=[anywhere, hbm],
            out_specs=hbm,
            scratch_shapes=[dma((3,))],
            input_output_aliases={1: 0},
            compiler_params=pltpu.CompilerParams(vmem_limit_bytes=2 * 1024 * 1024),
        )(rest, start_hbm)
    return (start_hbm[None], nodes_hbm[None])


OUT = pltpu.VMEM


def solution(mesh):
    in_specs = (P("tm", None, "space", None), P("tm", None, None, "space", None))
    out_specs = (P("tm", None, "space", None), P("tm", None, None, "space", None))
    return jax.shard_map(body, mesh=mesh, in_specs=in_specs, out_specs=out_specs, check_vma=False)
```
